32 devices in a mesh: dp: 1 (over z), wy: 4 (over y), wx: 8 (over x, core).
Axes of the slice: x: 4, y: 4, z: 1, core: 2. Of those that a mesh axis runs over, the one named last changes fastest.
The devices are a block of a 4x4x8 slice.
Arguments:
- x_tokens: bfloat16 [32, 128, 2048], P(('dp', 'wy', 'wx'))
- gamma_ln: float32 [2, 2048], replicated
- w_q: bfloat16 [2, 2048, 2048], P(None, 'wx', 'wy')
- w_kv: bfloat16 [2, 2048, 2, 128], P(None, 'wx')
- w_gu: bfloat16 [2, 2048, 2, 8192], P(None, 'wx', None, 'wy')
- w_o: bfloat16 [2, 2048, 2048], P(None, 'wy', 'wx')
- w_d: bfloat16 [2, 8192, 2048], P(None, 'wy', 'wx')
Outputs:
- output 1: bfloat16 [32, 128, 2048], P(('dp', 'wy', 'wx'))
- output 2: bfloat16 [2, 32, 128, 128], P(None, ('dp', 'wy', 'wx'))
- output 3: bfloat16 [2, 32, 128, 128], P(None, ('dp', 'wy', 'wx'))
All inputs are finite; a program needn't handle non-finite values.
Results may differ from the reference program's by a relative error of at most 0.0157459.
Values are sent between devices in bfloat16 or wider.
A program may use at most 768 MiB of HBM per device.

```python
import jax
import jax.numpy as jnp
from jax import lax

D_MODEL = 2048
NUM_HEADS = 16
HEAD_DIM = 128
D_FF = 8192
SEQ_LEN = 128
BATCH_SEQS = 32
N_LAYERS = 2
LN_EPS = 1e-6
ROPE_BASE = 10000.0
Q_WIDTH = NUM_HEADS * HEAD_DIM


def setup_inputs(seed: int = 0, part: int = 0) -> dict:
    base_key = jax.random.key(seed)
    keys_all = jax.random.split(base_key, 7)
    x_key = jax.random.fold_in(keys_all[0], part)
    x_tokens = jax.random.normal(x_key, (BATCH_SEQS, SEQ_LEN, D_MODEL), jnp.float32).astype(jnp.bfloat16)
    gamma_ln = 1.0 + 0.5 * jax.random.normal(keys_all[1], (N_LAYERS, D_MODEL), jnp.float32)
    w_q = (2.5 * D_MODEL ** -0.5) * jax.random.normal(keys_all[2], (N_LAYERS, D_MODEL, Q_WIDTH), jnp.float32)
    w_kv = D_MODEL ** -0.5 * jax.random.normal(keys_all[3], (N_LAYERS, D_MODEL, 2, HEAD_DIM), jnp.float32)
    w_gu = D_MODEL ** -0.5 * jax.random.normal(keys_all[4], (N_LAYERS, D_MODEL, 2, D_FF), jnp.float32)
    w_o = Q_WIDTH ** -0.5 * jax.random.normal(keys_all[5], (N_LAYERS, Q_WIDTH, D_MODEL), jnp.float32)
    w_d = D_FF ** -0.5 * jax.random.normal(keys_all[6], (N_LAYERS, D_FF, D_MODEL), jnp.float32)
    return {'x_tokens': x_tokens, 'gamma_ln': gamma_ln, 'w_q': w_q.astype(jnp.bfloat16), 'w_kv': w_kv.astype(jnp.bfloat16), 'w_gu': w_gu.astype(jnp.bfloat16), 'w_o': w_o.astype(jnp.bfloat16), 'w_d': w_d.astype(jnp.bfloat16)}


def rope_tables():
    half_dim = HEAD_DIM // 2
    inv_freq = ROPE_BASE ** (-2.0 * jnp.arange(half_dim, dtype=jnp.float32) / HEAD_DIM)
    angles = jnp.arange(SEQ_LEN, dtype=jnp.float32)[:, None] * inv_freq[None, :]
    return jnp.cos(angles), jnp.sin(angles)


def rotate(values_in, cos_tab, sin_tab):
    half_dim = HEAD_DIM // 2
    first_half = values_in[..., :half_dim]
    second_half = values_in[..., half_dim:]
    return jnp.concatenate([first_half * cos_tab - second_half * sin_tab, second_half * cos_tab + first_half * sin_tab], axis=-1)


def one_prompt(prompt, gamma_ln, w_q, w_kv, w_gu, w_o, w_d):
    cos_tab, sin_tab = rope_tables()
    allowed = jnp.arange(SEQ_LEN)[:, None] >= jnp.arange(SEQ_LEN)[None, :]

    def layer_step(resid, layer_weights):
        g_scale, wq_l, wkv_l, wgu_l, wo_l, wd_l = layer_weights
        resid_f = resid.astype(jnp.float32)
        centered = resid_f - jnp.mean(resid_f, axis=-1, keepdims=True)
        variance = jnp.mean(centered * centered, axis=-1, keepdims=True)
        normed = (centered * lax.rsqrt(variance + LN_EPS) * g_scale).astype(jnp.bfloat16)
        q_proj = jnp.dot(normed, wq_l, preferred_element_type=jnp.float32).astype(jnp.bfloat16)
        kv_proj = jnp.dot(normed, wkv_l.reshape(D_MODEL, 2 * HEAD_DIM), preferred_element_type=jnp.float32).astype(jnp.bfloat16)
        gu_proj = jnp.dot(normed, wgu_l.reshape(D_MODEL, 2 * D_FF), preferred_element_type=jnp.float32).astype(jnp.bfloat16)
        q_rot = rotate(q_proj.astype(jnp.float32).reshape(SEQ_LEN, NUM_HEADS, HEAD_DIM), cos_tab[:, None, :], sin_tab[:, None, :]).astype(jnp.bfloat16)
        k_rot = rotate(kv_proj[:, :HEAD_DIM].astype(jnp.float32), cos_tab, sin_tab).astype(jnp.bfloat16)
        v_val = kv_proj[:, HEAD_DIM:]
        scores = jnp.einsum('she,te->hst', q_rot.astype(jnp.float32), k_rot.astype(jnp.float32)) * HEAD_DIM ** -0.5
        scores = jnp.where(allowed[None, :, :], scores, -jnp.inf)
        attn_probs = jax.nn.softmax(scores, axis=-1).astype(jnp.bfloat16)
        attended = jnp.einsum('hst,te->she', attn_probs.astype(jnp.float32), v_val.astype(jnp.float32)).astype(jnp.bfloat16)
        hidden = (jax.nn.silu(gu_proj[:, :D_FF].astype(jnp.float32)) * gu_proj[:, D_FF:].astype(jnp.float32)).astype(jnp.bfloat16)
        mixed = jnp.dot(attended.reshape(SEQ_LEN, Q_WIDTH), wo_l, preferred_element_type=jnp.float32) + jnp.dot(hidden, wd_l, preferred_element_type=jnp.float32)
        return (resid_f + mixed).astype(jnp.bfloat16), (k_rot, v_val)

    y_seq, caches = lax.scan(layer_step, prompt, (gamma_ln, w_q, w_kv, w_gu, w_o, w_d))
    return y_seq, caches[0], caches[1]


def reference(x_tokens, gamma_ln, w_q, w_kv, w_gu, w_o, w_d):
    def per_prompt(prompt):
        return one_prompt(prompt, gamma_ln, w_q, w_kv, w_gu, w_o, w_d)
    y_out, k_all, v_all = lax.map(per_prompt, x_tokens)
    return y_out, jnp.swapaxes(k_all, 0, 1), jnp.swapaxes(v_all, 0, 1)
```

```python
import jax
import jax.numpy as jnp
from jax import lax
from jax.sharding import PartitionSpec as P

LN_EPS = 1e-6
ROPE_BASE = 10000.0


def rope_tables(seq_len, head_dim):
    half_dim = head_dim // 2
    inv_freq = ROPE_BASE ** (-2.0 * jnp.arange(half_dim, dtype=jnp.float32) / head_dim)
    angles = jnp.arange(seq_len, dtype=jnp.float32)[:, None] * inv_freq[None, :]
    return jnp.cos(angles), jnp.sin(angles)


def rotate(values_in, cos_tab, sin_tab):
    half_dim = values_in.shape[-1] // 2
    first_half = values_in[..., :half_dim].astype(jnp.float32)
    second_half = values_in[..., half_dim:].astype(jnp.float32)
    rotated = jnp.concatenate([first_half * cos_tab - second_half * sin_tab, second_half * cos_tab + first_half * sin_tab], axis=-1)
    return rotated.astype(jnp.bfloat16)


def layer_norm(resid, g_scale):
    resid_f = resid.astype(jnp.float32)
    centered = resid_f - jnp.mean(resid_f, axis=-1, keepdims=True)
    variance = jnp.mean(centered * centered, axis=-1, keepdims=True)
    return (centered * lax.rsqrt(variance + LN_EPS) * g_scale).astype(jnp.bfloat16)


def causal_attention(q_rot, k_rot, v_val):
    seq_len = q_rot.shape[1]
    score_scale = q_rot.shape[-1] ** -0.5
    scores = jnp.einsum('bshe,bte->bhst', q_rot, k_rot, preferred_element_type=jnp.float32) * score_scale
    allowed = jnp.arange(seq_len)[:, None] >= jnp.arange(seq_len)[None, :]
    scores = jnp.where(allowed, scores, -jnp.inf)
    attn_probs = jax.nn.softmax(scores, axis=-1).astype(jnp.bfloat16)
    attended = jnp.einsum('bhst,bte->bshe', attn_probs, v_val, preferred_element_type=jnp.float32)
    return attended.astype(jnp.bfloat16)


def decoder_layer(resid, g_scale, w_q, w_kv, w_gu, w_o, w_d, cos_tab, sin_tab):
    head_dim = w_kv.shape[-1]
    normed = layer_norm(resid, g_scale)
    group = lax.all_gather(normed, 'wy', axis=0, tiled=True)
    batch_grp, seq_len = group.shape[0], group.shape[1]
    q_proj = jnp.einsum('bsd,dn->bsn', group, w_q, preferred_element_type=jnp.float32).astype(jnp.bfloat16)
    kv_proj = jnp.einsum('bsd,dce->bsce', group, w_kv, preferred_element_type=jnp.float32).astype(jnp.bfloat16)
    gu_proj = jnp.einsum('bsd,dcf->bscf', group, w_gu, preferred_element_type=jnp.float32).astype(jnp.bfloat16)
    q_rot = rotate(q_proj.reshape(batch_grp, seq_len, -1, head_dim), cos_tab[:, None, :], sin_tab[:, None, :])
    k_rot = rotate(kv_proj[:, :, 0], cos_tab, sin_tab)
    v_val = kv_proj[:, :, 1]
    attended = causal_attention(q_rot, k_rot, v_val).reshape(batch_grp, seq_len, -1)
    hidden = (jax.nn.silu(gu_proj[:, :, 0].astype(jnp.float32)) * gu_proj[:, :, 1].astype(jnp.float32)).astype(jnp.bfloat16)
    partial = jnp.einsum('bsn,nd->bsd', attended, w_o, preferred_element_type=jnp.float32) + jnp.einsum('bsf,fd->bsd', hidden, w_d, preferred_element_type=jnp.float32)
    mixed = lax.psum_scatter(partial, 'wy', scatter_dimension=0, tiled=True)
    batch_loc = resid.shape[0]
    mine = lax.axis_index('wy') * batch_loc
    k_own = lax.dynamic_slice_in_dim(k_rot, mine, batch_loc, 0)
    v_own = lax.dynamic_slice_in_dim(v_val, mine, batch_loc, 0)
    return (resid.astype(jnp.float32) + mixed).astype(jnp.bfloat16), k_own, v_own


def solution(mesh):
    batch_axes = ('dp', 'wy', 'wx')
    in_specs = (P(batch_axes), P(), P(None, 'wx', 'wy'), P(None, 'wx'), P(None, 'wx', None, 'wy'), P(None, 'wy', 'wx'), P(None, 'wy', 'wx'))
    out_specs = (P(batch_axes), P(None, batch_axes), P(None, batch_axes))

    def device_step(x_tokens, gamma_ln, w_q, w_kv, w_gu, w_o, w_d):
        cos_tab, sin_tab = rope_tables(x_tokens.shape[1], w_kv.shape[-1])
        resid = x_tokens
        key_list = []
        value_list = []
        for layer_idx in range(w_q.shape[0]):
            full_q = lax.all_gather(w_q[layer_idx], 'wx', axis=0, tiled=True)
            full_kv = lax.all_gather(w_kv[layer_idx], 'wx', axis=0, tiled=True)
            full_gu = lax.all_gather(w_gu[layer_idx], 'wx', axis=0, tiled=True)
            full_o = lax.all_gather(w_o[layer_idx], 'wx', axis=1, tiled=True)
            full_d = lax.all_gather(w_d[layer_idx], 'wx', axis=1, tiled=True)
            resid, k_rot, v_val = decoder_layer(resid, gamma_ln[layer_idx], full_q, full_kv, full_gu, full_o, full_d, cos_tab, sin_tab)
            key_list.append(k_rot)
            value_list.append(v_val)
        return resid, jnp.stack(key_list), jnp.stack(value_list)

    return jax.shard_map(device_step, mesh=mesh, in_specs=in_specs, out_specs=out_specs, check_vma=False)
```

```python
import functools

import jax
import jax.numpy as jnp
from jax import lax
from jax.experimental import pallas as pl
from jax.experimental.pallas import tpu as pltpu
from jax.sharding import PartitionSpec as P

LN_EPS = 1e-6
ROPE_BASE = 10000.0
CORES = 2
GU_CHUNKS = 4
HALVES = 2
BF, F32 = jnp.bfloat16, jnp.float32

LOCAL, SIB, L0, L1, R0, R1, FL, FR = range(8)
A_SIB, A_L, A_R, A_TOP, A_BOT, A_SL, A_SR, A_STOP, A_SBOT = range(9)


def rope_tables(seq_len, head_dim):
    half_dim = head_dim // 2
    inv_freq = ROPE_BASE ** (-2.0 * jnp.arange(half_dim, dtype=F32) / head_dim)
    angles = jnp.arange(seq_len, dtype=F32)[:, None] * inv_freq[None, :]
    return jnp.cos(angles), jnp.sin(angles)


def layers_kernel(dims, x_ref, gamma_ref, cos_ref, sin_ref, wqkv, wgu, wo, wd,
                  y_out, k_out, v_out,
                  bqkv, bgu, bo, bd, hbuf, qbuf, kvbuf, obuf, mbuf, part, rs0, rs1, rs2, resid,
                  w_send, w_recv, a_send, a_recv, kv_send, kv_recv, r_send, r_recv, out_sem):
    layers, n_x, n_y, seq, head_dim, rows, width = dims
    heads = wo.shape[1] // CORES // head_dim
    hid = wd.shape[1] // CORES
    o_rows = wo.shape[1] // CORES
    q_cols = heads * head_dim
    g_cols = wgu.shape[-1] // 2
    n_prompts = CORES * n_y
    toks = n_prompts * seq
    keep = n_y * seq
    tile = toks // 4

    wx = lax.axis_index('wx')
    y = lax.axis_index('wy')
    x, c = wx // CORES, wx % CORES
    xr, xl, xo = (x + 1) % n_x, (x + n_x - 1) % n_x, (x + 2) % n_x
    yr, yl, yo = (y + 1) % n_y, (y + n_y - 1) % n_y, (y + 2) % n_y
    sibling = {'wx': x * CORES + 1 - c}
    right_y, left_y = {'wy': yr}, {'wy': yl}

    def at_x(chip, core):
        return {'wx': chip * CORES + core}

    barrier = pltpu.get_barrier_semaphore()
    peers = [sibling, right_y, left_y] + [at_x(chip, core) for chip in (xr, xl) for core in range(CORES)]
    for peer in peers:
        pl.semaphore_signal(barrier, inc=1, device_id=peer, device_id_type=pl.DeviceIdType.MESH)
    pl.semaphore_wait(barrier, len(peers))

    def remote(src, dst, send_sem, recv_sem, peer):
        return pltpu.make_async_remote_copy(src_ref=src, dst_ref=dst, send_sem=send_sem, recv_sem=recv_sem,
                                            device_id=peer, device_id_type=pl.DeviceIdType.MESH)

    def wait_in(ref, recv_sem, send_sem):
        remote(ref, ref, send_sem, recv_sem, sibling).wait_recv()

    def wait_out(ref, recv_sem, send_sem):
        remote(ref, ref, send_sem, recv_sem, sibling).wait_send()

    pieces = []
    n_blocks = 0
    for l in range(layers):
        pieces.append([('qkv', l, 0, n_blocks)])
        n_blocks += 1
        for j in range(GU_CHUNKS):
            pieces.append([('gu', l, j, n_blocks)])
            n_blocks += 1
        for hh in range(HALVES):
            pieces.append([('o', l, hh, n_blocks), ('d', l, hh, n_blocks + 1)])
            n_blocks += 2
    per_layer = len(pieces) // layers

    def source(block, core):
        kind, l, j, _ = block
        if kind == 'qkv':
            return wqkv.at[l, core]
        if kind == 'gu':
            return wgu.at[l, core, j]
        if kind == 'o':
            return wo.at[l, pl.ds(pl.multiple_of(core * o_rows, o_rows), o_rows), pl.ds(j * width, width)]
        return wd.at[l, pl.ds(pl.multiple_of(core * hid, hid), hid), pl.ds(j * width, width)]

    def landing(block, chip, core):
        kind, l, j, _ = block
        row = pl.ds(pl.multiple_of((chip * CORES + core) * rows, rows), rows)
        col = pl.ds(pl.multiple_of(core * width, width), width)
        if kind == 'qkv':
            return bqkv.at[l, row]
        if kind == 'gu':
            return bgu.at[l, j, row]
        if kind == 'o':
            return bo.at[l, j, chip, :, col]
        return bd.at[l, j, chip, :, col]

    def issue_own(p):
        if p >= len(pieces):
            return
        for block in pieces[p]:
            t = block[3]
            here = landing(block, x, c)
            for core in range(CORES):
                remote(source(block, core), here, w_send.at[t, 2 + core], w_recv.at[t, L0 + c], at_x(xr, core)).start()
                remote(source(block, core), here, w_send.at[t, 4 + core], w_recv.at[t, R0 + c], at_x(xl, core)).start()
            remote(source(block, 1 - c), here, w_send.at[t, SIB], w_recv.at[t, SIB], sibling).start()
            pltpu.make_async_copy(source(block, c), here, w_recv.at[t, LOCAL]).start()

    def wait_block(block, how):
        t = block[3]
        if how == LOCAL:
            pltpu.make_async_copy(source(block, c), landing(block, x, c), w_recv.at[t, LOCAL]).wait()
            return
        chip, core = {SIB: (x, 1 - c), L0: (xl, 0), L1: (xl, 1), R0: (xr, 0), R1: (xr, 1), FL: (xo, 0), FR: (xo, 1)}[how]
        wait_in(landing(block, chip, core), w_recv.at[t, how], w_send.at[t, 0])

    done = [0]

    def comm(p):
        if p >= len(pieces):
            return
        assert p == done[0]
        done[0] = p + 1
        for block in pieces[p]:
            t = block[3]
            wait_block(block, L0)
            from_left = landing(block, xl, 0)
            remote(from_left, from_left, w_send.at[t, 6], w_recv.at[t, FL], at_x(xr, c)).start()
            wait_block(block, R1)
            from_right = landing(block, xr, 1)
            remote(from_right, from_right, w_send.at[t, 7], w_recv.at[t, FR], at_x(xl, c)).start()
        issue_own(p + 2)

    def wait_piece(p, hows):
        for block in pieces[p]:
            for how in hows:
                wait_block(block, how)

    def drain_weights():
        for piece in pieces:
            for block in piece:
                for kind in range(1, 8):
                    wait_out(landing(block, x, c), w_recv.at[block[3], SIB], w_send.at[block[3], kind])

    def prompt(slot, part_of=None):
        if part_of is None:
            return hbuf.at[pl.ds(pl.multiple_of(slot * seq, seq), seq)]
        half = seq // 2
        return hbuf.at[pl.ds(pl.multiple_of(slot * seq + part_of * half, half), half)]

    def a_copy(l, src, dst, kind, peer):
        remote(src, dst, a_send.at[l, kind], a_recv.at[l, kind], peer).start()

    def a_wait(l, ref, kind):
        wait_in(ref, a_recv.at[l, kind], a_send.at[l, kind])

    def gather_send(l):
        a_copy(l, prompt(y), prompt(y), A_L, right_y)
        a_copy(l, prompt(y), prompt(y), A_R, left_y)
        a_copy(l, prompt(y), prompt(n_y + y), A_SIB, sibling)

    def gather_forward(l):
        a_wait(l, prompt(yl), A_L)
        a_copy(l, prompt(yl, 0), prompt(yl, 0), A_TOP, right_y)
        a_copy(l, prompt(yl), prompt(n_y + yl), A_SL, sibling)
        a_wait(l, prompt(yr), A_R)
        a_copy(l, prompt(yr, 1), prompt(yr, 1), A_BOT, left_y)
        a_copy(l, prompt(yr), prompt(n_y + yr), A_SR, sibling)

    def gather_share(l):
        a_wait(l, prompt(yo, 0), A_TOP)
        a_copy(l, prompt(yo, 0), prompt(n_y + yo, 0), A_STOP, sibling)
        a_wait(l, prompt(yo, 1), A_BOT)
        a_copy(l, prompt(yo, 1), prompt(n_y + yo, 1), A_SBOT, sibling)

    def gather_finish(l):
        a_wait(l, prompt(n_y + y), A_SIB)
        a_wait(l, prompt(n_y + yl), A_SL)
        a_wait(l, prompt(n_y + yr), A_SR)
        a_wait(l, prompt(n_y + yo, 0), A_STOP)
        a_wait(l, prompt(n_y + yo, 1), A_SBOT)

    def gather_drain(l):
        for kind in (A_L, A_R, A_SIB, A_SL, A_SR):
            wait_out(prompt(y), a_recv.at[l, kind], a_send.at[l, kind])
        for kind in (A_TOP, A_BOT, A_STOP, A_SBOT):
            wait_out(prompt(y, 0), a_recv.at[l, kind], a_send.at[l, kind])

    n_res = resid.shape[0]
    d_model = n_res * width

    def norm_own(l):
        total = jnp.zeros((seq, 1), F32)
        for i in range(n_res):
            total += jnp.sum(resid[i].astype(F32), axis=-1, keepdims=True)
        mean = total / d_model
        square = jnp.zeros((seq, 1), F32)
        for i in range(n_res):
            centered = resid[i].astype(F32) - mean
            square += jnp.sum(centered * centered, axis=-1, keepdims=True)
        scale = lax.rsqrt(square / d_model + LN_EPS)
        own = pl.ds(pl.multiple_of(y * seq, seq), seq)
        for i in range(n_res):
            value = (resid[i].astype(F32) - mean) * scale * gamma_ref[l, i]
            hbuf[own, i * width:(i + 1) * width] = value.astype(BF)

    def rotate(value):
        value = value.astype(F32)
        return (value * cos_ref[...] + pltpu.roll(value, head_dim // 2, 1) * sin_ref[...]).astype(BF)

    def tiles(body, n=4, size=tile):
        def step(i, carry):
            body(pl.multiple_of(i * size, size))
            return carry
        lax.fori_loop(0, n, step, 0)

    def project_qkv(l):
        def body(start):
            at = pl.ds(start, tile)
            acc = jnp.dot(hbuf[at, :], bqkv[l], preferred_element_type=F32).astype(BF)
            for n in range(heads):
                qbuf[at, n * head_dim:(n + 1) * head_dim] = rotate(acc[:, n * head_dim:(n + 1) * head_dim])
            kv = acc[:, q_cols:]
            kvbuf[c, at, :] = jnp.where(c == 0, rotate(kv), kv)
        tiles(body)

    def kv_refs(lo):
        return kvbuf.at[c, pl.ds(lo * keep, keep)]

    def kv_exchange(l):
        for lo in range(2):
            remote(kv_refs(lo), kv_refs(1 - lo), kv_send.at[l, lo], kv_recv.at[l, lo], sibling).start()

    def kv_outs(l):
        own = pl.ds(pl.multiple_of(y * seq, seq), seq)
        return [pltpu.make_async_copy(kvbuf.at[0, own], k_out.at[l, 0], out_sem.at[2 * l]),
                pltpu.make_async_copy(kvbuf.at[1, own], v_out.at[l, 0], out_sem.at[2 * l + 1])]

    def kv_finish(l):
        for lo in range(2):
            wait_in(kvbuf.at[1 - c, pl.ds((1 - lo) * keep, keep)], kv_recv.at[l, lo], kv_send.at[l, lo])
        for copy in kv_outs(l):
            copy.start()

    def kv_drain(l):
        for lo in range(2):
            wait_out(kv_refs(lo), kv_recv.at[l, lo], kv_send.at[l, lo])
        for copy in kv_outs(l):
            copy.wait()

    def attend():
        score_scale = head_dim ** -0.5
        allowed = lax.broadcasted_iota(jnp.int32, (seq, seq), 0) >= lax.broadcasted_iota(jnp.int32, (seq, seq), 1)

        def body(start):
            at = pl.ds(start, seq)
            key, val = kvbuf[0, at, :], kvbuf[1, at, :]
            for n in range(heads):
                query = qbuf[at, n * head_dim:(n + 1) * head_dim]
                scores = lax.dot_general(query, key, (((1,), (1,)), ((), ())), preferred_element_type=F32) * score_scale
                scores = jnp.where(allowed, scores, -jnp.inf)
                weights = jnp.exp(scores - jnp.max(scores, axis=-1, keepdims=True))
                probs = (weights / jnp.sum(weights, axis=-1, keepdims=True)).astype(BF)
                obuf[at, n * head_dim:(n + 1) * head_dim] = jnp.dot(probs, val, preferred_element_type=F32).astype(BF)
        tiles(body, n_prompts, seq)

    def gate_up(l, j):
        def body(start):
            at = pl.ds(start, tile)
            acc = jnp.dot(hbuf[at, :], bgu[l, j], preferred_element_type=F32).astype(BF).astype(F32)
            mbuf[at, j * g_cols:(j + 1) * g_cols] = (jax.nn.silu(acc[:, :g_cols]) * acc[:, g_cols:]).astype(BF)
        tiles(body)

    chips = [x, xl, xr, xo]
    half_w = width

    def chunk(b, hh):
        return b * HALVES + hh

    def project_out(l, b, hh):
        k = chunk(b, hh)

        def body(start):
            at = pl.ds(start, tile)
            part[k, at, :] = (jnp.dot(obuf[at, :], bo[l, hh, chips[b]], preferred_element_type=F32)
                              + jnp.dot(mbuf[at, :], bd[l, hh, chips[b]], preferred_element_type=F32))

        def step(i, carry):
            body(pl.multiple_of(((i + 2) % 4) * tile, tile))
            return carry
        lax.fori_loop(0, 4, step, 0)
        remote(part.at[k, pl.ds(keep, keep)], rs0.at[k], r_send.at[k, 0], r_recv.at[k, 0], sibling).start()

    def of_chip(k, yy):
        return part.at[k, pl.ds(pl.multiple_of(yy * seq, seq), seq)]

    def of_chip_half(k, yy, side):
        return part.at[k, pl.ds(pl.multiple_of(yy * seq, seq), seq), pl.ds(side * half_w, half_w)]

    def reduce_cores(b, hh):
        k = chunk(b, hh)
        wait_in(rs0.at[k], r_recv.at[k, 0], r_send.at[k, 0])
        part[k, 0:keep, :] += rs0[k]
        remote(of_chip_half(k, yo, 0), rs1.at[k, 0], r_send.at[k, 1], r_recv.at[k, 1], right_y).start()
        remote(of_chip_half(k, yo, 1), rs1.at[k, 1], r_send.at[k, 2], r_recv.at[k, 2], left_y).start()

    def reduce_far(b, hh):
        k = chunk(b, hh)
        for side, target, peer in ((0, yr, right_y), (1, yl, left_y)):
            wait_in(rs1.at[k, side], r_recv.at[k, 1 + side], r_send.at[k, 1 + side])
            at = pl.ds(pl.multiple_of(target * seq, seq), seq)
            part[k, at, side * half_w:(side + 1) * half_w] += rs1[k, side]
            remote(of_chip(k, target), rs2.at[k, side], r_send.at[k, 3 + side], r_recv.at[k, 3 + side], peer).start()

    def out_copy(i, k, core):
        return pltpu.make_async_copy(resid.at[i], y_out.at[0, :, pl.ds(pl.multiple_of(i * width, width), width)],
                                     out_sem.at[2 * layers + CORES * k + core])

    def reduce_last(l, b, hh):
        k = chunk(b, hh)
        for side in range(2):
            wait_in(rs2.at[k, side], r_recv.at[k, 3 + side], r_send.at[k, 3 + side])
        own = pl.ds(pl.multiple_of(y * seq, seq), seq)
        total = part[k, own, :] + rs2[k, 0] + rs2[k, 1]
        for core in range(CORES):
            i = (chips[b] * CORES + core) * HALVES + hh
            resid[i] = (resid[i].astype(F32) + total[:, core * width:(core + 1) * width]).astype(BF)
            if l == layers - 1:
                out_copy(i, k, core).start()

    def reduce_drain():
        for k in range(len(chips) * HALVES):
            wait_out(rs0.at[k], r_recv.at[k, 0], r_send.at[k, 0])
            for side in range(2):
                wait_out(rs1.at[k, side], r_recv.at[k, 1 + side], r_send.at[k, 1 + side])
                wait_out(rs2.at[k, side], r_recv.at[k, 3 + side], r_send.at[k, 3 + side])

    issue_own(0)
    issue_own(1)
    for i in range(n_res):
        resid[i] = x_ref[0, :, i * width:(i + 1) * width]
    norm_own(0)
    gather_send(0)
    comm(0)
    gather_forward(0)
    gather_share(0)
    gather_finish(0)
    rest = (LOCAL, SIB, L1, R0, FL, FR)
    OWN, LEFT, RIGHT, FAR = range(4)
    for l in range(layers):
        base = l * per_layer
        last = l == layers - 1

        def ahead(p):
            while done[0] <= p:
                comm(done[0])

        ahead(base + 1)
        wait_piece(base, rest)
        project_qkv(l)
        kv_exchange(l)
        ahead(base + 2)
        wait_piece(base + 1, rest)
        gate_up(l, 0)
        kv_finish(l)
        attend()
        for j in range(1, GU_CHUNKS):
            ahead(base + 2 + j)
            wait_piece(base + 1 + j, rest)
            gate_up(l, j)
        gather_drain(l)
        kv_drain(l)
        c0, c1 = base + 1 + GU_CHUNKS, base + 2 + GU_CHUNKS
        wait_piece(c0, (LOCAL, SIB))
        project_out(l, OWN, 0)
        wait_piece(c1, (LOCAL, SIB))
        project_out(l, OWN, 1)
        reduce_cores(OWN, 0)
        wait_piece(c0, (L1, R0))
        project_out(l, LEFT, 0)
        reduce_cores(OWN, 1)
        reduce_far(OWN, 0)
        project_out(l, RIGHT, 0)
        reduce_cores(LEFT, 0)
        reduce_far(OWN, 1)
        reduce_cores(RIGHT, 0)
        reduce_last(l, OWN, 0)
        reduce_far(LEFT, 0)
        comm(c1)
        wait_piece(c1, (L1, R0))
        project_out(l, LEFT, 1)
        reduce_far(RIGHT, 0)
        reduce_last(l, OWN, 1)
        project_out(l, RIGHT, 1)
        reduce_cores(LEFT, 1)
        wait_piece(c0, (FL, FR))
        project_out(l, FAR, 0)
        reduce_cores(RIGHT, 1)
        reduce_last(l, LEFT, 0)
        reduce_far(LEFT, 1)
        if not last:
            comm(c1 + 1)
        wait_piece(c1, (FL, FR))
        project_out(l, FAR, 1)
        reduce_cores(FAR, 0)
        reduce_last(l, RIGHT, 0)
        reduce_far(RIGHT, 1)
        reduce_cores(FAR, 1)
        reduce_last(l, LEFT, 1)
        reduce_far(FAR, 0)
        reduce_last(l, RIGHT, 1)
        reduce_far(FAR, 1)
        reduce_last(l, FAR, 0)
        reduce_last(l, FAR, 1)
        reduce_drain()
        if not last:
            norm_own(l + 1)
            comm(c1 + 2)
            gather_send(l + 1)
            gather_forward(l + 1)
            gather_share(l + 1)
            gather_finish(l + 1)
    drain_weights()
    for b in range(len(chips)):
        for hh in range(HALVES):
            for core in range(CORES):
                out_copy((chips[b] * CORES + core) * HALVES + hh, chunk(b, hh), core).wait()


def run_layers(mesh_sizes, x_tokens, gamma_ln, w_q, w_kv, w_gu, w_o, w_d):
    n_x, n_y = mesh_sizes['wx'] // CORES, mesh_sizes['wy']
    assert n_x == 4 and n_y == 4 and x_tokens.shape[0] == 1
    layers, rows, q_loc = w_q.shape
    seq, d_model = x_tokens.shape[1:]
    head_dim = w_kv.shape[-1]
    hid_loc = w_gu.shape[-1]
    hid = hid_loc // CORES
    g_cols = hid // GU_CHUNKS
    q_cols = q_loc // CORES
    width = rows // HALVES
    toks = CORES * n_y * seq
    n_chunks = n_x * HALVES
    n_res = d_model // width
    q_split = jnp.swapaxes(w_q.reshape(layers, rows, CORES, q_cols), 1, 2)
    wqkv = jnp.concatenate([q_split, jnp.swapaxes(w_kv, 1, 2)], axis=-1)
    wgu = w_gu.reshape(layers, rows, 2, CORES, GU_CHUNKS, g_cols).transpose(0, 3, 4, 1, 2, 5)
    wgu = wgu.reshape(layers, CORES, GU_CHUNKS, rows, 2 * g_cols)
    cos_tab, sin_tab = rope_tables(seq, head_dim)
    reps = toks // 4 // seq
    cos_all = jnp.tile(jnp.concatenate([cos_tab, cos_tab], axis=-1), (reps, 1))
    sin_all = jnp.tile(jnp.concatenate([-sin_tab, sin_tab], axis=-1), (reps, 1))
    gamma = gamma_ln.reshape(layers, n_res, 1, width)
    blocks = layers * (1 + GU_CHUNKS + 2 * HALVES)
    dma = pltpu.SemaphoreType.DMA
    in_vmem, anywhere = pl.BlockSpec(memory_space=pltpu.VMEM), pl.BlockSpec(memory_space=pl.ANY)
    cache = jax.ShapeDtypeStruct((layers, 1, seq, head_dim), BF)
    return pl.pallas_call(
        functools.partial(layers_kernel, (layers, n_x, n_y, seq, head_dim, rows, width)),
        out_shape=(jax.ShapeDtypeStruct(x_tokens.shape, BF), cache, cache),
        in_specs=[in_vmem] * 4 + [anywhere] * 4,
        out_specs=(anywhere,) * 3,
        scratch_shapes=[
            pltpu.VMEM((layers, d_model, q_cols + head_dim), BF),
            pltpu.VMEM((layers, GU_CHUNKS, d_model, 2 * g_cols), BF),
            pltpu.VMEM((layers, HALVES, n_x, q_cols, CORES * width), BF),
            pltpu.VMEM((layers, HALVES, n_x, hid, CORES * width), BF),
            pltpu.VMEM((toks, d_model), BF),
            pltpu.VMEM((toks, q_cols), BF),
            pltpu.VMEM((2, toks, head_dim), BF),
            pltpu.VMEM((toks, q_cols), BF),
            pltpu.VMEM((toks, hid), BF),
            pltpu.VMEM((n_chunks, toks, CORES * width), F32),
            pltpu.VMEM((n_chunks, toks // CORES, CORES * width), F32),
            pltpu.VMEM((n_chunks, 2, seq, width), F32),
            pltpu.VMEM((n_chunks, 2, seq, CORES * width), F32),
            pltpu.VMEM((n_res, seq, width), BF),
            dma((blocks, 8)), dma((blocks, 8)),
            dma((layers, 9)), dma((layers, 9)),
            dma((layers, 2)), dma((layers, 2)),
            dma((n_chunks, 5)), dma((n_chunks, 5)),
            dma((2 * layers + CORES * n_chunks,)),
        ],
        compiler_params=pltpu.CompilerParams(collective_id=0, has_side_effects=True, vmem_limit_bytes=67043328),
    )(x_tokens, gamma, cos_all, sin_all, wqkv, wgu, w_o, w_d)


def solution(mesh):
    batch_axes = ('dp', 'wy', 'wx')
    in_specs = (P(batch_axes), P(), P(None, 'wx', 'wy'), P(None, 'wx'), P(None, 'wx', None, 'wy'), P(None, 'wy', 'wx'), P(None, 'wy', 'wx'))
    out_specs = (P(batch_axes), P(None, batch_axes), P(None, batch_axes))
    sizes = dict(mesh.shape)
    return jax.shard_map(functools.partial(run_layers, sizes), mesh=mesh, in_specs=in_specs, out_specs=out_specs, check_vma=False)
```

```python
import functools

import jax
import jax.numpy as jnp
import numpy as np
from jax import lax
from jax.experimental import pallas as pl
from jax.experimental.pallas import tpu as pltpu
from jax.sharding import PartitionSpec as P

LN_EPS = 1e-6
ROPE_BASE = 10000.0
CORES = 2
GU_CHUNKS = 4
HALVES = 2
BF, F32 = jnp.bfloat16, jnp.float32

LOCAL, SIB, L0, L1, R0, R1, FL, FR = range(8)
A_SIB, A_L, A_R, A_TOP, A_BOT, A_SL, A_SR, A_STOP, A_SBOT = range(9)


def rope_tables(seq_len, head_dim):
    inv_freq = np.float32(ROPE_BASE) ** (-2.0 * np.arange(head_dim // 2, dtype=np.float32) / head_dim).astype(np.float32)
    angles = np.arange(seq_len, dtype=np.float32)[:, None] * inv_freq[None, :]
    cos_tab, sin_tab = np.cos(angles.astype(np.float64)), np.sin(angles.astype(np.float64))
    return (np.concatenate([cos_tab, cos_tab], axis=-1).astype(np.float32),
            np.concatenate([-sin_tab, sin_tab], axis=-1).astype(np.float32))


def layers_kernel(dims, gamma_ref, cos_ref, sin_ref, x_ref, wq, wkv, wgu, wo, wd,
                  y_out, k_out, v_out,
                  bqkv, bgu, bo, bd, hbuf, qbuf, kvbuf, obuf, mbuf, part, rs0, rs1, rs2, resid,
                  gu_raw, kv_raw, gu_stage, kv_stage, raw_sem,
                  w_send, w_recv, a_send, a_recv, kv_send, kv_recv, r_send, r_recv, out_sem):
    layers, n_x, n_y, seq, head_dim, rows, width = dims
    heads = wo.shape[1] // CORES // head_dim
    hid = wd.shape[1] // CORES
    o_rows = wo.shape[1] // CORES
    q_cols = heads * head_dim
    g_cols = hid // GU_CHUNKS
    n_prompts = CORES * n_y
    toks = n_prompts * seq
    keep = n_y * seq
    tile = toks // 4

    wx = lax.axis_index('wx')
    y = lax.axis_index('wy')
    x, c = wx // CORES, wx % CORES
    xr, xl, xo = (x + 1) % n_x, (x + n_x - 1) % n_x, (x + 2) % n_x
    yr, yl, yo = (y + 1) % n_y, (y + n_y - 1) % n_y, (y + 2) % n_y
    sibling = {'wx': x * CORES + 1 - c}
    right_y, left_y = {'wy': yr}, {'wy': yl}

    def at_x(chip, core):
        return {'wx': chip * CORES + core}

    n_gu = layers * GU_CHUNKS

    def gu_load(g, core):
        cols = pl.ds(core * hid + (g % GU_CHUNKS) * g_cols, g_cols)
        return pltpu.make_async_copy(wgu.at[g // GU_CHUNKS, :, :, cols], gu_raw.at[g % 2, core], raw_sem.at[g % 2, core])

    def kv_load(l):
        return pltpu.make_async_copy(wkv.at[l], kv_raw.at[l], raw_sem.at[2, l])

    def x_load(i):
        return pltpu.make_async_copy(x_ref.at[0, :, pl.ds(i * width, width)], resid.at[i], raw_sem.at[3 + i // 2, i % 2])

    kv_load(0).start()
    for g in range(2):
        for core in range(CORES):
            gu_load(g, core).start()
    for i in range(resid.shape[0]):
        x_load(i).start()
    for l in range(1, layers):
        kv_load(l).start()

    barrier = pltpu.get_barrier_semaphore()
    peers = [sibling, right_y, left_y] + [at_x(chip, core) for chip in (xr, xl) for core in range(CORES)]
    for peer in peers:
        pl.semaphore_signal(barrier, inc=1, device_id=peer, device_id_type=pl.DeviceIdType.MESH)
    pl.semaphore_wait(barrier, len(peers))

    def remote(src, dst, send_sem, recv_sem, peer):
        return pltpu.make_async_remote_copy(src_ref=src, dst_ref=dst, send_sem=send_sem, recv_sem=recv_sem,
                                            device_id=peer, device_id_type=pl.DeviceIdType.MESH)

    def wait_in(ref, recv_sem, send_sem):
        remote(ref, ref, send_sem, recv_sem, sibling).wait_recv()

    def wait_out(ref, recv_sem, send_sem):
        remote(ref, ref, send_sem, recv_sem, sibling).wait_send()

    pieces = []
    n_blocks = 0
    for l in range(layers):
        pieces.append([('q', l, 0, n_blocks), ('kv', l, 0, n_blocks + 1)])
        n_blocks += 2
        for j in range(GU_CHUNKS):
            pieces.append([('gu', l, j, n_blocks)])
            n_blocks += 1
        for hh in range(HALVES):
            pieces.append([('o', l, hh, n_blocks), ('d', l, hh, n_blocks + 1)])
            n_blocks += 2
    per_layer = len(pieces) // layers
    issue_after = [[p + 2] for p in range(len(pieces))]
    tail = len(pieces) - HALVES
    issue_after[tail - 2] = []
    issue_after[tail - 1] = [tail + hh for hh in range(HALVES)]
    issue_after[tail:] = [[] for _ in range(HALVES)]

    def source(block, core):
        kind, l, j, _ = block
        if kind == 'q':
            return wq.at[l, :, pl.ds(pl.multiple_of(core * q_cols, q_cols), q_cols)]
        if kind == 'kv':
            return kv_stage.at[l, core]
        if kind == 'gu':
            return gu_stage.at[l, j, core]
        if kind == 'o':
            return wo.at[l, pl.ds(pl.multiple_of(core * o_rows, o_rows), o_rows), pl.ds(j * width, width)]
        return wd.at[l, pl.ds(pl.multiple_of(core * hid, hid), hid), pl.ds(j * width, width)]

    def landing(block, chip, core):
        kind, l, j, _ = block
        row = pl.ds(pl.multiple_of((chip * CORES + core) * rows, rows), rows)
        col = pl.ds(pl.multiple_of(core * width, width), width)
        if kind == 'q':
            return bqkv.at[l, row, pl.ds(0, q_cols)]
        if kind == 'kv':
            return bqkv.at[l, row, pl.ds(q_cols, head_dim)]
        if kind == 'gu':
            return bgu.at[l, j, row]
        if kind == 'o':
            return bo.at[l, j, chip, :, col]
        return bd.at[l, j, chip, :, col]

    def prepare_kv(l):
        kv_load(l).wait()
        for core in range(CORES):
            kv_stage[l, core] = kv_raw[l, :, core, :]

    def prepare(p):
        if p >= len(pieces) or pieces[p][0][0] != 'gu':
            return
        _, l, j, _ = pieces[p][0]
        g = l * GU_CHUNKS + j
        step_rows = rows // 4
        for core in range(CORES):
            gu_load(g, core).wait()

            def step(i, carry):
                at = pl.ds(pl.multiple_of(i * step_rows, step_rows), step_rows)
                for which in range(2):
                    gu_stage[l, j, core, at, which * g_cols:(which + 1) * g_cols] = gu_raw[g % 2, core, at, which, :]
                return carry
            lax.fori_loop(0, 4, step, 0)
            if g + 2 < n_gu:
                gu_load(g + 2, core).start()

    def issue_own(p, only=None):
        if p >= len(pieces):
            return
        for block in pieces[p] if only is None else [pieces[p][only]]:
            t = block[3]
            here = landing(block, x, c)
            for core in range(CORES):
                remote(source(block, core), here, w_send.at[t, 2 + core], w_recv.at[t, L0 + c], at_x(xr, core)).start()
                remote(source(block, core), here, w_send.at[t, 4 + core], w_recv.at[t, R0 + c], at_x(xl, core)).start()
            remote(source(block, 1 - c), here, w_send.at[t, SIB], w_recv.at[t, SIB], sibling).start()
            pltpu.make_async_copy(source(block, c), here, w_recv.at[t, LOCAL]).start()

    def wait_block(block, how):
        t = block[3]
        if how == LOCAL:
            pltpu.make_async_copy(source(block, c), landing(block, x, c), w_recv.at[t, LOCAL]).wait()
            return
        chip, core = {SIB: (x, 1 - c), L0: (xl, 0), L1: (xl, 1), R0: (xr, 0), R1: (xr, 1), FL: (xo, 0), FR: (xo, 1)}[how]
        wait_in(landing(block, chip, core), w_recv.at[t, how], w_send.at[t, 0])

    done = [0]

    def comm(p):
        if p >= len(pieces):
            return
        assert p == done[0]
        done[0] = p + 1
        for block in pieces[p]:
            t = block[3]
            wait_block(block, L0)
            from_left = landing(block, xl, 0)
            remote(from_left, from_left, w_send.at[t, 6], w_recv.at[t, FL], at_x(xr, c)).start()
            wait_block(block, R1)
            from_right = landing(block, xr, 1)
            remote(from_right, from_right, w_send.at[t, 7], w_recv.at[t, FR], at_x(xl, c)).start()
        for later in issue_after[p]:
            issue_own(later)
        prepare(p + 3)

    def wait_piece(p, hows):
        for block in pieces[p]:
            for how in hows:
                wait_block(block, how)

    def drain_weights():
        for piece in pieces:
            for block in piece:
                for kind in range(1, 8):
                    wait_out(landing(block, x, c), w_recv.at[block[3], SIB], w_send.at[block[3], kind])

    def prompt(slot, part_of=None):
        if part_of is None:
            return hbuf.at[pl.ds(pl.multiple_of(slot * seq, seq), seq)]
        half = seq // 2
        return hbuf.at[pl.ds(pl.multiple_of(slot * seq + part_of * half, half), half)]

    def a_copy(l, src, dst, kind, peer):
        remote(src, dst, a_send.at[l, kind], a_recv.at[l, kind], peer).start()

    def a_wait(l, ref, kind):
        wait_in(ref, a_recv.at[l, kind], a_send.at[l, kind])

    def gather_send(l):
        a_copy(l, prompt(y), prompt(y), A_L, right_y)
        a_copy(l, prompt(y), prompt(y), A_R, left_y)
        a_copy(l, prompt(y), prompt(n_y + y), A_SIB, sibling)

    def gather_forward(l):
        a_wait(l, prompt(yl), A_L)
        a_copy(l, prompt(yl, 0), prompt(yl, 0), A_TOP, right_y)
        a_copy(l, prompt(yl), prompt(n_y + yl), A_SL, sibling)
        a_wait(l, prompt(yr), A_R)
        a_copy(l, prompt(yr, 1), prompt(yr, 1), A_BOT, left_y)
        a_copy(l, prompt(yr), prompt(n_y + yr), A_SR, sibling)

    def gather_share(l):
        a_wait(l, prompt(yo, 0), A_TOP)
        a_copy(l, prompt(yo, 0), prompt(n_y + yo, 0), A_STOP, sibling)
        a_wait(l, prompt(yo, 1), A_BOT)
        a_copy(l, prompt(yo, 1), prompt(n_y + yo, 1), A_SBOT, sibling)

    def gather_finish(l):
        a_wait(l, prompt(n_y + y), A_SIB)
        a_wait(l, prompt(n_y + yl), A_SL)
        a_wait(l, prompt(n_y + yr), A_SR)
        a_wait(l, prompt(n_y + yo, 0), A_STOP)
        a_wait(l, prompt(n_y + yo, 1), A_SBOT)

    def gather_drain(l):
        for kind in (A_L, A_R, A_SIB, A_SL, A_SR):
            wait_out(prompt(y), a_recv.at[l, kind], a_send.at[l, kind])
        for kind in (A_TOP, A_BOT, A_STOP, A_SBOT):
            wait_out(prompt(y, 0), a_recv.at[l, kind], a_send.at[l, kind])

    n_res = resid.shape[0]
    d_model = n_res * width

    def norm_own(l):
        total = jnp.zeros((seq, 1), F32)
        for i in range(n_res):
            total += jnp.sum(resid[i].astype(F32), axis=-1, keepdims=True)
        mean = total / d_model
        square = jnp.zeros((seq, 1), F32)
        for i in range(n_res):
            centered = resid[i].astype(F32) - mean
            square += jnp.sum(centered * centered, axis=-1, keepdims=True)
        scale = lax.rsqrt(square / d_model + LN_EPS)
        own = pl.ds(pl.multiple_of(y * seq, seq), seq)
        for i in range(n_res):
            value = (resid[i].astype(F32) - mean) * scale * gamma_ref[l:l + 1, i * width:(i + 1) * width]
            hbuf[own, i * width:(i + 1) * width] = value.astype(BF)

    def rotate(value):
        value = value.astype(F32)
        cos_all = jnp.concatenate([cos_ref[...]] * (tile // seq), axis=0)
        sin_all = jnp.concatenate([sin_ref[...]] * (tile // seq), axis=0)
        return (value * cos_all + pltpu.roll(value, head_dim // 2, 1) * sin_all).astype(BF)

    def tiles(body, n=4, size=tile):
        def step(i, carry):
            body(pl.multiple_of(i * size, size))
            return carry
        lax.fori_loop(0, n, step, 0)

    def project_qkv(l):
        def body(start):
            at = pl.ds(start, tile)
            acc = jnp.dot(hbuf[at, :], bqkv[l], preferred_element_type=F32).astype(BF)
            for n in range(heads):
                qbuf[at, n * head_dim:(n + 1) * head_dim] = rotate(acc[:, n * head_dim:(n + 1) * head_dim])
            kv = acc[:, q_cols:]
            kvbuf[c, at, :] = jnp.where(c == 0, rotate(kv), kv)
        tiles(body)

    def kv_refs(lo):
        return kvbuf.at[c, pl.ds(lo * keep, keep)]

    def kv_exchange(l):
        for lo in range(2):
            remote(kv_refs(lo), kv_refs(1 - lo), kv_send.at[l, lo], kv_recv.at[l, lo], sibling).start()

    def kv_outs(l):
        own = pl.ds(pl.multiple_of(y * seq, seq), seq)
        return [pltpu.make_async_copy(kvbuf.at[0, own], k_out.at[l, 0], out_sem.at[2 * l]),
                pltpu.make_async_copy(kvbuf.at[1, own], v_out.at[l, 0], out_sem.at[2 * l + 1])]

    def kv_finish(l):
        for lo in range(2):
            wait_in(kvbuf.at[1 - c, pl.ds((1 - lo) * keep, keep)], kv_recv.at[l, lo], kv_send.at[l, lo])
        for copy in kv_outs(l):
            copy.start()

    def kv_drain(l):
        for lo in range(2):
            wait_out(kv_refs(lo), kv_recv.at[l, lo], kv_send.at[l, lo])
        for copy in kv_outs(l):
            copy.wait()

    def attend():
        score_scale = head_dim ** -0.5
        allowed = lax.broadcasted_iota(jnp.int32, (seq, seq), 0) >= lax.broadcasted_iota(jnp.int32, (seq, seq), 1)

        def body(start):
            at = pl.ds(start, seq)
            key, val = kvbuf[0, at, :], kvbuf[1, at, :]
            for n in range(heads):
                query = qbuf[at, n * head_dim:(n + 1) * head_dim]
                scores = lax.dot_general(query, key, (((1,), (1,)), ((), ())), preferred_element_type=F32) * score_scale
                scores = jnp.where(allowed, scores, -jnp.inf)
                weights = jnp.exp(scores - jnp.max(scores, axis=-1, keepdims=True))
                probs = (weights / jnp.sum(weights, axis=-1, keepdims=True)).astype(BF)
                obuf[at, n * head_dim:(n + 1) * head_dim] = jnp.dot(probs, val, preferred_element_type=F32).astype(BF)
        tiles(body, n_prompts, seq)

    def gate_up(l, j):
        def body(start):
            at = pl.ds(start, tile)
            acc = jnp.dot(hbuf[at, :], bgu[l, j], preferred_element_type=F32).astype(BF).astype(F32)
            mbuf[at, j * g_cols:(j + 1) * g_cols] = (jax.nn.silu(acc[:, :g_cols]) * acc[:, g_cols:]).astype(BF)
        tiles(body)

    chips = [x, xl, xr, xo]
    half_w = width

    def chunk(b, hh):
        return b * HALVES + hh

    def project_out(l, b, hh):
        k = chunk(b, hh)

        def body(start):
            at = pl.ds(start, tile)
            part[k, at, :] = (jnp.dot(obuf[at, :], bo[l, hh, chips[b]], preferred_element_type=F32)
                              + jnp.dot(mbuf[at, :], bd[l, hh, chips[b]], preferred_element_type=F32))

        def step(i, carry):
            body(pl.multiple_of(((i + 2) % 4) * tile, tile))
            return carry
        lax.fori_loop(0, 4, step, 0)
        remote(part.at[k, pl.ds(keep, keep)], rs0.at[k], r_send.at[k, 0], r_recv.at[k, 0], sibling).start()

    def of_chip(k, yy):
        return part.at[k, pl.ds(pl.multiple_of(yy * seq, seq), seq)]

    def of_chip_half(k, yy, side):
        return part.at[k, pl.ds(pl.multiple_of(yy * seq, seq), seq), pl.ds(side * half_w, half_w)]

    def reduce_cores(b, hh):
        k = chunk(b, hh)
        wait_in(rs0.at[k], r_recv.at[k, 0], r_send.at[k, 0])
        part[k, 0:keep, :] += rs0[k]
        remote(of_chip_half(k, yo, 0), rs1.at[k, 0], r_send.at[k, 1], r_recv.at[k, 1], right_y).start()
        remote(of_chip_half(k, yo, 1), rs1.at[k, 1], r_send.at[k, 2], r_recv.at[k, 2], left_y).start()

    def reduce_far(b, hh):
        k = chunk(b, hh)
        for side, target, peer in ((0, yr, right_y), (1, yl, left_y)):
            wait_in(rs1.at[k, side], r_recv.at[k, 1 + side], r_send.at[k, 1 + side])
            at = pl.ds(pl.multiple_of(target * seq, seq), seq)
            part[k, at, side * half_w:(side + 1) * half_w] += rs1[k, side]
            remote(of_chip(k, target), rs2.at[k, side], r_send.at[k, 3 + side], r_recv.at[k, 3 + side], peer).start()

    def out_copy(i, k, core):
        return pltpu.make_async_copy(resid.at[i], y_out.at[0, :, pl.ds(pl.multiple_of(i * width, width), width)],
                                     out_sem.at[2 * layers + CORES * k + core])

    def reduce_last(l, b, hh):
        k = chunk(b, hh)
        for side in range(2):
            wait_in(rs2.at[k, side], r_recv.at[k, 3 + side], r_send.at[k, 3 + side])
        own = pl.ds(pl.multiple_of(y * seq, seq), seq)
        total = part[k, own, :] + rs2[k, 0] + rs2[k, 1]
        for core in range(CORES):
            i = (chips[b] * CORES + core) * HALVES + hh
            resid[i] = (resid[i].astype(F32) + total[:, core * width:(core + 1) * width]).astype(BF)
            if l == layers - 1:
                out_copy(i, k, core).start()

    def reduce_drain():
        for k in range(len(chips) * HALVES):
            wait_out(rs0.at[k], r_recv.at[k, 0], r_send.at[k, 0])
            for side in range(2):
                wait_out(rs1.at[k, side], r_recv.at[k, 1 + side], r_send.at[k, 1 + side])
                wait_out(rs2.at[k, side], r_recv.at[k, 3 + side], r_send.at[k, 3 + side])

    issue_own(0, 0)
    for l in range(layers):
        prepare_kv(l)
    prepare(1)
    issue_own(0, 1)
    issue_own(1)
    prepare(2)
    for i in range(n_res):
        x_load(i).wait()
    norm_own(0)
    gather_send(0)
    comm(0)
    gather_forward(0)
    gather_share(0)
    gather_finish(0)
    rest = (LOCAL, SIB, L1, R0, FL, FR)
    OWN, LEFT, RIGHT, FAR = range(4)
    for l in range(layers):
        base = l * per_layer
        last = l == layers - 1

        def ahead(p):
            while done[0] <= p:
                comm(done[0])

        ahead(base + 1)
        wait_piece(base, rest)
        project_qkv(l)
        kv_exchange(l)
        ahead(base + 2)
        wait_piece(base + 1, rest)
        gate_up(l, 0)
        kv_finish(l)
        attend()
        for j in range(1, GU_CHUNKS):
            ahead(base + 1 + j if last and j == GU_CHUNKS - 1 else base + 2 + j)
            wait_piece(base + 1 + j, rest)
            gate_up(l, j)
        gather_drain(l)
        kv_drain(l)
        c0, c1 = base + 1 + GU_CHUNKS, base + 2 + GU_CHUNKS
        wait_piece(c0, (LOCAL, SIB))
        project_out(l, OWN, 0)
        wait_piece(c1, (LOCAL, SIB))
        project_out(l, OWN, 1)
        reduce_cores(OWN, 0)
        reduce_cores(OWN, 1)
        reduce_far(OWN, 0)
        ahead(c0)
        wait_piece(c0, (L1, R0))
        project_out(l, LEFT, 0)
        reduce_far(OWN, 1)
        project_out(l, RIGHT, 0)
        reduce_cores(LEFT, 0)
        reduce_cores(RIGHT, 0)
        reduce_last(l, OWN, 0)
        reduce_far(LEFT, 0)
        comm(c1)
        wait_piece(c1, (L1, R0))
        project_out(l, LEFT, 1)
        reduce_far(RIGHT, 0)
        reduce_last(l, OWN, 1)
        project_out(l, RIGHT, 1)
        reduce_cores(LEFT, 1)
        wait_piece(c0, (FL, FR))
        project_out(l, FAR, 0)
        reduce_cores(RIGHT, 1)
        reduce_last(l, LEFT, 0)
        reduce_far(LEFT, 1)
        if not last:
            comm(c1 + 1)
        wait_piece(c1, (FL, FR))
        project_out(l, FAR, 1)
        reduce_cores(FAR, 0)
        reduce_last(l, RIGHT, 0)
        reduce_far(RIGHT, 1)
        reduce_cores(FAR, 1)
        reduce_last(l, LEFT, 1)
        reduce_far(FAR, 0)
        reduce_last(l, RIGHT, 1)
        reduce_far(FAR, 1)
        reduce_last(l, FAR, 0)
        reduce_last(l, FAR, 1)
        reduce_drain()
        if not last:
            norm_own(l + 1)
            comm(c1 + 2)
            gather_send(l + 1)
            gather_forward(l + 1)
            gather_share(l + 1)
            gather_finish(l + 1)
    drain_weights()
    for b in range(len(chips)):
        for hh in range(HALVES):
            for core in range(CORES):
                out_copy((chips[b] * CORES + core) * HALVES + hh, chunk(b, hh), core).wait()


def take_over(*refs):
    sources, targets, held, sems = refs[:3], refs[3:6], refs[6:9], refs[9]
    loads = [pltpu.make_async_copy(sources[n], held[n], sems.at[0, n]) for n in range(3)]
    stores = [pltpu.make_async_copy(held[n], targets[n], sems.at[1, n]) for n in range(3)]
    for load in loads:
        load.start()
    for n in (1, 2, 0):
        loads[n].wait()
        stores[n].start()
    for store in stores:
        store.wait()


def run_layers(mesh_sizes, x_tokens, gamma_ln, w_q, w_kv, w_gu, w_o, w_d):
    n_x, n_y = mesh_sizes['wx'] // CORES, mesh_sizes['wy']
    assert n_x == 4 and n_y == 4 and x_tokens.shape[0] == 1
    layers, rows, q_loc = w_q.shape
    seq, d_model = x_tokens.shape[1:]
    head_dim = w_kv.shape[-1]
    hid_loc = w_gu.shape[-1]
    hid = hid_loc // CORES
    g_cols = hid // GU_CHUNKS
    q_cols = q_loc // CORES
    width = rows // HALVES
    toks = CORES * n_y * seq
    n_chunks = n_x * HALVES
    n_res = d_model // width
    cos_all, sin_all = rope_tables(seq, head_dim)
    blocks = layers * (2 + GU_CHUNKS + 2 * HALVES)
    dma = pltpu.SemaphoreType.DMA
    in_vmem, anywhere = pl.BlockSpec(memory_space=pltpu.VMEM), pl.BlockSpec(memory_space=pl.ANY)
    cache = jax.ShapeDtypeStruct((layers, 1, seq, head_dim), BF)
    results = pl.pallas_call(
        functools.partial(layers_kernel, (layers, n_x, n_y, seq, head_dim, rows, width)),
        out_shape=(jax.ShapeDtypeStruct(x_tokens.shape, BF), cache, cache),
        in_specs=[in_vmem] * 3 + [anywhere] * 6,
        out_specs=(anywhere,) * 3,
        scratch_shapes=[
            pltpu.VMEM((layers, d_model, q_cols + head_dim), BF),
            pltpu.VMEM((layers, GU_CHUNKS, d_model, 2 * g_cols), BF),
            pltpu.VMEM((layers, HALVES, n_x, q_cols, CORES * width), BF),
            pltpu.VMEM((layers, HALVES, n_x, hid, CORES * width), BF),
            pltpu.VMEM((toks, d_model), BF),
            pltpu.VMEM((toks, q_cols), BF),
            pltpu.VMEM((2, toks, head_dim), BF),
            pltpu.VMEM((toks, q_cols), BF),
            pltpu.VMEM((toks, hid), BF),
            pltpu.VMEM((n_chunks, toks, CORES * width), F32),
            pltpu.VMEM((n_chunks, toks // CORES, CORES * width), F32),
            pltpu.VMEM((n_chunks, 2, seq, width), F32),
            pltpu.VMEM((n_chunks, 2, seq, CORES * width), F32),
            pltpu.VMEM((n_res, seq, width), BF),
            pltpu.VMEM((2, CORES, rows, 2, g_cols), BF),
            pltpu.VMEM((layers, rows, 2, head_dim), BF),
            pltpu.VMEM((layers, GU_CHUNKS, CORES, rows, 2 * g_cols), BF),
            pltpu.VMEM((layers, 2, rows, head_dim), BF),
            dma((3 + n_res // 2, 2)),
            dma((blocks, 8)), dma((blocks, 8)),
            dma((layers, 9)), dma((layers, 9)),
            dma((layers, 2)), dma((layers, 2)),
            dma((n_chunks, 5)), dma((n_chunks, 5)),
            dma((2 * layers + CORES * n_chunks,)),
        ],
        compiler_params=pltpu.CompilerParams(collective_id=0, has_side_effects=True, vmem_limit_bytes=67043328),
    )(gamma_ln, cos_all, sin_all, x_tokens, w_q, w_kv, w_gu, w_o, w_d)
    shapes = [jax.ShapeDtypeStruct(r.shape, r.dtype) for r in results]
    return pl.pallas_call(
        take_over, out_shape=shapes, in_specs=[anywhere] * 3, out_specs=[anywhere] * 3,
        scratch_shapes=[pltpu.VMEM(r.shape, r.dtype) for r in results] + [dma((2, 3))],
    )(*results)


def solution(mesh):
    batch_axes = ('dp', 'wy', 'wx')
    in_specs = (P(batch_axes), P(), P(None, 'wx', 'wy'), P(None, 'wx'), P(None, 'wx', None, 'wy'), P(None, 'wy', 'wx'), P(None, 'wy', 'wx'))
    out_specs = (P(batch_axes), P(None, batch_axes), P(None, batch_axes))
    sizes = dict(mesh.shape)
    return jax.shard_map(functools.partial(run_layers, sizes), mesh=mesh, in_specs=in_specs, out_specs=out_specs, check_vma=False)
```

```python
import functools

import jax
import jax.numpy as jnp
import numpy as np
from jax import lax
from jax.experimental import pallas as pl
from jax.experimental.pallas import tpu as pltpu
from jax.sharding import PartitionSpec as P

LN_EPS = 1e-6
ROPE_BASE = 10000.0
CORES = 2
GU_CHUNKS = 4
HALVES = 2
BF, F32 = jnp.bfloat16, jnp.float32

L0, R1, SIDES, OWN_CHIP, FAR_CHIP = range(5)
A_L, A_R, A_TOP, A_BOT, A_SIB = range(5)


def rope_tables(seq_len, head_dim):
    inv_freq = np.float32(ROPE_BASE) ** (-2.0 * np.arange(head_dim // 2, dtype=np.float32) / head_dim).astype(np.float32)
    angles = np.arange(seq_len, dtype=np.float32)[:, None] * inv_freq[None, :]
    cos_tab, sin_tab = np.cos(angles.astype(np.float64)), np.sin(angles.astype(np.float64))
    return (np.concatenate([cos_tab, cos_tab], axis=-1).astype(np.float32),
            np.concatenate([-sin_tab, sin_tab], axis=-1).astype(np.float32))


def layers_kernel(dims, gamma_ref, cos_ref, sin_ref, x_ref, wq, wkv, wgu, wo, wd,
                  y_out, k_out, v_out,
                  bq, bkv, bgu, bo, bd, hbuf, qbuf, kvbuf, obuf, mbuf, part, rs0, rs1, rs2, resid,
                  gu_raw, kv_raw, gu_stage, kv_stage, raw_sem,
                  w_send, w_recv, kvw_send, kvw_recv, a_send, a_recv, kv_send, kv_recv, r_send, r_recv, out_sem):
    layers, n_x, n_y, seq, head_dim, rows, width = dims
    heads = wo.shape[1] // CORES // head_dim
    hid = wd.shape[1] // CORES
    o_rows = wo.shape[1] // CORES
    q_cols = heads * head_dim
    g_cols = hid // GU_CHUNKS
    n_prompts = CORES * n_y
    toks = n_prompts * seq
    keep = n_y * seq
    tile = toks // 4

    wx = lax.axis_index('wx')
    y = lax.axis_index('wy')
    x, c = wx // CORES, wx % CORES
    xr, xl, xo = (x + 1) % n_x, (x + n_x - 1) % n_x, (x + 2) % n_x
    yr, yl, yo = (y + 1) % n_y, (y + n_y - 1) % n_y, (y + 2) % n_y
    sibling = {'wx': x * CORES + 1 - c}
    right_y, left_y = {'wy': yr}, {'wy': yl}

    def at_x(chip, core):
        return {'wx': chip * CORES + core}

    n_gu = layers * GU_CHUNKS
    kv_rows = rows // n_y

    def gu_load(g, core):
        cols = pl.ds(core * hid + (g % GU_CHUNKS) * g_cols, g_cols)
        return pltpu.make_async_copy(wgu.at[g // GU_CHUNKS, :, :, cols], gu_raw.at[g % 2, core], raw_sem.at[g % 2])

    def kv_load(l):
        mine = pl.ds(pl.multiple_of(y * kv_rows, kv_rows), kv_rows)
        return pltpu.make_async_copy(wkv.at[l, mine], kv_raw.at[l], raw_sem.at[3 + l])

    def x_load(i):
        return pltpu.make_async_copy(x_ref.at[0, :, pl.ds(i * width, width)], resid.at[i], raw_sem.at[2])

    kv_load(0).start()
    for g in range(2):
        for core in range(CORES):
            gu_load(g, core).start()
    for i in range(resid.shape[0]):
        x_load(i).start()
    for l in range(1, layers):
        kv_load(l).start()

    barrier = pltpu.get_barrier_semaphore()
    peers = [sibling, right_y, left_y] + [at_x(chip, core) for chip in (xr, xl) for core in range(CORES)]
    for peer in peers:
        pl.semaphore_signal(barrier, inc=1, device_id=peer, device_id_type=pl.DeviceIdType.MESH)
    pl.semaphore_wait(barrier, len(peers))

    def remote(src, dst, send_sem, recv_sem, peer):
        return pltpu.make_async_remote_copy(src_ref=src, dst_ref=dst, send_sem=send_sem, recv_sem=recv_sem,
                                            device_id=peer, device_id_type=pl.DeviceIdType.MESH)

    def wait_in(ref, recv_sem, send_sem):
        remote(ref, ref, send_sem, recv_sem, sibling).wait_recv()

    def wait_out(ref, recv_sem, send_sem):
        remote(ref, ref, send_sem, recv_sem, sibling).wait_send()

    order = ('q', 'kv', 'gu', 'o', 'd')
    pieces = []
    n_blocks = 0
    for l in range(layers):
        pieces.append([('q', l, 0, n_blocks), ('kv', l, 0, n_blocks + 1)])
        n_blocks += 2
        for j in range(GU_CHUNKS):
            pieces.append([('gu', l, j, n_blocks)])
            n_blocks += 1
        for hh in range(HALVES):
            pieces.append([('o', l, hh, n_blocks), ('d', l, hh, n_blocks + 1)])
            n_blocks += 2
    per_layer = len(pieces) // layers
    issue_after = [[p + 2] for p in range(len(pieces))]
    tail = len(pieces) - HALVES
    issue_after[tail - 2] = []
    issue_after[tail - 1] = [tail + hh for hh in range(HALVES)]
    issue_after[tail:] = [[] for _ in range(HALVES)]

    def source(block, core):
        kind, l, j, _ = block
        if kind == 'q':
            return wq.at[l, :, pl.ds(pl.multiple_of(core * q_cols, q_cols), q_cols)]
        if kind == 'kv':
            return kv_stage.at[l, core]
        if kind == 'gu':
            return gu_stage.at[l, j, core]
        if kind == 'o':
            return wo.at[l, pl.ds(pl.multiple_of(core * o_rows, o_rows), o_rows), pl.ds(j * width, width)]
        return wd.at[l, pl.ds(pl.multiple_of(core * hid, hid), hid), pl.ds(j * width, width)]

    def landing(block, chip, core):
        kind, l, j, _ = block
        row = pl.ds(pl.multiple_of((chip * CORES + core) * rows, rows), rows)
        col = pl.ds(pl.multiple_of(core * width, width), width)
        if kind == 'q':
            return bq.at[l, row]
        if kind == 'kv':
            return bkv.at[l, chip * CORES + core, y]
        if kind == 'gu':
            return bgu.at[l, j, row]
        if kind == 'o':
            return bo.at[l, j, chip, :, col]
        return bd.at[l, j, chip, :, col]

    def prepare_kv(l):
        kv_load(l).wait()
        for core in range(CORES):
            kv_stage[l, core] = kv_raw[l, :, core, :]

    def prepare(p):
        if p >= len(pieces) or pieces[p][0][0] != 'gu':
            return
        _, l, j, _ = pieces[p][0]
        g = l * GU_CHUNKS + j
        step_rows = rows // 4
        pltpu.make_async_copy(gu_raw.at[g % 2], gu_raw.at[g % 2], raw_sem.at[g % 2]).wait()
        for core in range(CORES):
            def step(i, carry):
                at = pl.ds(pl.multiple_of(i * step_rows, step_rows), step_rows)
                for which in range(2):
                    gu_stage[l, j, core, at, which * g_cols:(which + 1) * g_cols] = gu_raw[g % 2, core, at, which, :]
                return carry
            lax.fori_loop(0, 4, step, 0)
            if g + 2 < n_gu:
                gu_load(g + 2, core).start()

    def issue_own(p, only=None):
        if p >= len(pieces):
            return
        for block in pieces[p] if only is None else [pieces[p][only]]:
            t = block[3]
            here = landing(block, x, c)
            sent = w_send.at[order.index(block[0])]
            side = [SIDES * c, SIDES - c]
            for core in range(CORES):
                remote(source(block, core), here, sent, w_recv.at[t, side[0]], at_x(xr, core)).start()
                remote(source(block, core), here, sent, w_recv.at[t, side[1]], at_x(xl, core)).start()
            remote(source(block, 1 - c), here, sent, w_recv.at[t, OWN_CHIP], sibling).start()
            pltpu.make_async_copy(source(block, c), here, w_recv.at[t, OWN_CHIP]).start()

    def pair(block, chip):
        kind, l, j, _ = block
        row = pl.ds(pl.multiple_of(chip * CORES * rows, CORES * rows), CORES * rows)
        if kind == 'q':
            return bq.at[l, row]
        if kind == 'kv':
            return bkv.at[l, pl.ds(chip * CORES, CORES), y]
        if kind == 'gu':
            return bgu.at[l, j, row]
        return (bo if kind == 'o' else bd).at[l, j, chip]

    def wait_block(block, how):
        ref = {L0: lambda: landing(block, xl, 0), R1: lambda: landing(block, xr, 1), SIDES: lambda: pair(block, xl),
               OWN_CHIP: lambda: pair(block, x), FAR_CHIP: lambda: pair(block, xo)}[how]()
        wait_in(ref, w_recv.at[block[3], how], w_send.at[0])

    done = [0]

    def comm(p):
        if p >= len(pieces):
            return
        assert p == done[0]
        done[0] = p + 1
        for block in pieces[p]:
            t = block[3]
            wait_block(block, L0)
            from_left = landing(block, xl, 0)
            remote(from_left, from_left, w_send.at[order.index(block[0])], w_recv.at[t, FAR_CHIP], at_x(xr, c)).start()
            wait_block(block, R1)
            from_right = landing(block, xr, 1)
            remote(from_right, from_right, w_send.at[order.index(block[0])], w_recv.at[t, FAR_CHIP], at_x(xl, c)).start()
        for later in issue_after[p]:
            issue_own(later)
        prepare(p + 3)

    def wait_piece(p, hows):
        for block in pieces[p]:
            for how in hows:
                wait_block(block, how)

    def drain_weights():
        sources = n_x * CORES
        for n, ref in enumerate((bq.at[:, pl.ds(0, (sources - 1) * rows)], bkv.at[:, pl.ds(0, sources - 1), 0],
                                 bgu.at[:, :, pl.ds(0, (sources - 1) * rows)],
                                 bo.at[:, :, :, pl.ds(0, o_rows // sources * (sources - 1))],
                                 bd.at[:, :, :, pl.ds(0, hid // sources * (sources - 1))])):
            wait_out(ref, w_recv.at[0, 0], w_send.at[n])

    def kv_quarter(l, yy, half=None):
        n_src = n_x * CORES
        return bkv.at[l, pl.ds(0 if half is None else half * (n_src // 2), n_src if half is None else n_src // 2), yy]

    def kvw_copy(l, ref, kind, peer):
        remote(ref, ref, kvw_send.at[l], kvw_recv.at[l, kind], peer).start()

    def kvw_send_own(l):
        kvw_copy(l, kv_quarter(l, y), A_L, right_y)
        kvw_copy(l, kv_quarter(l, y), A_R, left_y)

    def kvw_forward(l):
        wait_in(kv_quarter(l, yl), kvw_recv.at[l, A_L], kvw_send.at[l])
        kvw_copy(l, kv_quarter(l, yl, 0), A_TOP, right_y)
        wait_in(kv_quarter(l, yr), kvw_recv.at[l, A_R], kvw_send.at[l])
        kvw_copy(l, kv_quarter(l, yr, 1), A_BOT, left_y)

    def kvw_finish(l):
        wait_in(kv_quarter(l, yo, 0), kvw_recv.at[l, A_TOP], kvw_send.at[l])
        wait_in(kv_quarter(l, yo, 1), kvw_recv.at[l, A_BOT], kvw_send.at[l])
        wait_out(bkv.at[l, :, pl.ds(0, n_y - 1)], kvw_recv.at[l, A_L], kvw_send.at[l])

    def prompt(slot, part_of=None):
        if part_of is None:
            return hbuf.at[pl.ds(pl.multiple_of(slot * seq, seq), seq)]
        half = seq // 2
        return hbuf.at[pl.ds(pl.multiple_of(slot * seq + part_of * half, half), half)]

    def a_copy(l, src, dst, kind, peer):
        remote(src, dst, a_send.at[l], a_recv.at[l, kind], peer).start()

    def a_wait(l, ref, kind):
        wait_in(ref, a_recv.at[l, kind], a_send.at[l])

    def gather_send(l):
        a_copy(l, prompt(y), prompt(y), A_L, right_y)
        a_copy(l, prompt(y), prompt(y), A_R, left_y)
        a_copy(l, prompt(y), prompt(n_y + y), A_SIB, sibling)

    def gather_forward(l):
        a_wait(l, prompt(yl), A_L)
        a_copy(l, prompt(yl, 0), prompt(yl, 0), A_TOP, right_y)
        a_copy(l, prompt(yl), prompt(n_y + yl), A_SIB, sibling)
        a_wait(l, prompt(yr), A_R)
        a_copy(l, prompt(yr, 1), prompt(yr, 1), A_BOT, left_y)
        a_copy(l, prompt(yr), prompt(n_y + yr), A_SIB, sibling)

    def gather_share(l):
        a_wait(l, prompt(yo, 0), A_TOP)
        a_copy(l, prompt(yo, 0), prompt(n_y + yo, 0), A_SIB, sibling)
        a_wait(l, prompt(yo, 1), A_BOT)
        a_copy(l, prompt(yo, 1), prompt(n_y + yo, 1), A_SIB, sibling)

    def gather_finish(l):
        a_wait(l, hbuf.at[pl.ds(keep, keep)], A_SIB)

    def gather_drain(l):
        wait_out(hbuf.at[pl.ds(0, 7 * seq)], a_recv.at[l, A_L], a_send.at[l])

    n_res = resid.shape[0]
    d_model = n_res * width

    def norm_own(l):
        total = jnp.zeros((seq, 1), F32)
        for i in range(n_res):
            total += jnp.sum(resid[i].astype(F32), axis=-1, keepdims=True)
        mean = total / d_model
        square = jnp.zeros((seq, 1), F32)
        for i in range(n_res):
            centered = resid[i].astype(F32) - mean
            square += jnp.sum(centered * centered, axis=-1, keepdims=True)
        scale = lax.rsqrt(square / d_model + LN_EPS)
        own = pl.ds(pl.multiple_of(y * seq, seq), seq)
        for i in range(n_res):
            value = (resid[i].astype(F32) - mean) * scale * gamma_ref[l:l + 1, i * width:(i + 1) * width]
            hbuf[own, i * width:(i + 1) * width] = value.astype(BF)

    def rotate(value):
        value = value.astype(F32)
        cos_all = jnp.concatenate([cos_ref[...]] * (tile // seq), axis=0)
        sin_all = jnp.concatenate([sin_ref[...]] * (tile // seq), axis=0)
        return (value * cos_all + pltpu.roll(value, head_dim // 2, 1) * sin_all).astype(BF)

    def tiles(body, n=4, size=tile):
        def step(i, carry):
            body(pl.multiple_of(i * size, size))
            return carry
        lax.fori_loop(0, n, step, 0)

    def project_q(l):
        def body(start):
            at = pl.ds(start, tile)
            acc = jnp.dot(hbuf[at, :], bq[l], preferred_element_type=F32).astype(BF)
            for n in range(heads):
                qbuf[at, n * head_dim:(n + 1) * head_dim] = rotate(acc[:, n * head_dim:(n + 1) * head_dim])
        tiles(body)

    def project_kv(l):
        def body(start):
            at = pl.ds(start, tile)
            weights = bkv[l].reshape(d_model, head_dim)
            kv = jnp.dot(hbuf[at, :], weights, preferred_element_type=F32).astype(BF)
            kvbuf[c, at, :] = jnp.where(c == 0, rotate(kv), kv)
        tiles(body)

    def kv_refs(lo):
        return kvbuf.at[c, pl.ds(lo * keep, keep)]

    def kv_exchange(l):
        for lo in range(2):
            remote(kv_refs(lo), kv_refs(1 - lo), kv_send.at[l], kv_recv.at[l], sibling).start()

    def kv_outs(l):
        own = pl.ds(pl.multiple_of(y * seq, seq), seq)
        return [pltpu.make_async_copy(kvbuf.at[0, own], k_out.at[l, 0], out_sem.at[l]),
                pltpu.make_async_copy(kvbuf.at[1, own], v_out.at[l, 0], out_sem.at[l])]

    def kv_finish(l):
        wait_in(kvbuf.at[1 - c], kv_recv.at[l], kv_send.at[l])
        for copy in kv_outs(l):
            copy.start()

    def kv_drain(l):
        wait_out(kvbuf.at[c], kv_recv.at[l], kv_send.at[l])
        both = kvbuf.at[0, pl.ds(0, 2 * seq)]
        pltpu.make_async_copy(both, both, out_sem.at[l]).wait()

    def attend():
        score_scale = head_dim ** -0.5
        allowed = lax.broadcasted_iota(jnp.int32, (seq, seq), 0) >= lax.broadcasted_iota(jnp.int32, (seq, seq), 1)

        def body(start):
            at = pl.ds(start, seq)
            key, val = kvbuf[0, at, :], kvbuf[1, at, :]
            for n in range(heads):
                query = qbuf[at, n * head_dim:(n + 1) * head_dim]
                scores = lax.dot_general(query, key, (((1,), (1,)), ((), ())), preferred_element_type=F32) * score_scale
                scores = jnp.where(allowed, scores, -jnp.inf)
                weights = jnp.exp(scores - jnp.max(scores, axis=-1, keepdims=True))
                probs = (weights / jnp.sum(weights, axis=-1, keepdims=True)).astype(BF)
                obuf[at, n * head_dim:(n + 1) * head_dim] = jnp.dot(probs, val, preferred_element_type=F32).astype(BF)
        tiles(body, n_prompts, seq)

    def gate_up(l, j):
        def body(start):
            at = pl.ds(start, tile)
            acc = jnp.dot(hbuf[at, :], bgu[l, j], preferred_element_type=F32).astype(BF).astype(F32)
            mbuf[at, j * g_cols:(j + 1) * g_cols] = (jax.nn.silu(acc[:, :g_cols]) * acc[:, g_cols:]).astype(BF)
        tiles(body)

    chips = [x, xl, xr, xo]
    half_w = width

    def chunk(b, hh):
        return b * HALVES + hh

    def project_out(l, b, hh):
        k = chunk(b, hh)

        def body(start):
            at = pl.ds(start, tile)
            part[k, at, :] = (jnp.dot(obuf[at, :], bo[l, hh, chips[b]], preferred_element_type=F32)
                              + jnp.dot(mbuf[at, :], bd[l, hh, chips[b]], preferred_element_type=F32))

        def step(i, carry):
            body(pl.multiple_of(((i + 2) % 4) * tile, tile))

            @pl.when(i == 1)
            def _():
                remote(part.at[k, pl.ds(keep, keep)], rs0.at[k], r_send.at[0], r_recv.at[k, 0], sibling).start()
            return carry
        lax.fori_loop(0, 4, step, 0)

    def of_chip(k, yy):
        return part.at[k, pl.ds(pl.multiple_of(yy * seq, seq), seq)]

    def of_chip_half(k, yy, side):
        return part.at[k, pl.ds(pl.multiple_of(yy * seq, seq), seq), pl.ds(side * half_w, half_w)]

    def reduce_cores(b, hh):
        k = chunk(b, hh)
        wait_in(rs0.at[k], r_recv.at[k, 0], r_send.at[0])
        part[k, 0:keep, :] += rs0[k]
        remote(of_chip_half(k, yo, 0), rs1.at[k, 0], r_send.at[1], r_recv.at[k, 1], right_y).start()
        remote(of_chip_half(k, yo, 1), rs1.at[k, 1], r_send.at[1], r_recv.at[k, 2], left_y).start()

    def reduce_far(b, hh):
        k = chunk(b, hh)
        for side, target, peer in ((0, yr, right_y), (1, yl, left_y)):
            wait_in(rs1.at[k, side], r_recv.at[k, 1 + side], r_send.at[1])
            at = pl.ds(pl.multiple_of(target * seq, seq), seq)
            part[k, at, side * half_w:(side + 1) * half_w] += rs1[k, side]
            remote(of_chip(k, target), rs2.at[k, side], r_send.at[2], r_recv.at[k, 3], peer).start()

    def out_copy(i):
        return pltpu.make_async_copy(resid.at[i], y_out.at[0, :, pl.ds(pl.multiple_of(i * width, width), width)],
                                     out_sem.at[layers])

    def reduce_last(l, b, hh):
        k = chunk(b, hh)
        wait_in(rs2.at[k], r_recv.at[k, 3], r_send.at[2])
        own = pl.ds(pl.multiple_of(y * seq, seq), seq)
        total = part[k, own, :] + rs2[k, 0] + rs2[k, 1]
        for core in range(CORES):
            i = (chips[b] * CORES + core) * HALVES + hh
            resid[i] = (resid[i].astype(F32) + total[:, core * width:(core + 1) * width]).astype(BF)
            if l == layers - 1:
                out_copy(i).start()

    def reduce_drain():
        for n, ref in enumerate((rs0, rs1, rs2)):
            wait_out(ref, r_recv.at[0, 0], r_send.at[n])

    issue_own(0, 0)
    for l in range(layers):
        prepare_kv(l)
    prepare(1)
    issue_own(0, 1)
    issue_own(1)
    prepare(2)
    pltpu.make_async_copy(resid, resid, raw_sem.at[2]).wait()
    norm_own(0)
    gather_send(0)
    comm(0)
    gather_forward(0)
    gather_share(0)
    gather_finish(0)
    OWN, LEFT, RIGHT, FAR = range(4)
    rest = (OWN_CHIP, SIDES, FAR_CHIP)
    for l in range(layers):
        base = l * per_layer
        last = l == layers - 1

        def ahead(p):
            while done[0] <= p:
                comm(done[0])

        ahead(base + 1)
        wait_piece(base, rest)
        kvw_send_own(l)
        project_q(l)
        ahead(base + 2)
        kvw_forward(l)
        wait_piece(base + 1, rest)
        gate_up(l, 0)
        kvw_finish(l)
        project_kv(l)
        kv_exchange(l)
        for j in range(1, GU_CHUNKS):
            ahead(base + 1 + j if last and j == GU_CHUNKS - 1 else base + 2 + j)
            wait_piece(base + 1 + j, rest)
            gate_up(l, j)
            if j == 1:
                kv_finish(l)
                attend()
        gather_drain(l)
        kv_drain(l)
        c0, c1 = base + 1 + GU_CHUNKS, base + 2 + GU_CHUNKS
        wait_piece(c0, (OWN_CHIP,))
        project_out(l, OWN, 0)
        wait_piece(c1, (OWN_CHIP,))
        project_out(l, OWN, 1)
        reduce_cores(OWN, 0)
        reduce_cores(OWN, 1)
        reduce_far(OWN, 0)
        ahead(c0)
        wait_piece(c0, (SIDES,))
        project_out(l, LEFT, 0)
        reduce_far(OWN, 1)
        project_out(l, RIGHT, 0)
        reduce_cores(LEFT, 0)
        reduce_cores(RIGHT, 0)
        reduce_last(l, OWN, 0)
        reduce_far(LEFT, 0)
        comm(c1)
        wait_piece(c1, (SIDES,))
        project_out(l, LEFT, 1)
        reduce_far(RIGHT, 0)
        reduce_last(l, OWN, 1)
        project_out(l, RIGHT, 1)
        reduce_cores(LEFT, 1)
        reduce_cores(RIGHT, 1)
        wait_piece(c0, (FAR_CHIP,))
        project_out(l, FAR, 0)
        reduce_last(l, LEFT, 0)
        reduce_far(LEFT, 1)
        reduce_far(RIGHT, 1)
        reduce_cores(FAR, 0)
        if not last:
            comm(c1 + 1)
        reduce_far(FAR, 0)
        wait_piece(c1, (FAR_CHIP,))
        project_out(l, FAR, 1)
        reduce_last(l, RIGHT, 0)
        reduce_cores(FAR, 1)
        reduce_last(l, LEFT, 1)
        reduce_last(l, RIGHT, 1)
        reduce_far(FAR, 1)
        reduce_last(l, FAR, 0)
        reduce_last(l, FAR, 1)
        reduce_drain()
        if not last:
            norm_own(l + 1)
            comm(c1 + 2)
            gather_send(l + 1)
            gather_forward(l + 1)
            gather_share(l + 1)
            gather_finish(l + 1)
    drain_weights()
    pltpu.make_async_copy(resid, resid, out_sem.at[layers]).wait()


def take_over(*refs):
    sources, targets, held, sems = refs[:3], refs[3:6], refs[6:9], refs[9]
    loads = [pltpu.make_async_copy(sources[n], held[n], sems.at[0, n]) for n in range(3)]
    stores = [pltpu.make_async_copy(held[n], targets[n], sems.at[1, n]) for n in range(3)]
    for load in loads:
        load.start()
    for n in (1, 2, 0):
        loads[n].wait()
        stores[n].start()
    for store in stores:
        store.wait()


def run_layers(mesh_sizes, x_tokens, gamma_ln, w_q, w_kv, w_gu, w_o, w_d):
    n_x, n_y = mesh_sizes['wx'] // CORES, mesh_sizes['wy']
    assert n_x == 4 and n_y == 4 and x_tokens.shape[0] == 1
    layers, rows, q_loc = w_q.shape
    seq, d_model = x_tokens.shape[1:]
    head_dim = w_kv.shape[-1]
    hid_loc = w_gu.shape[-1]
    hid = hid_loc // CORES
    g_cols = hid // GU_CHUNKS
    q_cols = q_loc // CORES
    width = rows // HALVES
    toks = CORES * n_y * seq
    n_chunks = n_x * HALVES
    n_res = d_model // width
    cos_all, sin_all = rope_tables(seq, head_dim)
    blocks = layers * (2 + GU_CHUNKS + 2 * HALVES)
    dma = pltpu.SemaphoreType.DMA
    in_vmem, anywhere = pl.BlockSpec(memory_space=pltpu.VMEM), pl.BlockSpec(memory_space=pl.ANY)
    cache = jax.ShapeDtypeStruct((layers, 1, seq, head_dim), BF)
    results = pl.pallas_call(
        functools.partial(layers_kernel, (layers, n_x, n_y, seq, head_dim, rows, width)),
        out_shape=(jax.ShapeDtypeStruct(x_tokens.shape, BF), cache, cache),
        in_specs=[in_vmem] * 3 + [anywhere] * 6,
        out_specs=(anywhere,) * 3,
        scratch_shapes=[
            pltpu.VMEM((layers, d_model, q_cols), BF),
            pltpu.VMEM((layers, n_x * CORES, n_y, rows // n_y, head_dim), BF),
            pltpu.VMEM((layers, GU_CHUNKS, d_model, 2 * g_cols), BF),
            pltpu.VMEM((layers, HALVES, n_x, q_cols, CORES * width), BF),
            pltpu.VMEM((layers, HALVES, n_x, hid, CORES * width), BF),
            pltpu.VMEM((toks, d_model), BF),
            pltpu.VMEM((toks, q_cols), BF),
            pltpu.VMEM((2, toks, head_dim), BF),
            pltpu.VMEM((toks, q_cols), BF),
            pltpu.VMEM((toks, hid), BF),
            pltpu.VMEM((n_chunks, toks, CORES * width), F32),
            pltpu.VMEM((n_chunks, toks // CORES, CORES * width), F32),
            pltpu.VMEM((n_chunks, 2, seq, width), F32),
            pltpu.VMEM((n_chunks, 2, seq, CORES * width), F32),
            pltpu.VMEM((n_res, seq, width), BF),
            pltpu.VMEM((2, CORES, rows, 2, g_cols), BF),
            pltpu.VMEM((layers, rows // n_y, 2, head_dim), BF),
            pltpu.VMEM((layers, GU_CHUNKS, CORES, rows, 2 * g_cols), BF),
            pltpu.VMEM((layers, 2, rows // n_y, head_dim), BF),
            dma((3 + layers,)),
            dma((5,)), dma((blocks, 5)),
            dma((layers,)), dma((layers, 4)),
            dma((layers,)), dma((layers, 5)),
            dma((layers,)), dma((layers,)),
            dma((3,)), dma((n_chunks, 4)),
            dma((layers + 1,)),
        ],
        compiler_params=pltpu.CompilerParams(collective_id=0, has_side_effects=True, vmem_limit_bytes=67043328),
    )(gamma_ln, cos_all, sin_all, x_tokens, w_q, w_kv, w_gu, w_o, w_d)
    shapes = [jax.ShapeDtypeStruct(r.shape, r.dtype) for r in results]
    return pl.pallas_call(
        take_over, out_shape=shapes, in_specs=[anywhere] * 3, out_specs=[anywhere] * 3,
        scratch_shapes=[pltpu.VMEM(r.shape, r.dtype) for r in results] + [dma((2, 3))],
    )(*results)


def solution(mesh):
    batch_axes = ('dp', 'wy', 'wx')
    in_specs = (P(batch_axes), P(), P(None, 'wx', 'wy'), P(None, 'wx'), P(None, 'wx', None, 'wy'), P(None, 'wy', 'wx'), P(None, 'wy', 'wx'))
    out_specs = (P(batch_axes), P(None, batch_axes), P(None, batch_axes))
    sizes = dict(mesh.shape)
    return jax.shard_map(functools.partial(run_layers, sizes), mesh=mesh, in_specs=in_specs, out_specs=out_specs, check_vma=False)
```

```python
import functools

import jax
import jax.numpy as jnp
import numpy as np
from jax import lax
from jax.experimental import pallas as pl
from jax.experimental.pallas import tpu as pltpu
from jax.sharding import PartitionSpec as P

LN_EPS = 1e-6
ROPE_BASE = 10000.0
CORES = 2
GU_CHUNKS = 4
HALVES = 2
BF, F32 = jnp.bfloat16, jnp.float32

L0, R1, SIDES, OWN_CHIP, FAR_CHIP = range(5)
A_L, A_R, A_TOP, A_BOT, A_SIB = range(5)


def rope_tables(seq_len, head_dim):
    inv_freq = np.float32(ROPE_BASE) ** (-2.0 * np.arange(head_dim // 2, dtype=np.float32) / head_dim).astype(np.float32)
    angles = np.arange(seq_len, dtype=np.float32)[:, None] * inv_freq[None, :]
    cos_tab, sin_tab = np.cos(angles.astype(np.float64)), np.sin(angles.astype(np.float64))
    return (np.concatenate([cos_tab, cos_tab], axis=-1).astype(np.float32),
            np.concatenate([-sin_tab, sin_tab], axis=-1).astype(np.float32))


def scoped(fn):
    @functools.wraps(fn)
    def inner(*args):
        def text(a):
            return ''.join(str(v) for v in a) if isinstance(a, tuple) else str(a)
        with jax.named_scope(fn.__name__ + '_' + '_'.join(text(a) for a in args)):
            return fn(*args)
    return inner


def layers_kernel(dims, gamma_ref, cos_ref, sin_ref, x_ref, wq, wkv, wgu, wo, wd,
                  y_out, k_out, v_out,
                  bq, bkv, bgu, bo, bd, hbuf, qbuf, kvbuf, obuf, mbuf, part, rs0, rs1, rs2, resid,
                  gu_raw, kv_raw, gu_stage, kv_stage, raw_sem,
                  w_send, w_recv, kvw_send, kvw_recv, a_send, a_recv, kv_send, kv_recv, r_send, r_recv, out_sem):
    layers, n_x, n_y, seq, head_dim, rows, width = dims
    heads = wo.shape[1] // CORES // head_dim
    hid = wd.shape[1] // CORES
    o_rows = wo.shape[1] // CORES
    q_cols = heads * head_dim
    g_cols = hid // GU_CHUNKS
    n_prompts = CORES * n_y
    toks = n_prompts * seq
    keep = n_y * seq
    tile = toks // 4

    wx = lax.axis_index('wx')
    y = lax.axis_index('wy')
    x, c = wx // CORES, wx % CORES
    xr, xl, xo = (x + 1) % n_x, (x + n_x - 1) % n_x, (x + 2) % n_x
    yr, yl, yo = (y + 1) % n_y, (y + n_y - 1) % n_y, (y + 2) % n_y
    sibling = {'wx': x * CORES + 1 - c}
    right_y, left_y = {'wy': yr}, {'wy': yl}

    def at_x(chip, core):
        return {'wx': chip * CORES + core}

    n_gu = layers * GU_CHUNKS
    kv_rows = rows // n_y

    def gu_load(g, core):
        cols = pl.ds(core * hid + (g % GU_CHUNKS) * g_cols, g_cols)
        return pltpu.make_async_copy(wgu.at[g // GU_CHUNKS, :, :, cols], gu_raw.at[g % 2, core], raw_sem.at[g % 2])

    def kv_load(l):
        mine = pl.ds(pl.multiple_of(y * kv_rows, kv_rows), kv_rows)
        return pltpu.make_async_copy(wkv.at[l, mine], kv_raw.at[l], raw_sem.at[3 + l])

    def x_load(i):
        return pltpu.make_async_copy(x_ref.at[0, :, pl.ds(i * width, width)], resid.at[i], raw_sem.at[2])

    kv_load(0).start()
    for g in range(2):
        for core in range(CORES):
            gu_load(g, core).start()
    for i in range(resid.shape[0]):
        x_load(i).start()
    for l in range(1, layers):
        kv_load(l).start()

    barrier = pltpu.get_barrier_semaphore()
    peers = [sibling, right_y, left_y] + [at_x(chip, core) for chip in (xr, xl) for core in range(CORES)]
    for peer in peers:
        pl.semaphore_signal(barrier, inc=1, device_id=peer, device_id_type=pl.DeviceIdType.MESH)
    with jax.named_scope('barrier'):
        pl.semaphore_wait(barrier, len(peers))

    def remote(src, dst, send_sem, recv_sem, peer):
        return pltpu.make_async_remote_copy(src_ref=src, dst_ref=dst, send_sem=send_sem, recv_sem=recv_sem,
                                            device_id=peer, device_id_type=pl.DeviceIdType.MESH)

    def wait_in(ref, recv_sem, send_sem):
        remote(ref, ref, send_sem, recv_sem, sibling).wait_recv()

    def wait_out(ref, recv_sem, send_sem):
        remote(ref, ref, send_sem, recv_sem, sibling).wait_send()

    order = ('q', 'kv', 'gu', 'o', 'd')
    pieces = []
    n_blocks = 0
    for l in range(layers):
        pieces.append([('q', l, 0, n_blocks), ('kv', l, 0, n_blocks + 1)])
        n_blocks += 2
        for j in range(GU_CHUNKS):
            pieces.append([('gu', l, j, n_blocks)])
            n_blocks += 1
        for hh in range(HALVES):
            pieces.append([('o', l, hh, n_blocks), ('d', l, hh, n_blocks + 1)])
            n_blocks += 2
    per_layer = len(pieces) // layers
    issue_after = [[p + 2] for p in range(len(pieces))]
    tail = len(pieces) - HALVES
    issue_after[tail - 2] = []
    issue_after[tail - 1] = [tail + hh for hh in range(HALVES)]
    issue_after[tail:] = [[] for _ in range(HALVES)]

    def source(block, core):
        kind, l, j, _ = block
        if kind == 'q':
            return wq.at[l, :, pl.ds(pl.multiple_of(core * q_cols, q_cols), q_cols)]
        if kind == 'kv':
            return kv_stage.at[l, core]
        if kind == 'gu':
            return gu_stage.at[l, j, core]
        if kind == 'o':
            return wo.at[l, pl.ds(pl.multiple_of(core * o_rows, o_rows), o_rows), pl.ds(j * width, width)]
        return wd.at[l, pl.ds(pl.multiple_of(core * hid, hid), hid), pl.ds(j * width, width)]

    def landing(block, chip, core):
        kind, l, j, _ = block
        row = pl.ds(pl.multiple_of((chip * CORES + core) * rows, rows), rows)
        col = pl.ds(pl.multiple_of(core * width, width), width)
        if kind == 'q':
            return bq.at[l, row]
        if kind == 'kv':
            return bkv.at[l, chip * CORES + core, y]
        if kind == 'gu':
            return bgu.at[l, j, row]
        if kind == 'o':
            return bo.at[l, j, chip, :, col]
        return bd.at[l, j, chip, :, col]

    def prepare_kv(l):
        kv_load(l).wait()
        for core in range(CORES):
            kv_stage[l, core] = kv_raw[l, :, core, :]

    @scoped
    def prepare(p):
        if p >= len(pieces) or pieces[p][0][0] != 'gu':
            return
        _, l, j, _ = pieces[p][0]
        g = l * GU_CHUNKS + j
        step_rows = rows // 4
        pltpu.make_async_copy(gu_raw.at[g % 2], gu_raw.at[g % 2], raw_sem.at[g % 2]).wait()
        for core in range(CORES):
            def step(i, carry):
                at = pl.ds(pl.multiple_of(i * step_rows, step_rows), step_rows)
                for which in range(2):
                    gu_stage[l, j, core, at, which * g_cols:(which + 1) * g_cols] = gu_raw[g % 2, core, at, which, :]
                return carry
            lax.fori_loop(0, 4, step, 0)
            if g + 2 < n_gu:
                gu_load(g + 2, core).start()

    @scoped
    def issue_own(p, only=None):
        if p >= len(pieces):
            return
        for block in pieces[p] if only is None else [pieces[p][only]]:
            t = block[3]
            here = landing(block, x, c)
            sent = w_send.at[order.index(block[0])]
            side = [SIDES * c, SIDES - c]
            for core in range(CORES):
                remote(source(block, core), here, sent, w_recv.at[t, side[0]], at_x(xr, core)).start()
                remote(source(block, core), here, sent, w_recv.at[t, side[1]], at_x(xl, core)).start()
            remote(source(block, 1 - c), here, sent, w_recv.at[t, OWN_CHIP], sibling).start()
            pltpu.make_async_copy(source(block, c), here, w_recv.at[t, OWN_CHIP]).start()

    def pair(block, chip):
        kind, l, j, _ = block
        row = pl.ds(pl.multiple_of(chip * CORES * rows, CORES * rows), CORES * rows)
        if kind == 'q':
            return bq.at[l, row]
        if kind == 'kv':
            return bkv.at[l, pl.ds(chip * CORES, CORES), y]
        if kind == 'gu':
            return bgu.at[l, j, row]
        return (bo if kind == 'o' else bd).at[l, j, chip]

    def wait_block(block, how):
        ref = {L0: lambda: landing(block, xl, 0), R1: lambda: landing(block, xr, 1), SIDES: lambda: pair(block, xl),
               OWN_CHIP: lambda: pair(block, x), FAR_CHIP: lambda: pair(block, xo)}[how]()
        wait_in(ref, w_recv.at[block[3], how], w_send.at[0])

    done = [0]

    @scoped
    def comm(p):
        if p >= len(pieces):
            return
        assert p == done[0]
        done[0] = p + 1
        for block in pieces[p]:
            t = block[3]
            wait_block(block, L0)
            from_left = landing(block, xl, 0)
            remote(from_left, from_left, w_send.at[order.index(block[0])], w_recv.at[t, FAR_CHIP], at_x(xr, c)).start()
            wait_block(block, R1)
            from_right = landing(block, xr, 1)
            remote(from_right, from_right, w_send.at[order.index(block[0])], w_recv.at[t, FAR_CHIP], at_x(xl, c)).start()
        for later in issue_after[p]:
            issue_own(later)
        prepare(p + 3)

    @scoped
    def wait_piece(p, hows):
        for block in pieces[p]:
            for how in hows:
                wait_block(block, how)

    @scoped
    def drain_weights():
        sources = n_x * CORES
        for n, ref in enumerate((bq.at[:, pl.ds(0, (sources - 1) * rows)], bkv.at[:, pl.ds(0, sources - 1), 0],
                                 bgu.at[:, :, pl.ds(0, (sources - 1) * rows)],
                                 bo.at[:, :, :, pl.ds(0, o_rows // sources * (sources - 1))],
                                 bd.at[:, :, :, pl.ds(0, hid // sources * (sources - 1))])):
            wait_out(ref, w_recv.at[0, 0], w_send.at[n])

    def kv_quarter(l, yy, half=None):
        n_src = n_x * CORES
        return bkv.at[l, pl.ds(0 if half is None else half * (n_src // 2), n_src if half is None else n_src // 2), yy]

    def kvw_copy(l, ref, kind, peer):
        remote(ref, ref, kvw_send.at[l], kvw_recv.at[l, kind], peer).start()

    @scoped
    def kvw_send_own(l):
        kvw_copy(l, kv_quarter(l, y), A_L, right_y)
        kvw_copy(l, kv_quarter(l, y), A_R, left_y)

    @scoped
    def kvw_forward(l):
        wait_in(kv_quarter(l, yl), kvw_recv.at[l, A_L], kvw_send.at[l])
        kvw_copy(l, kv_quarter(l, yl, 0), A_TOP, right_y)
        wait_in(kv_quarter(l, yr), kvw_recv.at[l, A_R], kvw_send.at[l])
        kvw_copy(l, kv_quarter(l, yr, 1), A_BOT, left_y)

    @scoped
    def kvw_finish(l):
        wait_in(kv_quarter(l, yo, 0), kvw_recv.at[l, A_TOP], kvw_send.at[l])
        wait_in(kv_quarter(l, yo, 1), kvw_recv.at[l, A_BOT], kvw_send.at[l])
        wait_out(bkv.at[l, :, pl.ds(0, n_y - 1)], kvw_recv.at[l, A_L], kvw_send.at[l])

    def prompt(slot, part_of=None):
        if part_of is None:
            return hbuf.at[pl.ds(pl.multiple_of(slot * seq, seq), seq)]
        half = seq // 2
        return hbuf.at[pl.ds(pl.multiple_of(slot * seq + part_of * half, half), half)]

    def a_copy(l, src, dst, kind, peer):
        remote(src, dst, a_send.at[l], a_recv.at[l, kind], peer).start()

    def a_wait(l, ref, kind):
        wait_in(ref, a_recv.at[l, kind], a_send.at[l])

    @scoped
    def gather_send(l):
        a_copy(l, prompt(y), prompt(y), A_L, right_y)
        a_copy(l, prompt(y), prompt(y), A_R, left_y)
        a_copy(l, prompt(y), prompt(n_y + y), A_SIB, sibling)

    @scoped
    def gather_forward(l):
        a_wait(l, prompt(yl), A_L)
        a_copy(l, prompt(yl, 0), prompt(yl, 0), A_TOP, right_y)
        a_copy(l, prompt(yl), prompt(n_y + yl), A_SIB, sibling)
        a_wait(l, prompt(yr), A_R)
        a_copy(l, prompt(yr, 1), prompt(yr, 1), A_BOT, left_y)
        a_copy(l, prompt(yr), prompt(n_y + yr), A_SIB, sibling)

    @scoped
    def gather_share(l):
        a_wait(l, prompt(yo, 0), A_TOP)
        a_copy(l, prompt(yo, 0), prompt(n_y + yo, 0), A_SIB, sibling)
        a_wait(l, prompt(yo, 1), A_BOT)
        a_copy(l, prompt(yo, 1), prompt(n_y + yo, 1), A_SIB, sibling)

    @scoped
    def gather_finish(l):
        a_wait(l, hbuf.at[pl.ds(keep, keep)], A_SIB)

    @scoped
    def gather_drain(l):
        wait_out(hbuf.at[pl.ds(0, 7 * seq)], a_recv.at[l, A_L], a_send.at[l])

    n_res = resid.shape[0]
    d_model = n_res * width

    @scoped
    def norm_own(l):
        total = jnp.zeros((seq, 1), F32)
        for i in range(n_res):
            total += jnp.sum(resid[i].astype(F32), axis=-1, keepdims=True)
        mean = total / d_model
        square = jnp.zeros((seq, 1), F32)
        for i in range(n_res):
            centered = resid[i].astype(F32) - mean
            square += jnp.sum(centered * centered, axis=-1, keepdims=True)
        scale = lax.rsqrt(square / d_model + LN_EPS)
        own = pl.ds(pl.multiple_of(y * seq, seq), seq)
        for i in range(n_res):
            value = (resid[i].astype(F32) - mean) * scale * gamma_ref[l:l + 1, i * width:(i + 1) * width]
            hbuf[own, i * width:(i + 1) * width] = value.astype(BF)

    def rotate(value):
        value = value.astype(F32)
        cos_all = jnp.concatenate([cos_ref[...]] * (tile // seq), axis=0)
        sin_all = jnp.concatenate([sin_ref[...]] * (tile // seq), axis=0)
        return (value * cos_all + pltpu.roll(value, head_dim // 2, 1) * sin_all).astype(BF)

    def tiles(body, n=4, size=tile):
        def step(i, carry):
            body(pl.multiple_of(i * size, size))
            return carry
        lax.fori_loop(0, n, step, 0)

    @scoped
    def project_q(l):
        def body(start):
            at = pl.ds(start, tile)
            acc = jnp.dot(hbuf[at, :], bq[l], preferred_element_type=F32).astype(BF)
            for n in range(heads):
                qbuf[at, n * head_dim:(n + 1) * head_dim] = rotate(acc[:, n * head_dim:(n + 1) * head_dim])
        tiles(body)

    @scoped
    def project_kv(l):
        def body(start):
            at = pl.ds(start, tile)
            weights = bkv[l].reshape(d_model, head_dim)
            kv = jnp.dot(hbuf[at, :], weights, preferred_element_type=F32).astype(BF)
            kvbuf[c, at, :] = jnp.where(c == 0, rotate(kv), kv)
        tiles(body)

    def kv_refs(lo):
        return kvbuf.at[c, pl.ds(lo * keep, keep)]

    @scoped
    def kv_exchange(l):
        for lo in range(2):
            remote(kv_refs(lo), kv_refs(1 - lo), kv_send.at[l], kv_recv.at[l], sibling).start()

    def kv_outs(l):
        own = pl.ds(pl.multiple_of(y * seq, seq), seq)
        return [pltpu.make_async_copy(kvbuf.at[0, own], k_out.at[l, 0], out_sem.at[l]),
                pltpu.make_async_copy(kvbuf.at[1, own], v_out.at[l, 0], out_sem.at[l])]

    @scoped
    def kv_finish(l):
        wait_in(kvbuf.at[1 - c], kv_recv.at[l], kv_send.at[l])
        for copy in kv_outs(l):
            copy.start()

    @scoped
    def kv_drain(l):
        wait_out(kvbuf.at[c], kv_recv.at[l], kv_send.at[l])
        both = kvbuf.at[0, pl.ds(0, 2 * seq)]
        pltpu.make_async_copy(both, both, out_sem.at[l]).wait()

    @scoped
    def attend():
        score_scale = head_dim ** -0.5
        allowed = lax.broadcasted_iota(jnp.int32, (seq, seq), 0) >= lax.broadcasted_iota(jnp.int32, (seq, seq), 1)

        def body(start):
            at = pl.ds(start, seq)
            key, val = kvbuf[0, at, :], kvbuf[1, at, :]
            for n in range(heads):
                query = qbuf[at, n * head_dim:(n + 1) * head_dim]
                scores = lax.dot_general(query, key, (((1,), (1,)), ((), ())), preferred_element_type=F32) * score_scale
                scores = jnp.where(allowed, scores, -jnp.inf)
                weights = jnp.exp(scores - jnp.max(scores, axis=-1, keepdims=True))
                probs = (weights / jnp.sum(weights, axis=-1, keepdims=True)).astype(BF)
                obuf[at, n * head_dim:(n + 1) * head_dim] = jnp.dot(probs, val, preferred_element_type=F32).astype(BF)
        tiles(body, n_prompts, seq)

    @scoped
    def gate_up(l, j):
        def body(start):
            at = pl.ds(start, tile)
            acc = jnp.dot(hbuf[at, :], bgu[l, j], preferred_element_type=F32).astype(BF).astype(F32)
            mbuf[at, j * g_cols:(j + 1) * g_cols] = (jax.nn.silu(acc[:, :g_cols]) * acc[:, g_cols:]).astype(BF)
        tiles(body)

    chips = [x, xl, xr, xo]
    half_w = width

    def chunk(b, hh):
        return b * HALVES + hh

    @scoped
    def project_out(l, b, hh):
        k = chunk(b, hh)

        def body(start):
            at = pl.ds(start, tile)
            part[k, at, :] = (jnp.dot(obuf[at, :], bo[l, hh, chips[b]], preferred_element_type=F32)
                              + jnp.dot(mbuf[at, :], bd[l, hh, chips[b]], preferred_element_type=F32))

        def step(i, carry):
            body(pl.multiple_of(((i + 2) % 4) * tile, tile))

            @pl.when(i == 1)
            def _():
                remote(part.at[k, pl.ds(keep, keep)], rs0.at[k], r_send.at[0], r_recv.at[k, 0], sibling).start()
            return carry
        lax.fori_loop(0, 4, step, 0)

    def of_chip(k, yy):
        return part.at[k, pl.ds(pl.multiple_of(yy * seq, seq), seq)]

    def of_chip_half(k, yy, side):
        return part.at[k, pl.ds(pl.multiple_of(yy * seq, seq), seq), pl.ds(side * half_w, half_w)]

    @scoped
    def reduce_cores(b, hh):
        k = chunk(b, hh)
        wait_in(rs0.at[k], r_recv.at[k, 0], r_send.at[0])
        part[k, 0:keep, :] += rs0[k]
        remote(of_chip_half(k, yo, 0), rs1.at[k, 0], r_send.at[1], r_recv.at[k, 1], right_y).start()
        remote(of_chip_half(k, yo, 1), rs1.at[k, 1], r_send.at[1], r_recv.at[k, 2], left_y).start()

    @scoped
    def reduce_far(b, hh):
        k = chunk(b, hh)
        for side, target, peer in ((0, yr, right_y), (1, yl, left_y)):
            wait_in(rs1.at[k, side], r_recv.at[k, 1 + side], r_send.at[1])
            at = pl.ds(pl.multiple_of(target * seq, seq), seq)
            part[k, at, side * half_w:(side + 1) * half_w] += rs1[k, side]
            remote(of_chip(k, target), rs2.at[k, side], r_send.at[2], r_recv.at[k, 3], peer).start()

    def out_copy(i):
        return pltpu.make_async_copy(resid.at[i], y_out.at[0, :, pl.ds(pl.multiple_of(i * width, width), width)],
                                     out_sem.at[layers])

    @scoped
    def reduce_last(l, b, hh):
        k = chunk(b, hh)
        wait_in(rs2.at[k], r_recv.at[k, 3], r_send.at[2])
        own = pl.ds(pl.multiple_of(y * seq, seq), seq)
        total = part[k, own, :] + rs2[k, 0] + rs2[k, 1]
        for core in range(CORES):
            i = (chips[b] * CORES + core) * HALVES + hh
            resid[i] = (resid[i].astype(F32) + total[:, core * width:(core + 1) * width]).astype(BF)
            if l == layers - 1:
                out_copy(i).start()

    @scoped
    def reduce_drain():
        for n, ref in enumerate((rs0, rs1, rs2)):
            wait_out(ref, r_recv.at[0, 0], r_send.at[n])

    issue_own(0, 0)
    for l in range(layers):
        prepare_kv(l)
    prepare(1)
    issue_own(0, 1)
    issue_own(1)
    prepare(2)
    pltpu.make_async_copy(resid, resid, raw_sem.at[2]).wait()
    norm_own(0)
    gather_send(0)
    comm(0)
    gather_forward(0)
    gather_share(0)
    gather_finish(0)
    OWN, LEFT, RIGHT, FAR = range(4)
    rest = (OWN_CHIP, SIDES, FAR_CHIP)
    for l in range(layers):
        base = l * per_layer
        last = l == layers - 1

        def ahead(p):
            while done[0] <= p:
                comm(done[0])

        ahead(base + 1)
        if l == 0:
            wait_piece(base, rest)
            kvw_send_own(l)
        project_q(l)
        ahead(base + 2)
        if l == 0:
            kvw_forward(l)
        wait_piece(base + 1, rest)
        gate_up(l, 0)
        kvw_finish(l)
        project_kv(l)
        kv_exchange(l)
        for j in range(1, GU_CHUNKS):
            ahead(base + 1 + j if last and j == GU_CHUNKS - 1 else base + 2 + j)
            wait_piece(base + 1 + j, rest)
            gate_up(l, j)
            if j == 1:
                kv_finish(l)
                attend()
        gather_drain(l)
        kv_drain(l)
        c0, c1 = base + 1 + GU_CHUNKS, base + 2 + GU_CHUNKS
        wait_piece(c0, (OWN_CHIP,))
        project_out(l, OWN, 0)
        wait_piece(c1, (OWN_CHIP,))
        project_out(l, OWN, 1)
        reduce_cores(OWN, 0)
        reduce_cores(OWN, 1)
        reduce_far(OWN, 0)
        ahead(c0)
        wait_piece(c0, (SIDES,))
        project_out(l, LEFT, 0)
        reduce_far(OWN, 1)
        project_out(l, RIGHT, 0)
        reduce_cores(LEFT, 0)
        reduce_cores(RIGHT, 0)
        reduce_last(l, OWN, 0)
        reduce_far(LEFT, 0)
        comm(c1)
        wait_piece(c1, (SIDES,))
        project_out(l, LEFT, 1)
        reduce_far(RIGHT, 0)
        reduce_last(l, OWN, 1)
        project_out(l, RIGHT, 1)
        reduce_cores(LEFT, 1)
        reduce_cores(RIGHT, 1)
        wait_piece(c0, (FAR_CHIP,))
        project_out(l, FAR, 0)
        reduce_last(l, LEFT, 0)
        reduce_far(LEFT, 1)
        reduce_far(RIGHT, 1)
        reduce_cores(FAR, 0)
        if not last:
            comm(c1 + 1)
        wait_piece(c1, (FAR_CHIP,))
        project_out(l, FAR, 1)
        reduce_cores(FAR, 1)
        reduce_far(FAR, 0)
        reduce_last(l, RIGHT, 0)
        reduce_last(l, LEFT, 1)
        reduce_last(l, RIGHT, 1)
        reduce_far(FAR, 1)
        reduce_last(l, FAR, 0)
        reduce_last(l, FAR, 1)
        reduce_drain()
        if not last:
            norm_own(l + 1)
            comm(c1 + 2)
            gather_send(l + 1)
            wait_piece(base + per_layer, rest)
            kvw_send_own(l + 1)
            gather_forward(l + 1)
            gather_share(l + 1)
            kvw_forward(l + 1)
            gather_finish(l + 1)
    drain_weights()
    pltpu.make_async_copy(resid, resid, out_sem.at[layers]).wait()


def take_over(*refs):
    sources, targets, held, sems = refs[:3], refs[3:6], refs[6:9], refs[9]
    loads = [pltpu.make_async_copy(sources[n], held[n], sems.at[0, n]) for n in range(3)]
    stores = [pltpu.make_async_copy(held[n], targets[n], sems.at[1, n]) for n in range(3)]
    for load in loads:
        load.start()
    for n in (1, 2, 0):
        loads[n].wait()
        stores[n].start()
    for store in stores:
        store.wait()


def run_layers(mesh_sizes, x_tokens, gamma_ln, w_q, w_kv, w_gu, w_o, w_d):
    n_x, n_y = mesh_sizes['wx'] // CORES, mesh_sizes['wy']
    assert n_x == 4 and n_y == 4 and x_tokens.shape[0] == 1
    layers, rows, q_loc = w_q.shape
    seq, d_model = x_tokens.shape[1:]
    head_dim = w_kv.shape[-1]
    hid_loc = w_gu.shape[-1]
    hid = hid_loc // CORES
    g_cols = hid // GU_CHUNKS
    q_cols = q_loc // CORES
    width = rows // HALVES
    toks = CORES * n_y * seq
    n_chunks = n_x * HALVES
    n_res = d_model // width
    cos_all, sin_all = rope_tables(seq, head_dim)
    blocks = layers * (2 + GU_CHUNKS + 2 * HALVES)
    dma = pltpu.SemaphoreType.DMA
    in_vmem, anywhere = pl.BlockSpec(memory_space=pltpu.VMEM), pl.BlockSpec(memory_space=pl.ANY)
    cache = jax.ShapeDtypeStruct((layers, 1, seq, head_dim), BF)
    results = pl.pallas_call(
        functools.partial(layers_kernel, (layers, n_x, n_y, seq, head_dim, rows, width)),
        out_shape=(jax.ShapeDtypeStruct(x_tokens.shape, BF), cache, cache),
        in_specs=[in_vmem] * 3 + [anywhere] * 6,
        out_specs=(anywhere,) * 3,
        scratch_shapes=[
            pltpu.VMEM((layers, d_model, q_cols), BF),
            pltpu.VMEM((layers, n_x * CORES, n_y, rows // n_y, head_dim), BF),
            pltpu.VMEM((layers, GU_CHUNKS, d_model, 2 * g_cols), BF),
            pltpu.VMEM((layers, HALVES, n_x, q_cols, CORES * width), BF),
            pltpu.VMEM((layers, HALVES, n_x, hid, CORES * width), BF),
            pltpu.VMEM((toks, d_model), BF),
            pltpu.VMEM((toks, q_cols), BF),
            pltpu.VMEM((2, toks, head_dim), BF),
            pltpu.VMEM((toks, q_cols), BF),
            pltpu.VMEM((toks, hid), BF),
            pltpu.VMEM((n_chunks, toks, CORES * width), F32),
            pltpu.VMEM((n_chunks, toks // CORES, CORES * width), F32),
            pltpu.VMEM((n_chunks, 2, seq, width), F32),
            pltpu.VMEM((n_chunks, 2, seq, CORES * width), F32),
            pltpu.VMEM((n_res, seq, width), BF),
            pltpu.VMEM((2, CORES, rows, 2, g_cols), BF),
            pltpu.VMEM((layers, rows // n_y, 2, head_dim), BF),
            pltpu.VMEM((layers, GU_CHUNKS, CORES, rows, 2 * g_cols), BF),
            pltpu.VMEM((layers, 2, rows // n_y, head_dim), BF),
            dma((3 + layers,)),
            dma((5,)), dma((blocks, 5)),
            dma((layers,)), dma((layers, 4)),
            dma((layers,)), dma((layers, 5)),
            dma((layers,)), dma((layers,)),
            dma((3,)), dma((n_chunks, 4)),
            dma((layers + 1,)),
        ],
        compiler_params=pltpu.CompilerParams(collective_id=0, has_side_effects=True, vmem_limit_bytes=67043328),
    )(gamma_ln, cos_all, sin_all, x_tokens, w_q, w_kv, w_gu, w_o, w_d)
    shapes = [jax.ShapeDtypeStruct(r.shape, r.dtype) for r in results]
    return pl.pallas_call(
        take_over, out_shape=shapes, in_specs=[anywhere] * 3, out_specs=[anywhere] * 3,
        scratch_shapes=[pltpu.VMEM(r.shape, r.dtype) for r in results] + [dma((2, 3))],
    )(*results)


def solution(mesh):
    batch_axes = ('dp', 'wy', 'wx')
    in_specs = (P(batch_axes), P(), P(None, 'wx', 'wy'), P(None, 'wx'), P(None, 'wx', None, 'wy'), P(None, 'wy', 'wx'), P(None, 'wy', 'wx'))
    out_specs = (P(batch_axes), P(None, batch_axes), P(None, batch_axes))
    sizes = dict(mesh.shape)
    return jax.shard_map(functools.partial(run_layers, sizes), mesh=mesh, in_specs=in_specs, out_specs=out_specs, check_vma=False)
```

```python
import functools

import jax
import jax.numpy as jnp
import numpy as np
from jax import lax
from jax.experimental import pallas as pl
from jax.experimental.pallas import tpu as pltpu
from jax.sharding import PartitionSpec as P

LN_EPS = 1e-6
ROPE_BASE = 10000.0
CORES = 2
GU_CHUNKS = 4
HALVES = 2
BF, F32 = jnp.bfloat16, jnp.float32

L0, R1, SIDES, OWN_CHIP, FAR_CHIP = range(5)
A_L, A_R, A_TOP, A_BOT, A_SIB = range(5)


def rope_tables(seq_len, head_dim):
    inv_freq = np.float32(ROPE_BASE) ** (-2.0 * np.arange(head_dim // 2, dtype=np.float32) / head_dim).astype(np.float32)
    angles = np.arange(seq_len, dtype=np.float32)[:, None] * inv_freq[None, :]
    cos_tab, sin_tab = np.cos(angles.astype(np.float64)), np.sin(angles.astype(np.float64))
    return (np.concatenate([cos_tab, cos_tab], axis=-1).astype(np.float32),
            np.concatenate([-sin_tab, sin_tab], axis=-1).astype(np.float32))


def scoped(fn):
    @functools.wraps(fn)
    def inner(*args):
        def text(a):
            return ''.join(str(v) for v in a) if isinstance(a, tuple) else str(a)
        with jax.named_scope(fn.__name__ + '_' + '_'.join(text(a) for a in args)):
            return fn(*args)
    return inner


def layers_kernel(dims, gamma_ref, cos_ref, sin_ref, x_ref, wq, wkv, wgu, wo, wd,
                  y_out, k_out, v_out,
                  bq, bkv, bgu, bod, hbuf, qbuf, kvbuf, ombuf, part, rs0, rs1, rs2, resid,
                  gu_raw, kv_raw, gu_stage, kv_stage, raw_sem,
                  w_send, w_recv, c_recv, kvw_send, kvw_recv, a_send, a_recv, kv_send, kv_recv, r_send, r_recv, out_sem):
    layers, n_x, n_y, seq, head_dim, rows, width = dims
    heads = wo.shape[1] // CORES // head_dim
    hid = wd.shape[1] // CORES
    o_rows = wo.shape[1] // CORES
    q_cols = heads * head_dim
    g_cols = hid // GU_CHUNKS
    n_prompts = CORES * n_y
    toks = n_prompts * seq
    keep = n_y * seq
    tile = toks // 4

    wx = lax.axis_index('wx')
    y = lax.axis_index('wy')
    x, c = wx // CORES, wx % CORES
    xr, xl, xo = (x + 1) % n_x, (x + n_x - 1) % n_x, (x + 2) % n_x
    yr, yl, yo = (y + 1) % n_y, (y + n_y - 1) % n_y, (y + 2) % n_y
    sibling = {'wx': x * CORES + 1 - c}
    right_y, left_y = {'wy': yr}, {'wy': yl}

    def at_x(chip, core):
        return {'wx': chip * CORES + core}

    n_gu = layers * GU_CHUNKS
    kv_rows = rows // n_y

    def gu_load(g, core):
        cols = pl.ds(core * hid + (g % GU_CHUNKS) * g_cols, g_cols)
        return pltpu.make_async_copy(wgu.at[g // GU_CHUNKS, :, :, cols], gu_raw.at[g % 2, core], raw_sem.at[g % 2])

    def kv_load(l):
        mine = pl.ds(pl.multiple_of(y * kv_rows, kv_rows), kv_rows)
        return pltpu.make_async_copy(wkv.at[l, mine], kv_raw.at[l], raw_sem.at[3 + l])

    def x_load(i):
        return pltpu.make_async_copy(x_ref.at[0, :, pl.ds(i * width, width)], resid.at[i], raw_sem.at[2])

    kv_load(0).start()
    for g in range(2):
        for core in range(CORES):
            gu_load(g, core).start()
    for i in range(resid.shape[0]):
        x_load(i).start()
    for l in range(1, layers):
        kv_load(l).start()

    barrier = pltpu.get_barrier_semaphore()
    peers = [sibling, right_y, left_y] + [at_x(chip, core) for chip in (xr, xl) for core in range(CORES)]
    for peer in peers:
        pl.semaphore_signal(barrier, inc=1, device_id=peer, device_id_type=pl.DeviceIdType.MESH)
    with jax.named_scope('barrier'):
        pl.semaphore_wait(barrier, len(peers))

    def remote(src, dst, send_sem, recv_sem, peer):
        return pltpu.make_async_remote_copy(src_ref=src, dst_ref=dst, send_sem=send_sem, recv_sem=recv_sem,
                                            device_id=peer, device_id_type=pl.DeviceIdType.MESH)

    def wait_in(ref, recv_sem, send_sem):
        remote(ref, ref, send_sem, recv_sem, sibling).wait_recv()

    def wait_out(ref, recv_sem, send_sem):
        remote(ref, ref, send_sem, recv_sem, sibling).wait_send()

    order = ('q', 'kv', 'gu', 'od')
    pieces = []
    n_blocks = n_outs = 0
    for l in range(layers):
        pieces.append([('q', l, 0, n_blocks), ('kv', l, 0, n_blocks + 1)])
        n_blocks += 2
        for j in range(GU_CHUNKS):
            pieces.append([('gu', l, j, n_blocks)])
            n_blocks += 1
        for hh in range(HALVES):
            pieces.append([('od', l, hh, n_outs)])
            n_outs += 1
    per_layer = len(pieces) // layers
    issue_after = [[p + 2] for p in range(len(pieces))]
    tail = len(pieces) - HALVES
    issue_after[tail - 2] = []
    issue_after[tail - 1] = [tail + hh for hh in range(HALVES)]
    issue_after[tail:] = [[] for _ in range(HALVES)]

    def sources(block, core):
        kind, l, j, _ = block
        if kind == 'q':
            return [wq.at[l, :, pl.ds(pl.multiple_of(core * q_cols, q_cols), q_cols)]]
        if kind == 'kv':
            return [kv_stage.at[l, core]]
        if kind == 'gu':
            return [gu_stage.at[l, j, core]]
        cols = pl.ds(j * width, width)
        return [wo.at[l, pl.ds(pl.multiple_of(core * o_rows, o_rows), o_rows), cols],
                wd.at[l, pl.ds(pl.multiple_of(core * hid, hid), hid), cols]]

    def landing(block, chip, core):
        kind, l, j, _ = block
        if kind == 'kv':
            return bkv.at[l, chip * CORES + core, y]
        if kind == 'od':
            return bod.at[l, j, chip, :, pl.ds(pl.multiple_of(core * width, width), width)]
        row = pl.ds(pl.multiple_of((chip * CORES + core) * rows, rows), rows)
        return bq.at[l, row] if kind == 'q' else bgu.at[l, j, row]

    def landings(block):
        here = landing(block, x, c)
        return [here.at[pl.ds(0, o_rows)], here.at[pl.ds(o_rows, hid)]] if block[0] == 'od' else [here]

    def received(block, how):
        return c_recv.at[block[3], how] if block[0] == 'od' else w_recv.at[block[3], how]

    def prepare_kv(l):
        kv_load(l).wait()
        for core in range(CORES):
            kv_stage[l, core] = kv_raw[l, :, core, :]

    @scoped
    def prepare(p):
        if p >= len(pieces) or pieces[p][0][0] != 'gu':
            return
        _, l, j, _ = pieces[p][0]
        g = l * GU_CHUNKS + j
        step_rows = rows // 4
        pltpu.make_async_copy(gu_raw.at[g % 2], gu_raw.at[g % 2], raw_sem.at[g % 2]).wait()
        for core in range(CORES):
            def step(i, carry):
                at = pl.ds(pl.multiple_of(i * step_rows, step_rows), step_rows)
                for which in range(2):
                    gu_stage[l, j, core, at, which * g_cols:(which + 1) * g_cols] = gu_raw[g % 2, core, at, which, :]
                return carry
            lax.fori_loop(0, 4, step, 0)
            if g + 2 < n_gu:
                gu_load(g + 2, core).start()

    @scoped
    def issue_own(p, only=None):
        if p >= len(pieces):
            return
        for block in pieces[p] if only is None else [pieces[p][only]]:
            sent = w_send.at[order.index(block[0])]
            side = [SIDES * c, SIDES - c]
            near = OWN_CHIP if block[0] == 'od' else SIDES
            for core in range(CORES):
                for src, dst in zip(sources(block, core), landings(block)):
                    remote(src, dst, sent, received(block, side[0]), at_x(xr, core)).start()
                    remote(src, dst, sent, received(block, side[1]), at_x(xl, core)).start()
            for src, dst in zip(sources(block, 1 - c), landings(block)):
                remote(src, dst, sent, received(block, near), sibling).start()
            for src, dst in zip(sources(block, c), landings(block)):
                pltpu.make_async_copy(src, dst, received(block, near)).start()

    def wait_block(block, how):
        kind, l, j, _ = block
        if how in (L0, R1):
            ref = landing(block, xl, 0) if how == L0 else landing(block, xr, 1)
        elif kind == 'od':
            ref = bod.at[l, j, {SIDES: xl, OWN_CHIP: x, FAR_CHIP: xo}[how]]
        else:
            others = n_x * CORES - 2
            ref = bkv.at[l, pl.ds(0, others), y] if kind == 'kv' else (
                bq.at[l, pl.ds(0, others * rows)] if kind == 'q' else bgu.at[l, j, pl.ds(0, others * rows)])
        wait_in(ref, received(block, how), w_send.at[0])

    done = [0]

    @scoped
    def comm(p):
        if p >= len(pieces):
            return
        assert p == done[0]
        done[0] = p + 1
        for block in pieces[p]:
            far = FAR_CHIP if block[0] == 'od' else SIDES
            wait_block(block, L0)
            from_left = landing(block, xl, 0)
            remote(from_left, from_left, w_send.at[order.index(block[0])], received(block, far), at_x(xr, c)).start()
            wait_block(block, R1)
            from_right = landing(block, xr, 1)
            remote(from_right, from_right, w_send.at[order.index(block[0])], received(block, far), at_x(xl, c)).start()
        for later in issue_after[p]:
            issue_own(later)
        prepare(p + 3)

    @scoped
    def wait_piece(p, hows):
        for block in pieces[p]:
            for how in hows:
                wait_block(block, how)

    @scoped
    def drain_weights():
        n_src = n_x * CORES
        for n, ref in enumerate((bq.at[:, pl.ds(0, (n_src - 1) * rows)], bkv.at[:, pl.ds(0, n_src - 1), 0],
                                 bgu.at[:, :, pl.ds(0, (n_src - 1) * rows)],
                                 bod.at[:, :, :, pl.ds(0, (o_rows + hid) // n_src * (n_src - 1))])):
            wait_out(ref, w_recv.at[0, 0], w_send.at[n])

    def kv_quarter(l, yy, half=None):
        n_src = n_x * CORES
        return bkv.at[l, pl.ds(0 if half is None else half * (n_src // 2), n_src if half is None else n_src // 2), yy]

    def kvw_copy(l, ref, kind, peer):
        remote(ref, ref, kvw_send.at[l], kvw_recv.at[l, kind], peer).start()

    @scoped
    def kvw_send_own(l):
        kvw_copy(l, kv_quarter(l, y), A_L, right_y)
        kvw_copy(l, kv_quarter(l, y), A_R, left_y)

    @scoped
    def kvw_forward(l):
        wait_in(kv_quarter(l, yl), kvw_recv.at[l, A_L], kvw_send.at[l])
        kvw_copy(l, kv_quarter(l, yl, 0), A_TOP, right_y)
        wait_in(kv_quarter(l, yr), kvw_recv.at[l, A_R], kvw_send.at[l])
        kvw_copy(l, kv_quarter(l, yr, 1), A_BOT, left_y)

    @scoped
    def kvw_finish(l):
        wait_in(kv_quarter(l, yo, 0), kvw_recv.at[l, A_TOP], kvw_send.at[l])
        wait_in(kv_quarter(l, yo, 1), kvw_recv.at[l, A_BOT], kvw_send.at[l])
        wait_out(bkv.at[l, :, pl.ds(0, n_y - 1)], kvw_recv.at[l, A_L], kvw_send.at[l])

    def prompt(slot, part_of=None):
        if part_of is None:
            return hbuf.at[pl.ds(pl.multiple_of(slot * seq, seq), seq)]
        half = seq // 2
        return hbuf.at[pl.ds(pl.multiple_of(slot * seq + part_of * half, half), half)]

    def a_copy(l, src, dst, kind, peer):
        remote(src, dst, a_send.at[l], a_recv.at[l, kind], peer).start()

    def a_wait(l, ref, kind):
        wait_in(ref, a_recv.at[l, kind], a_send.at[l])

    @scoped
    def gather_send(l):
        a_copy(l, prompt(y), prompt(y), A_L, right_y)
        a_copy(l, prompt(y), prompt(y), A_R, left_y)
        a_copy(l, prompt(y), prompt(n_y + y), A_SIB, sibling)

    @scoped
    def gather_forward(l):
        a_wait(l, prompt(yl), A_L)
        a_copy(l, prompt(yl, 0), prompt(yl, 0), A_TOP, right_y)
        a_copy(l, prompt(yl), prompt(n_y + yl), A_SIB, sibling)
        a_wait(l, prompt(yr), A_R)
        a_copy(l, prompt(yr, 1), prompt(yr, 1), A_BOT, left_y)
        a_copy(l, prompt(yr), prompt(n_y + yr), A_SIB, sibling)

    @scoped
    def gather_share(l):
        a_wait(l, prompt(yo, 0), A_TOP)
        a_copy(l, prompt(yo, 0), prompt(n_y + yo, 0), A_SIB, sibling)
        a_wait(l, prompt(yo, 1), A_BOT)
        a_copy(l, prompt(yo, 1), prompt(n_y + yo, 1), A_SIB, sibling)

    @scoped
    def gather_finish(l):
        a_wait(l, hbuf.at[pl.ds(keep, keep)], A_SIB)

    @scoped
    def gather_drain(l):
        wait_out(hbuf.at[pl.ds(0, 7 * seq)], a_recv.at[l, A_L], a_send.at[l])

    n_res = resid.shape[0]
    d_model = n_res * width

    @scoped
    def norm_own(l):
        total = jnp.zeros((seq, 1), F32)
        for i in range(n_res):
            total += jnp.sum(resid[i].astype(F32), axis=-1, keepdims=True)
        mean = total / d_model
        square = jnp.zeros((seq, 1), F32)
        for i in range(n_res):
            centered = resid[i].astype(F32) - mean
            square += jnp.sum(centered * centered, axis=-1, keepdims=True)
        scale = lax.rsqrt(square / d_model + LN_EPS)
        own = pl.ds(pl.multiple_of(y * seq, seq), seq)
        for i in range(n_res):
            value = (resid[i].astype(F32) - mean) * scale * gamma_ref[l:l + 1, i * width:(i + 1) * width]
            hbuf[own, i * width:(i + 1) * width] = value.astype(BF)

    def rotate(value):
        value = value.astype(F32)
        cos_all = jnp.concatenate([cos_ref[...]] * (tile // seq), axis=0)
        sin_all = jnp.concatenate([sin_ref[...]] * (tile // seq), axis=0)
        return (value * cos_all + pltpu.roll(value, head_dim // 2, 1) * sin_all).astype(BF)

    def tiles(body, n=4, size=tile):
        def step(i, carry):
            body(pl.multiple_of(i * size, size))
            return carry
        lax.fori_loop(0, n, step, 0)

    @scoped
    def project_q(l):
        def body(start):
            at = pl.ds(start, tile)
            acc = jnp.dot(hbuf[at, :], bq[l], preferred_element_type=F32).astype(BF)
            for n in range(heads):
                qbuf[at, n * head_dim:(n + 1) * head_dim] = rotate(acc[:, n * head_dim:(n + 1) * head_dim])
        tiles(body)

    @scoped
    def project_kv(l):
        def body(start):
            at = pl.ds(start, tile)
            weights = bkv[l].reshape(d_model, head_dim)
            kv = jnp.dot(hbuf[at, :], weights, preferred_element_type=F32).astype(BF)
            kvbuf[c, at, :] = jnp.where(c == 0, rotate(kv), kv)
        tiles(body)

    def kv_refs(lo):
        return kvbuf.at[c, pl.ds(lo * keep, keep)]

    @scoped
    def kv_exchange(l):
        for lo in range(2):
            remote(kv_refs(lo), kv_refs(1 - lo), kv_send.at[l], kv_recv.at[l], sibling).start()

    def kv_outs(l):
        own = pl.ds(pl.multiple_of(y * seq, seq), seq)
        return [pltpu.make_async_copy(kvbuf.at[0, own], k_out.at[l, 0], out_sem.at[l]),
                pltpu.make_async_copy(kvbuf.at[1, own], v_out.at[l, 0], out_sem.at[l])]

    @scoped
    def kv_finish(l):
        wait_in(kvbuf.at[1 - c], kv_recv.at[l], kv_send.at[l])
        for copy in kv_outs(l):
            copy.start()

    @scoped
    def kv_drain(l):
        wait_out(kvbuf.at[c], kv_recv.at[l], kv_send.at[l])
        both = kvbuf.at[0, pl.ds(0, 2 * seq)]
        pltpu.make_async_copy(both, both, out_sem.at[l]).wait()

    @scoped
    def attend():
        score_scale = head_dim ** -0.5
        allowed = lax.broadcasted_iota(jnp.int32, (seq, seq), 0) >= lax.broadcasted_iota(jnp.int32, (seq, seq), 1)

        def body(start):
            at = pl.ds(start, seq)
            key, val = kvbuf[0, at, :], kvbuf[1, at, :]
            for n in range(heads):
                query = qbuf[at, n * head_dim:(n + 1) * head_dim]
                scores = lax.dot_general(query, key, (((1,), (1,)), ((), ())), preferred_element_type=F32) * score_scale
                scores = jnp.where(allowed, scores, -jnp.inf)
                weights = jnp.exp(scores - jnp.max(scores, axis=-1, keepdims=True))
                probs = (weights / jnp.sum(weights, axis=-1, keepdims=True)).astype(BF)
                ombuf[at, n * head_dim:(n + 1) * head_dim] = jnp.dot(probs, val, preferred_element_type=F32).astype(BF)
        tiles(body, n_prompts, seq)

    @scoped
    def gate_up(l, j):
        def body(start):
            at = pl.ds(start, tile)
            acc = jnp.dot(hbuf[at, :], bgu[l, j], preferred_element_type=F32).astype(BF).astype(F32)
            ombuf[at, q_cols + j * g_cols:q_cols + (j + 1) * g_cols] = (jax.nn.silu(acc[:, :g_cols]) * acc[:, g_cols:]).astype(BF)
        tiles(body)

    chips = [x, xl, xr, xo]
    half_w = width

    def chunk(b, hh):
        return b * HALVES + hh

    @scoped
    def project_out(l, b, hh):
        k = chunk(b, hh)

        def step(i, carry):
            at = pl.ds(pl.multiple_of((1 - i) * keep, keep), keep)
            part[k, at, :] = jnp.dot(ombuf[at, :], bod[l, hh, chips[b]], preferred_element_type=F32)

            @pl.when(i == 0)
            def _():
                remote(part.at[k, pl.ds(keep, keep)], rs0.at[k], r_send.at[0], r_recv.at[k, 0], sibling).start()
            return carry
        lax.fori_loop(0, 2, step, 0)

    def of_chip_half(k, yy, side):
        return part.at[k, pl.ds(pl.multiple_of(yy * seq, seq), seq), pl.ds(side * half_w, half_w)]

    def send_near(k, target, side, half, peer):
        remote(of_chip_half(k, target, half), rs2.at[k, side, :, pl.ds(half * half_w, half_w)],
               r_send.at[2], r_recv.at[k, 3], peer).start()

    @scoped
    def reduce_cores(b, hh):
        k = chunk(b, hh)
        wait_in(rs0.at[k], r_recv.at[k, 0], r_send.at[0])
        part[k, 0:keep, :] += rs0[k]
        remote(of_chip_half(k, yo, 0), rs1.at[k, 0], r_send.at[1], r_recv.at[k, 1], right_y).start()
        remote(of_chip_half(k, yo, 1), rs1.at[k, 1], r_send.at[1], r_recv.at[k, 2], left_y).start()
        send_near(k, yr, 0, 1, right_y)
        send_near(k, yl, 1, 0, left_y)

    @scoped
    def reduce_far(b, hh):
        k = chunk(b, hh)
        for side, target, peer in ((0, yr, right_y), (1, yl, left_y)):
            wait_in(rs1.at[k, side], r_recv.at[k, 1 + side], r_send.at[1])
            at = pl.ds(pl.multiple_of(target * seq, seq), seq)
            part[k, at, side * half_w:(side + 1) * half_w] += rs1[k, side]
            send_near(k, target, side, side, peer)

    def out_copy(i):
        return pltpu.make_async_copy(resid.at[i], y_out.at[0, :, pl.ds(pl.multiple_of(i * width, width), width)],
                                     out_sem.at[layers])

    @scoped
    def reduce_last(l, b, hh):
        k = chunk(b, hh)
        wait_in(rs2.at[k], r_recv.at[k, 3], r_send.at[2])
        own = pl.ds(pl.multiple_of(y * seq, seq), seq)
        total = part[k, own, :] + rs2[k, 0] + rs2[k, 1]
        for core in range(CORES):
            i = (chips[b] * CORES + core) * HALVES + hh
            resid[i] = (resid[i].astype(F32) + total[:, core * width:(core + 1) * width]).astype(BF)
            if l == layers - 1:
                out_copy(i).start()

    @scoped
    def reduce_drain():
        for n, ref in enumerate((rs0, rs1, rs2)):
            wait_out(ref, r_recv.at[0, 0], r_send.at[n])

    issue_own(0, 0)
    for l in range(layers):
        prepare_kv(l)
    prepare(1)
    issue_own(0, 1)
    issue_own(1)
    prepare(2)
    pltpu.make_async_copy(resid, resid, raw_sem.at[2]).wait()
    norm_own(0)
    gather_send(0)
    comm(0)
    gather_forward(0)
    gather_share(0)
    gather_finish(0)
    OWN, LEFT, RIGHT, FAR = range(4)
    rest = (SIDES,)
    for l in range(layers):
        base = l * per_layer
        last = l == layers - 1

        def ahead(p):
            while done[0] <= p:
                comm(done[0])

        ahead(base + 1)
        if l == 0:
            wait_piece(base, rest)
            kvw_send_own(l)
        project_q(l)
        ahead(base + 2)
        if l == 0:
            kvw_forward(l)
        wait_piece(base + 1, rest)
        gate_up(l, 0)
        kvw_finish(l)
        project_kv(l)
        kv_exchange(l)
        for j in range(1, GU_CHUNKS):
            ahead(base + 1 + j if last and j == GU_CHUNKS - 1 else base + 2 + j)
            wait_piece(base + 1 + j, rest)
            gate_up(l, j)
            if j == 1:
                kv_finish(l)
                attend()
        gather_drain(l)
        kv_drain(l)
        c0, c1 = base + 1 + GU_CHUNKS, base + 2 + GU_CHUNKS
        wait_piece(c0, (OWN_CHIP,))
        project_out(l, OWN, 0)
        wait_piece(c1, (OWN_CHIP,))
        project_out(l, OWN, 1)
        reduce_cores(OWN, 0)
        reduce_cores(OWN, 1)
        reduce_far(OWN, 0)
        ahead(c0)
        wait_piece(c0, (SIDES,))
        project_out(l, LEFT, 0)
        reduce_far(OWN, 1)
        project_out(l, RIGHT, 0)
        reduce_cores(LEFT, 0)
        reduce_cores(RIGHT, 0)
        reduce_last(l, OWN, 0)
        reduce_far(LEFT, 0)
        comm(c1)
        wait_piece(c1, (SIDES,))
        project_out(l, LEFT, 1)
        reduce_far(RIGHT, 0)
        reduce_last(l, OWN, 1)
        project_out(l, RIGHT, 1)
        reduce_cores(LEFT, 1)
        reduce_cores(RIGHT, 1)
        wait_piece(c0, (FAR_CHIP,))
        project_out(l, FAR, 0)
        reduce_last(l, LEFT, 0)
        reduce_far(LEFT, 1)
        reduce_far(RIGHT, 1)
        reduce_cores(FAR, 0)
        if not last:
            comm(c1 + 1)
        wait_piece(c1, (FAR_CHIP,))
        project_out(l, FAR, 1)
        reduce_cores(FAR, 1)
        reduce_far(FAR, 0)
        reduce_last(l, RIGHT, 0)
        reduce_last(l, LEFT, 1)
        reduce_last(l, RIGHT, 1)
        reduce_far(FAR, 1)
        reduce_last(l, FAR, 0)
        reduce_last(l, FAR, 1)
        reduce_drain()
        if not last:
            norm_own(l + 1)
            comm(c1 + 2)
            gather_send(l + 1)
            wait_piece(base + per_layer, rest)
            kvw_send_own(l + 1)
            gather_forward(l + 1)
            comm(c1 + 3)
            gather_share(l + 1)
            kvw_forward(l + 1)
            gather_finish(l + 1)
    drain_weights()
    pltpu.make_async_copy(resid, resid, out_sem.at[layers]).wait()


def take_over(*refs):
    sources, targets, held, sems = refs[:3], refs[3:6], refs[6:9], refs[9]
    loads = [pltpu.make_async_copy(sources[n], held[n], sems.at[0, n]) for n in range(3)]
    stores = [pltpu.make_async_copy(held[n], targets[n], sems.at[1, n]) for n in range(3)]
    for load in loads:
        load.start()
    for n in (1, 2, 0):
        loads[n].wait()
        stores[n].start()
    for store in stores:
        store.wait()


def run_layers(mesh_sizes, x_tokens, gamma_ln, w_q, w_kv, w_gu, w_o, w_d):
    n_x, n_y = mesh_sizes['wx'] // CORES, mesh_sizes['wy']
    assert n_x == 4 and n_y == 4 and x_tokens.shape[0] == 1
    layers, rows, q_loc = w_q.shape
    seq, d_model = x_tokens.shape[1:]
    head_dim = w_kv.shape[-1]
    hid_loc = w_gu.shape[-1]
    hid = hid_loc // CORES
    g_cols = hid // GU_CHUNKS
    q_cols = q_loc // CORES
    width = rows // HALVES
    toks = CORES * n_y * seq
    n_chunks = n_x * HALVES
    n_res = d_model // width
    cos_all, sin_all = rope_tables(seq, head_dim)
    dma = pltpu.SemaphoreType.DMA
    in_vmem, anywhere = pl.BlockSpec(memory_space=pltpu.VMEM), pl.BlockSpec(memory_space=pl.ANY)
    cache = jax.ShapeDtypeStruct((layers, 1, seq, head_dim), BF)
    results = pl.pallas_call(
        functools.partial(layers_kernel, (layers, n_x, n_y, seq, head_dim, rows, width)),
        out_shape=(jax.ShapeDtypeStruct(x_tokens.shape, BF), cache, cache),
        in_specs=[in_vmem] * 3 + [anywhere] * 6,
        out_specs=(anywhere,) * 3,
        scratch_shapes=[
            pltpu.VMEM((layers, d_model, q_cols), BF),
            pltpu.VMEM((layers, n_x * CORES, n_y, rows // n_y, head_dim), BF),
            pltpu.VMEM((layers, GU_CHUNKS, d_model, 2 * g_cols), BF),
            pltpu.VMEM((layers, HALVES, n_x, q_cols + hid, CORES * width), BF),
            pltpu.VMEM((toks, d_model), BF),
            pltpu.VMEM((toks, q_cols), BF),
            pltpu.VMEM((2, toks, head_dim), BF),
            pltpu.VMEM((toks, q_cols + hid), BF),
            pltpu.VMEM((n_chunks, toks, CORES * width), F32),
            pltpu.VMEM((n_chunks, toks // CORES, CORES * width), F32),
            pltpu.VMEM((n_chunks, 2, seq, width), F32),
            pltpu.VMEM((n_chunks, 2, seq, CORES * width), F32),
            pltpu.VMEM((n_res, seq, width), BF),
            pltpu.VMEM((2, CORES, rows, 2, g_cols), BF),
            pltpu.VMEM((layers, rows // n_y, 2, head_dim), BF),
            pltpu.VMEM((layers, GU_CHUNKS, CORES, rows, 2 * g_cols), BF),
            pltpu.VMEM((layers, 2, rows // n_y, head_dim), BF),
            dma((3 + layers,)),
            dma((4,)), dma((layers * (2 + GU_CHUNKS), 3)), dma((layers * HALVES, 5)),
            dma((layers,)), dma((layers, 4)),
            dma((layers,)), dma((layers, 5)),
            dma((layers,)), dma((layers,)),
            dma((3,)), dma((n_chunks, 4)),
            dma((layers + 1,)),
        ],
        compiler_params=pltpu.CompilerParams(collective_id=0, has_side_effects=True, vmem_limit_bytes=67043328),
    )(gamma_ln, cos_all, sin_all, x_tokens, w_q, w_kv, w_gu, w_o, w_d)
    shapes = [jax.ShapeDtypeStruct(r.shape, r.dtype) for r in results]
    return pl.pallas_call(
        take_over, out_shape=shapes, in_specs=[anywhere] * 3, out_specs=[anywhere] * 3,
        scratch_shapes=[pltpu.VMEM(r.shape, r.dtype) for r in results] + [dma((2, 3))],
    )(*results)


def solution(mesh):
    batch_axes = ('dp', 'wy', 'wx')
    in_specs = (P(batch_axes), P(), P(None, 'wx', 'wy'), P(None, 'wx'), P(None, 'wx', None, 'wy'), P(None, 'wy', 'wx'), P(None, 'wy', 'wx'))
    out_specs = (P(batch_axes), P(None, batch_axes), P(None, batch_axes))
    sizes = dict(mesh.shape)
    return jax.shard_map(functools.partial(run_layers, sizes), mesh=mesh, in_specs=in_specs, out_specs=out_specs, check_vma=False)
```

```python
import functools

import jax
import jax.numpy as jnp
import numpy as np
from jax import lax
from jax.experimental import pallas as pl
from jax.experimental.pallas import tpu as pltpu
from jax.sharding import PartitionSpec as P

LN_EPS = 1e-6
ROPE_BASE = 10000.0
CORES = 2
GU_CHUNKS = 4
HALVES = 2
BF, F32 = jnp.bfloat16, jnp.float32

L0, R1, SIDES, OWN_CHIP, FAR_CHIP = range(5)
A_L, A_R, A_TOP, A_BOT, A_SIB = range(5)


def rope_tables(seq_len, head_dim):
    inv_freq = np.float32(ROPE_BASE) ** (-2.0 * np.arange(head_dim // 2, dtype=np.float32) / head_dim).astype(np.float32)
    angles = np.arange(seq_len, dtype=np.float32)[:, None] * inv_freq[None, :]
    cos_tab, sin_tab = np.cos(angles.astype(np.float64)), np.sin(angles.astype(np.float64))
    return (np.concatenate([cos_tab, cos_tab], axis=-1).astype(np.float32),
            np.concatenate([-sin_tab, sin_tab], axis=-1).astype(np.float32))


def scoped(fn):
    @functools.wraps(fn)
    def inner(*args):
        def text(a):
            return ''.join(str(v) for v in a) if isinstance(a, tuple) else str(a)
        with jax.named_scope(fn.__name__ + '_' + '_'.join(text(a) for a in args)):
            return fn(*args)
    return inner


def layers_kernel(dims, gamma_in, cos_in, sin_in, x_ref, wq, wkv, wgu, wo, wd,
                  y_out, k_out, v_out,
                  bq, bkv, bgu, bod, hbuf, qbuf, kvbuf, ombuf, part, rs0, rs1, rs2, resid,
                  gu_raw, kv_raw, gu_stage, kv_stage, gamma_ref, cos_ref, sin_ref, raw_sem,
                  w_send, w_recv, c_recv, kvw_send, kvw_recv, a_send, a_recv, kv_send, kv_recv, r_send, r_recv, out_sem):
    layers, n_x, n_y, seq, head_dim, rows, width = dims
    heads = wo.shape[1] // CORES // head_dim
    hid = wd.shape[1] // CORES
    o_rows = wo.shape[1] // CORES
    q_cols = heads * head_dim
    g_cols = hid // GU_CHUNKS
    n_prompts = CORES * n_y
    toks = n_prompts * seq
    keep = n_y * seq
    tile = toks // 4

    wx = lax.axis_index('wx')
    y = lax.axis_index('wy')
    x, c = wx // CORES, wx % CORES
    xr, xl, xo = (x + 1) % n_x, (x + n_x - 1) % n_x, (x + 2) % n_x
    yr, yl, yo = (y + 1) % n_y, (y + n_y - 1) % n_y, (y + 2) % n_y
    sibling = {'wx': x * CORES + 1 - c}
    right_y, left_y = {'wy': yr}, {'wy': yl}

    def at_x(chip, core):
        return {'wx': chip * CORES + core}

    n_gu = layers * GU_CHUNKS
    tables = ((gamma_in, gamma_ref), (cos_in, cos_ref), (sin_in, sin_ref))
    kv_rows = rows // n_y

    def gu_load(g, core):
        cols = pl.ds(core * hid + (g % GU_CHUNKS) * g_cols, g_cols)
        return pltpu.make_async_copy(wgu.at[g // GU_CHUNKS, :, :, cols], gu_raw.at[g % 2, core], raw_sem.at[g % 2])

    def kv_load(l):
        mine = pl.ds(pl.multiple_of(y * kv_rows, kv_rows), kv_rows)
        return pltpu.make_async_copy(wkv.at[l, mine], kv_raw.at[l], raw_sem.at[3 + l])

    def x_load(i):
        return pltpu.make_async_copy(x_ref.at[0, :, pl.ds(i * width, width)], resid.at[i], raw_sem.at[2])

    barrier = pltpu.get_barrier_semaphore()
    peers = [sibling, right_y, left_y] + [at_x(chip, core) for chip in (xr, xl) for core in range(CORES)]
    for peer in peers:
        pl.semaphore_signal(barrier, inc=1, device_id=peer, device_id_type=pl.DeviceIdType.MESH)
    kv_load(0).start()
    for core in range(CORES):
        gu_load(0, core).start()
    for core in range(CORES):
        gu_load(1, core).start()
    for i in range(resid.shape[0]):
        x_load(i).start()
    for n, (table, held) in enumerate(tables):
        pltpu.make_async_copy(table, held, raw_sem.at[3 + layers + n]).start()
    for l in range(1, layers):
        kv_load(l).start()
    with jax.named_scope('barrier'):
        pl.semaphore_wait(barrier, len(peers))

    def remote(src, dst, send_sem, recv_sem, peer):
        return pltpu.make_async_remote_copy(src_ref=src, dst_ref=dst, send_sem=send_sem, recv_sem=recv_sem,
                                            device_id=peer, device_id_type=pl.DeviceIdType.MESH)

    def wait_in(ref, recv_sem, send_sem):
        remote(ref, ref, send_sem, recv_sem, sibling).wait_recv()

    def wait_out(ref, recv_sem, send_sem):
        remote(ref, ref, send_sem, recv_sem, sibling).wait_send()

    order = ('q', 'kv', 'gu', 'od')
    pieces = []
    n_blocks = n_outs = 0
    for l in range(layers):
        pieces.append([('q', l, 0, n_blocks), ('kv', l, 0, n_blocks + 1)])
        n_blocks += 2
        for j in range(GU_CHUNKS):
            pieces.append([('gu', l, j, n_blocks)])
            n_blocks += 1
        for hh in range(HALVES):
            pieces.append([('od', l, hh, n_outs)])
            n_outs += 1
    per_layer = len(pieces) // layers
    issue_after = [[p + 2] for p in range(len(pieces))]
    tail = len(pieces) - HALVES
    issue_after[tail - 2] = []
    issue_after[tail - 1] = [tail + hh for hh in range(HALVES)]
    issue_after[tail:] = [[] for _ in range(HALVES)]

    def sources(block, core):
        kind, l, j, _ = block
        if kind == 'q':
            return [wq.at[l, :, pl.ds(pl.multiple_of(core * q_cols, q_cols), q_cols)]]
        if kind == 'kv':
            return [kv_stage.at[l, core]]
        if kind == 'gu':
            return [gu_stage.at[l, j, core]]
        cols = pl.ds(j * width, width)
        return [wo.at[l, pl.ds(pl.multiple_of(core * o_rows, o_rows), o_rows), cols],
                wd.at[l, pl.ds(pl.multiple_of(core * hid, hid), hid), cols]]

    def landing(block, chip, core):
        kind, l, j, _ = block
        if kind == 'kv':
            return bkv.at[l, chip * CORES + core, y]
        if kind == 'od':
            return bod.at[l, j, chip, :, pl.ds(pl.multiple_of(core * width, width), width)]
        row = pl.ds(pl.multiple_of((chip * CORES + core) * rows, rows), rows)
        return bq.at[l, row] if kind == 'q' else bgu.at[l, j, row]

    def landings(block):
        here = landing(block, x, c)
        return [here.at[pl.ds(0, o_rows)], here.at[pl.ds(o_rows, hid)]] if block[0] == 'od' else [here]

    def received(block, how):
        return c_recv.at[block[3], how] if block[0] == 'od' else w_recv.at[block[3], how]

    def prepare_kv(l):
        kv_load(l).wait()
        for core in range(CORES):
            kv_stage[l, core] = kv_raw[l, :, core, :]

    @scoped
    def prepare(p):
        if p >= len(pieces) or pieces[p][0][0] != 'gu':
            return
        _, l, j, _ = pieces[p][0]
        g = l * GU_CHUNKS + j
        step_rows = rows // 4
        pltpu.make_async_copy(gu_raw.at[g % 2], gu_raw.at[g % 2], raw_sem.at[g % 2]).wait()
        for core in range(CORES):
            def step(i, carry):
                at = pl.ds(pl.multiple_of(i * step_rows, step_rows), step_rows)
                for which in range(2):
                    gu_stage[l, j, core, at, which * g_cols:(which + 1) * g_cols] = gu_raw[g % 2, core, at, which, :]
                return carry
            lax.fori_loop(0, 4, step, 0)
            if g + 2 < n_gu:
                gu_load(g + 2, core).start()

    @scoped
    def issue_own(p, only=None):
        if p >= len(pieces):
            return
        for block in pieces[p] if only is None else [pieces[p][only]]:
            sent = w_send.at[order.index(block[0])]
            side = [SIDES * c, SIDES - c]
            near = OWN_CHIP if block[0] == 'od' else SIDES
            for core in range(CORES):
                for src, dst in zip(sources(block, core), landings(block)):
                    remote(src, dst, sent, received(block, side[0]), at_x(xr, core)).start()
                    remote(src, dst, sent, received(block, side[1]), at_x(xl, core)).start()
            for src, dst in zip(sources(block, 1 - c), landings(block)):
                remote(src, dst, sent, received(block, near), sibling).start()
            for src, dst in zip(sources(block, c), landings(block)):
                pltpu.make_async_copy(src, dst, received(block, near)).start()

    def wait_block(block, how):
        kind, l, j, _ = block
        if how in (L0, R1):
            ref = landing(block, xl, 0) if how == L0 else landing(block, xr, 1)
        elif kind == 'od':
            ref = bod.at[l, j, {SIDES: xl, OWN_CHIP: x, FAR_CHIP: xo}[how]]
        else:
            others = n_x * CORES - 2
            ref = bkv.at[l, pl.ds(0, others), y] if kind == 'kv' else (
                bq.at[l, pl.ds(0, others * rows)] if kind == 'q' else bgu.at[l, j, pl.ds(0, others * rows)])
        wait_in(ref, received(block, how), w_send.at[0])

    done = [0]

    @scoped
    def comm(p):
        if p >= len(pieces):
            return
        assert p == done[0]
        done[0] = p + 1
        for block in pieces[p]:
            far = FAR_CHIP if block[0] == 'od' else SIDES
            wait_block(block, L0)
            from_left = landing(block, xl, 0)
            remote(from_left, from_left, w_send.at[order.index(block[0])], received(block, far), at_x(xr, c)).start()
            wait_block(block, R1)
            from_right = landing(block, xr, 1)
            remote(from_right, from_right, w_send.at[order.index(block[0])], received(block, far), at_x(xl, c)).start()
        for later in issue_after[p]:
            issue_own(later)
        prepare(p + 3)

    @scoped
    def wait_piece(p, hows):
        for block in pieces[p]:
            for how in hows:
                wait_block(block, how)

    @scoped
    def drain_weights():
        n_src = n_x * CORES
        for n, ref in enumerate((bq.at[:, pl.ds(0, (n_src - 1) * rows)], bkv.at[:, pl.ds(0, n_src - 1), 0],
                                 bgu.at[:, :, pl.ds(0, (n_src - 1) * rows)],
                                 bod.at[:, :, :, pl.ds(0, (o_rows + hid) // n_src * (n_src - 1))])):
            wait_out(ref, w_recv.at[0, 0], w_send.at[n])

    def kv_quarter(l, yy, half=None):
        n_src = n_x * CORES
        return bkv.at[l, pl.ds(0 if half is None else half * (n_src // 2), n_src if half is None else n_src // 2), yy]

    def kvw_copy(l, ref, kind, peer):
        remote(ref, ref, kvw_send.at[l], kvw_recv.at[l, kind], peer).start()

    @scoped
    def kvw_send_own(l):
        kvw_copy(l, kv_quarter(l, y), A_L, right_y)
        kvw_copy(l, kv_quarter(l, y), A_R, left_y)

    @scoped
    def kvw_forward(l):
        wait_in(kv_quarter(l, yl), kvw_recv.at[l, A_L], kvw_send.at[l])
        kvw_copy(l, kv_quarter(l, yl, 0), A_TOP, right_y)
        wait_in(kv_quarter(l, yr), kvw_recv.at[l, A_R], kvw_send.at[l])
        kvw_copy(l, kv_quarter(l, yr, 1), A_BOT, left_y)

    @scoped
    def kvw_finish(l):
        wait_in(kv_quarter(l, yo, 0), kvw_recv.at[l, A_TOP], kvw_send.at[l])
        wait_in(kv_quarter(l, yo, 1), kvw_recv.at[l, A_BOT], kvw_send.at[l])
        wait_out(bkv.at[l, :, pl.ds(0, n_y - 1)], kvw_recv.at[l, A_L], kvw_send.at[l])

    def prompt(slot, part_of=None):
        if part_of is None:
            return hbuf.at[pl.ds(pl.multiple_of(slot * seq, seq), seq)]
        half = seq // 2
        return hbuf.at[pl.ds(pl.multiple_of(slot * seq + part_of * half, half), half)]

    def a_copy(l, src, dst, kind, peer):
        remote(src, dst, a_send.at[l], a_recv.at[l, kind], peer).start()

    def a_wait(l, ref, kind):
        wait_in(ref, a_recv.at[l, kind], a_send.at[l])

    @scoped
    def gather_send(l):
        a_copy(l, prompt(y), prompt(y), A_L, right_y)
        a_copy(l, prompt(y), prompt(y), A_R, left_y)
        a_copy(l, prompt(y), prompt(n_y + y), A_SIB, sibling)

    @scoped
    def gather_forward(l):
        a_wait(l, prompt(yl), A_L)
        a_copy(l, prompt(yl, 0), prompt(yl, 0), A_TOP, right_y)
        a_copy(l, prompt(yl), prompt(n_y + yl), A_SIB, sibling)
        a_wait(l, prompt(yr), A_R)
        a_copy(l, prompt(yr, 1), prompt(yr, 1), A_BOT, left_y)
        a_copy(l, prompt(yr), prompt(n_y + yr), A_SIB, sibling)

    @scoped
    def gather_share(l):
        a_wait(l, prompt(yo, 0), A_TOP)
        a_copy(l, prompt(yo, 0), prompt(n_y + yo, 0), A_SIB, sibling)
        a_wait(l, prompt(yo, 1), A_BOT)
        a_copy(l, prompt(yo, 1), prompt(n_y + yo, 1), A_SIB, sibling)

    @scoped
    def gather_finish(l):
        a_wait(l, hbuf.at[pl.ds(keep, keep)], A_SIB)

    @scoped
    def gather_drain(l):
        wait_out(hbuf.at[pl.ds(0, 7 * seq)], a_recv.at[l, A_L], a_send.at[l])

    n_res = resid.shape[0]
    d_model = n_res * width

    @scoped
    def norm_own(l):
        total = jnp.zeros((seq, 1), F32)
        for i in range(n_res):
            total += jnp.sum(resid[i].astype(F32), axis=-1, keepdims=True)
        mean = total / d_model
        square = jnp.zeros((seq, 1), F32)
        for i in range(n_res):
            centered = resid[i].astype(F32) - mean
            square += jnp.sum(centered * centered, axis=-1, keepdims=True)
        scale = lax.rsqrt(square / d_model + LN_EPS)
        own = pl.ds(pl.multiple_of(y * seq, seq), seq)
        for i in range(n_res):
            value = (resid[i].astype(F32) - mean) * scale * gamma_ref[l:l + 1, i * width:(i + 1) * width]
            hbuf[own, i * width:(i + 1) * width] = value.astype(BF)

    def rotate(value):
        value = value.astype(F32)
        cos_all = jnp.concatenate([cos_ref[...]] * (tile // seq), axis=0)
        sin_all = jnp.concatenate([sin_ref[...]] * (tile // seq), axis=0)
        return (value * cos_all + pltpu.roll(value, head_dim // 2, 1) * sin_all).astype(BF)

    def tiles(body, n=4, size=tile):
        def step(i, carry):
            body(pl.multiple_of(i * size, size))
            return carry
        lax.fori_loop(0, n, step, 0)

    @scoped
    def project_q(l):
        def body(start):
            at = pl.ds(start, tile)
            acc = jnp.dot(hbuf[at, :], bq[l], preferred_element_type=F32).astype(BF)
            for n in range(heads):
                qbuf[at, n * head_dim:(n + 1) * head_dim] = rotate(acc[:, n * head_dim:(n + 1) * head_dim])
        tiles(body)

    @scoped
    def project_kv(l):
        def body(start):
            at = pl.ds(start, tile)
            weights = bkv[l].reshape(d_model, head_dim)
            kv = jnp.dot(hbuf[at, :], weights, preferred_element_type=F32).astype(BF)
            kvbuf[c, at, :] = jnp.where(c == 0, rotate(kv), kv)
        tiles(body)

    def kv_refs(lo):
        return kvbuf.at[c, pl.ds(lo * keep, keep)]

    @scoped
    def kv_exchange(l):
        for lo in range(2):
            remote(kv_refs(lo), kv_refs(1 - lo), kv_send.at[l], kv_recv.at[l], sibling).start()

    def kv_outs(l):
        own = pl.ds(pl.multiple_of(y * seq, seq), seq)
        return [pltpu.make_async_copy(kvbuf.at[0, own], k_out.at[l, 0], out_sem.at[l]),
                pltpu.make_async_copy(kvbuf.at[1, own], v_out.at[l, 0], out_sem.at[l])]

    @scoped
    def kv_finish(l):
        wait_in(kvbuf.at[1 - c], kv_recv.at[l], kv_send.at[l])
        for copy in kv_outs(l):
            copy.start()

    @scoped
    def kv_drain(l):
        wait_out(kvbuf.at[c], kv_recv.at[l], kv_send.at[l])
        both = kvbuf.at[0, pl.ds(0, 2 * seq)]
        pltpu.make_async_copy(both, both, out_sem.at[l]).wait()

    @scoped
    def attend():
        score_scale = head_dim ** -0.5
        allowed = lax.broadcasted_iota(jnp.int32, (seq, seq), 0) >= lax.broadcasted_iota(jnp.int32, (seq, seq), 1)

        def body(start):
            at = pl.ds(start, seq)
            key, val = kvbuf[0, at, :], kvbuf[1, at, :]
            for n in range(heads):
                query = qbuf[at, n * head_dim:(n + 1) * head_dim]
                scores = lax.dot_general(query, key, (((1,), (1,)), ((), ())), preferred_element_type=F32) * score_scale
                scores = jnp.where(allowed, scores, -jnp.inf)
                weights = jnp.exp(scores - jnp.max(scores, axis=-1, keepdims=True))
                probs = (weights / jnp.sum(weights, axis=-1, keepdims=True)).astype(BF)
                ombuf[at, n * head_dim:(n + 1) * head_dim] = jnp.dot(probs, val, preferred_element_type=F32).astype(BF)
        tiles(body, n_prompts, seq)

    @scoped
    def gate_up(l, j):
        def body(start):
            at = pl.ds(start, tile)
            acc = jnp.dot(hbuf[at, :], bgu[l, j], preferred_element_type=F32).astype(BF).astype(F32)
            ombuf[at, q_cols + j * g_cols:q_cols + (j + 1) * g_cols] = (jax.nn.silu(acc[:, :g_cols]) * acc[:, g_cols:]).astype(BF)
        tiles(body)

    chips = [x, xl, xr, xo]
    half_w = width

    def chunk(b, hh):
        return b * HALVES + hh

    @scoped
    def project_out(l, b, hh):
        k = chunk(b, hh)

        def step(i, carry):
            at = pl.ds(pl.multiple_of((1 - i) * keep, keep), keep)
            part[k, at, :] = jnp.dot(ombuf[at, :], bod[l, hh, chips[b]], preferred_element_type=F32)

            @pl.when(i == 0)
            def _():
                remote(part.at[k, pl.ds(keep, keep)], rs0.at[k], r_send.at[0], r_recv.at[k, 0], sibling).start()
            return carry
        lax.fori_loop(0, 2, step, 0)

    def of_chip_half(k, yy, side):
        return part.at[k, pl.ds(pl.multiple_of(yy * seq, seq), seq), pl.ds(side * half_w, half_w)]

    def send_near(k, target, side, half, peer):
        remote(of_chip_half(k, target, half), rs2.at[k, side, :, pl.ds(half * half_w, half_w)],
               r_send.at[2], r_recv.at[k, 3], peer).start()

    @scoped
    def reduce_cores(b, hh):
        k = chunk(b, hh)
        wait_in(rs0.at[k], r_recv.at[k, 0], r_send.at[0])
        part[k, 0:keep, :] += rs0[k]
        remote(of_chip_half(k, yo, 0), rs1.at[k, 0], r_send.at[1], r_recv.at[k, 1], right_y).start()
        remote(of_chip_half(k, yo, 1), rs1.at[k, 1], r_send.at[1], r_recv.at[k, 2], left_y).start()
        send_near(k, yr, 0, 1, right_y)
        send_near(k, yl, 1, 0, left_y)

    @scoped
    def reduce_far(b, hh):
        k = chunk(b, hh)
        for side, target, peer in ((0, yr, right_y), (1, yl, left_y)):
            wait_in(rs1.at[k, side], r_recv.at[k, 1 + side], r_send.at[1])
            at = pl.ds(pl.multiple_of(target * seq, seq), seq)
            part[k, at, side * half_w:(side + 1) * half_w] += rs1[k, side]
            send_near(k, target, side, side, peer)

    def out_copy(i):
        return pltpu.make_async_copy(resid.at[i], y_out.at[0, :, pl.ds(pl.multiple_of(i * width, width), width)],
                                     out_sem.at[layers])

    @scoped
    def reduce_last(l, b, hh):
        k = chunk(b, hh)
        wait_in(rs2.at[k], r_recv.at[k, 3], r_send.at[2])
        own = pl.ds(pl.multiple_of(y * seq, seq), seq)
        total = part[k, own, :] + rs2[k, 0] + rs2[k, 1]
        for core in range(CORES):
            i = (chips[b] * CORES + core) * HALVES + hh
            resid[i] = (resid[i].astype(F32) + total[:, core * width:(core + 1) * width]).astype(BF)
            if l == layers - 1:
                out_copy(i).start()

    @scoped
    def reduce_drain():
        for n, ref in enumerate((rs0, rs1, rs2)):
            wait_out(ref, r_recv.at[0, 0], r_send.at[n])

    issue_own(0, 0)
    for l in range(layers):
        prepare_kv(l)
    prepare(1)
    issue_own(0, 1)
    issue_own(1)
    prepare(2)
    pltpu.make_async_copy(resid, resid, raw_sem.at[2]).wait()
    for n, (table, held) in enumerate(tables):
        pltpu.make_async_copy(table, held, raw_sem.at[3 + layers + n]).wait()
    norm_own(0)
    gather_send(0)
    comm(0)
    gather_forward(0)
    gather_share(0)
    gather_finish(0)
    OWN, LEFT, RIGHT, FAR = range(4)
    rest = (SIDES,)
    for l in range(layers):
        base = l * per_layer
        last = l == layers - 1

        def ahead(p):
            while done[0] <= p:
                comm(done[0])

        ahead(base + 1)
        if l == 0:
            wait_piece(base, rest)
            kvw_send_own(l)
        project_q(l)
        ahead(base + 2)
        if l == 0:
            kvw_forward(l)
        wait_piece(base + 1, rest)
        gate_up(l, 0)
        kvw_finish(l)
        project_kv(l)
        kv_exchange(l)
        for j in range(1, GU_CHUNKS):
            ahead(base + 1 + j if last and j == GU_CHUNKS - 1 else base + 2 + j)
            wait_piece(base + 1 + j, rest)
            gate_up(l, j)
            if j == 1:
                kv_finish(l)
                attend()
        gather_drain(l)
        kv_drain(l)
        c0, c1 = base + 1 + GU_CHUNKS, base + 2 + GU_CHUNKS
        wait_piece(c0, (OWN_CHIP,))
        project_out(l, OWN, 0)
        wait_piece(c1, (OWN_CHIP,))
        project_out(l, OWN, 1)
        reduce_cores(OWN, 0)
        reduce_cores(OWN, 1)
        reduce_far(OWN, 0)
        ahead(c0)
        wait_piece(c0, (SIDES,))
        project_out(l, LEFT, 0)
        reduce_far(OWN, 1)
        project_out(l, RIGHT, 0)
        reduce_cores(LEFT, 0)
        reduce_cores(RIGHT, 0)
        reduce_last(l, OWN, 0)
        reduce_far(LEFT, 0)
        comm(c1)
        wait_piece(c1, (SIDES,))
        project_out(l, LEFT, 1)
        reduce_far(RIGHT, 0)
        reduce_last(l, OWN, 1)
        project_out(l, RIGHT, 1)
        reduce_cores(LEFT, 1)
        reduce_cores(RIGHT, 1)
        wait_piece(c0, (FAR_CHIP,))
        project_out(l, FAR, 0)
        reduce_last(l, LEFT, 0)
        reduce_far(LEFT, 1)
        reduce_far(RIGHT, 1)
        reduce_cores(FAR, 0)
        if not last:
            comm(c1 + 1)
        wait_piece(c1, (FAR_CHIP,))
        project_out(l, FAR, 1)
        reduce_far(FAR, 0)
        reduce_cores(FAR, 1)
        reduce_last(l, RIGHT, 0)
        reduce_last(l, LEFT, 1)
        reduce_last(l, RIGHT, 1)
        reduce_far(FAR, 1)
        reduce_last(l, FAR, 0)
        reduce_last(l, FAR, 1)
        reduce_drain()
        if not last:
            norm_own(l + 1)
            comm(c1 + 2)
            gather_send(l + 1)
            wait_piece(base + per_layer, rest)
            kvw_send_own(l + 1)
            gather_forward(l + 1)
            comm(c1 + 3)
            gather_share(l + 1)
            kvw_forward(l + 1)
            gather_finish(l + 1)
    drain_weights()
    pltpu.make_async_copy(resid, resid, out_sem.at[layers]).wait()


def take_over(y_in, k_in, v_in, y_out, k_out, v_out, held, sems):
    quarter = y_in.shape[1] // 4
    caches = [pltpu.make_async_copy(k_in, k_out, sems.at[0, 4]), pltpu.make_async_copy(v_in, v_out, sems.at[1, 4])]
    rows = [pl.ds(n * quarter, quarter) for n in range(4)]
    loads = [pltpu.make_async_copy(y_in.at[0, rows[n]], held.at[rows[n]], sems.at[0, n]) for n in range(4)]
    stores = [pltpu.make_async_copy(held.at[rows[n]], y_out.at[0, rows[n]], sems.at[1, n]) for n in range(4)]
    for copy in caches + loads:
        copy.start()
    for n in range(4):
        loads[n].wait()
        stores[n].start()
    for copy in stores + caches:
        copy.wait()


def run_layers(mesh_sizes, x_tokens, gamma_ln, w_q, w_kv, w_gu, w_o, w_d):
    n_x, n_y = mesh_sizes['wx'] // CORES, mesh_sizes['wy']
    assert n_x == 4 and n_y == 4 and x_tokens.shape[0] == 1
    layers, rows, q_loc = w_q.shape
    seq, d_model = x_tokens.shape[1:]
    head_dim = w_kv.shape[-1]
    hid_loc = w_gu.shape[-1]
    hid = hid_loc // CORES
    g_cols = hid // GU_CHUNKS
    q_cols = q_loc // CORES
    width = rows // HALVES
    toks = CORES * n_y * seq
    n_chunks = n_x * HALVES
    n_res = d_model // width
    cos_all, sin_all = rope_tables(seq, head_dim)
    dma = pltpu.SemaphoreType.DMA
    anywhere = pl.BlockSpec(memory_space=pl.ANY)
    cache = jax.ShapeDtypeStruct((layers, 1, seq, head_dim), BF)
    results = pl.pallas_call(
        functools.partial(layers_kernel, (layers, n_x, n_y, seq, head_dim, rows, width)),
        out_shape=(jax.ShapeDtypeStruct(x_tokens.shape, BF), cache, cache),
        in_specs=[anywhere] * 9,
        out_specs=(anywhere,) * 3,
        scratch_shapes=[
            pltpu.VMEM((layers, d_model, q_cols), BF),
            pltpu.VMEM((layers, n_x * CORES, n_y, rows // n_y, head_dim), BF),
            pltpu.VMEM((layers, GU_CHUNKS, d_model, 2 * g_cols), BF),
            pltpu.VMEM((layers, HALVES, n_x, q_cols + hid, CORES * width), BF),
            pltpu.VMEM((toks, d_model), BF),
            pltpu.VMEM((toks, q_cols), BF),
            pltpu.VMEM((2, toks, head_dim), BF),
            pltpu.VMEM((toks, q_cols + hid), BF),
            pltpu.VMEM((n_chunks, toks, CORES * width), F32),
            pltpu.VMEM((n_chunks, toks // CORES, CORES * width), F32),
            pltpu.VMEM((n_chunks, 2, seq, width), F32),
            pltpu.VMEM((n_chunks, 2, seq, CORES * width), F32),
            pltpu.VMEM((n_res, seq, width), BF),
            pltpu.VMEM((2, CORES, rows, 2, g_cols), BF),
            pltpu.VMEM((layers, rows // n_y, 2, head_dim), BF),
            pltpu.VMEM((layers, GU_CHUNKS, CORES, rows, 2 * g_cols), BF),
            pltpu.VMEM((layers, 2, rows // n_y, head_dim), BF),
            pltpu.VMEM(gamma_ln.shape, F32), pltpu.VMEM(cos_all.shape, F32), pltpu.VMEM(sin_all.shape, F32),
            dma((6 + layers,)),
            dma((4,)), dma((layers * (2 + GU_CHUNKS), 3)), dma((layers * HALVES, 5)),
            dma((layers,)), dma((layers, 4)),
            dma((layers,)), dma((layers, 5)),
            dma((layers,)), dma((layers,)),
            dma((3,)), dma((n_chunks, 4)),
            dma((layers + 1,)),
        ],
        compiler_params=pltpu.CompilerParams(collective_id=0, has_side_effects=True, vmem_limit_bytes=67043328),
    )(gamma_ln, cos_all, sin_all, x_tokens, w_q, w_kv, w_gu, w_o, w_d)
    shapes = [jax.ShapeDtypeStruct(r.shape, r.dtype) for r in results]
    return pl.pallas_call(
        take_over, out_shape=shapes, in_specs=[anywhere] * 3, out_specs=[anywhere] * 3,
        scratch_shapes=[pltpu.VMEM((seq, d_model), BF), dma((2, 5))],
    )(*results)


def solution(mesh):
    batch_axes = ('dp', 'wy', 'wx')
    in_specs = (P(batch_axes), P(), P(None, 'wx', 'wy'), P(None, 'wx'), P(None, 'wx', None, 'wy'), P(None, 'wy', 'wx'), P(None, 'wy', 'wx'))
    out_specs = (P(batch_axes), P(None, batch_axes), P(None, batch_axes))
    sizes = dict(mesh.shape)
    return jax.shard_map(functools.partial(run_layers, sizes), mesh=mesh, in_specs=in_specs, out_specs=out_specs, check_vma=False)
```

```python
import functools

import jax
import jax.numpy as jnp
import numpy as np
from jax import lax
from jax.experimental import pallas as pl
from jax.experimental.pallas import tpu as pltpu
from jax.sharding import PartitionSpec as P

LN_EPS = 1e-6
ROPE_BASE = 10000.0
CORES = 2
GU_CHUNKS = 4
HALVES = 2
BF, F32 = jnp.bfloat16, jnp.float32

L0, R1, SIDES, OWN_CHIP, FAR_CHIP = range(5)
A_L, A_R, A_TOP, A_BOT, A_SIB = range(5)


def rope_tables(seq_len, head_dim):
    inv_freq = np.float32(ROPE_BASE) ** (-2.0 * np.arange(head_dim // 2, dtype=np.float32) / head_dim).astype(np.float32)
    angles = np.arange(seq_len, dtype=np.float32)[:, None] * inv_freq[None, :]
    cos_tab, sin_tab = np.cos(angles.astype(np.float64)), np.sin(angles.astype(np.float64))
    return (np.concatenate([cos_tab, cos_tab], axis=-1).astype(np.float32),
            np.concatenate([-sin_tab, sin_tab], axis=-1).astype(np.float32))


def layers_kernel(dims, gamma_in, cos_in, sin_in, x_ref, wq, wkv, wgu, wo, wd,
                  y_out, k_out, v_out,
                  bq, bkv, bgu, bod, hbuf, qbuf, kvbuf, ombuf, part, rs0, rs1, rs2, resid,
                  gu_raw, kv_raw, gu_stage, kv_stage, gamma_ref, cos_ref, sin_ref, raw_sem,
                  w_send, w_recv, c_recv, kvw_send, kvw_recv, a_send, a_recv, kv_send, kv_recv, r_send, r_recv, out_sem):
    layers, n_x, n_y, seq, head_dim, rows, width = dims
    heads = wo.shape[1] // CORES // head_dim
    hid = wd.shape[1] // CORES
    o_rows = wo.shape[1] // CORES
    q_cols = heads * head_dim
    g_cols = hid // GU_CHUNKS
    n_prompts = CORES * n_y
    toks = n_prompts * seq
    keep = n_y * seq
    tile = toks // 4

    wx = lax.axis_index('wx')
    y = lax.axis_index('wy')
    x, c = wx // CORES, wx % CORES
    xr, xl, xo = (x + 1) % n_x, (x + n_x - 1) % n_x, (x + 2) % n_x
    yr, yl, yo = (y + 1) % n_y, (y + n_y - 1) % n_y, (y + 2) % n_y
    sibling = {'wx': x * CORES + 1 - c}
    right_y, left_y = {'wy': yr}, {'wy': yl}

    def at_x(chip, core):
        return {'wx': chip * CORES + core}

    n_gu = layers * GU_CHUNKS
    tables = ((gamma_in, gamma_ref), (cos_in, cos_ref), (sin_in, sin_ref))
    kv_rows = rows // n_y

    def gu_load(g, core):
        cols = pl.ds(core * hid + (g % GU_CHUNKS) * g_cols, g_cols)
        return pltpu.make_async_copy(wgu.at[g // GU_CHUNKS, :, :, cols], gu_raw.at[g % 2, core], raw_sem.at[g % 2])

    def kv_load(l):
        mine = pl.ds(pl.multiple_of(y * kv_rows, kv_rows), kv_rows)
        return pltpu.make_async_copy(wkv.at[l, mine], kv_raw.at[l], raw_sem.at[3 + l])

    def x_load(i):
        return pltpu.make_async_copy(x_ref.at[0, :, pl.ds(i * width, width)], resid.at[i], raw_sem.at[2])

    barrier = pltpu.get_barrier_semaphore()
    peers = [sibling, right_y, left_y] + [at_x(chip, core) for chip in (xr, xl) for core in range(CORES)]
    for peer in peers:
        pl.semaphore_signal(barrier, inc=1, device_id=peer, device_id_type=pl.DeviceIdType.MESH)
    kv_load(0).start()
    for core in range(CORES):
        gu_load(0, core).start()
    for core in range(CORES):
        gu_load(1, core).start()
    for i in range(resid.shape[0]):
        x_load(i).start()
    for n, (table, held) in enumerate(tables):
        pltpu.make_async_copy(table, held, raw_sem.at[3 + layers + n]).start()
    for l in range(1, layers):
        kv_load(l).start()
    pl.semaphore_wait(barrier, len(peers))

    def remote(src, dst, send_sem, recv_sem, peer):
        return pltpu.make_async_remote_copy(src_ref=src, dst_ref=dst, send_sem=send_sem, recv_sem=recv_sem,
                                            device_id=peer, device_id_type=pl.DeviceIdType.MESH)

    def wait_in(ref, recv_sem, send_sem):
        remote(ref, ref, send_sem, recv_sem, sibling).wait_recv()

    def wait_out(ref, recv_sem, send_sem):
        remote(ref, ref, send_sem, recv_sem, sibling).wait_send()

    order = ('q', 'kv', 'gu', 'od')
    pieces = []
    n_blocks = n_outs = 0
    for l in range(layers):
        pieces.append([('q', l, 0, n_blocks), ('kv', l, 0, n_blocks + 1)])
        n_blocks += 2
        for j in range(GU_CHUNKS):
            pieces.append([('gu', l, j, n_blocks)])
            n_blocks += 1
        for hh in range(HALVES):
            pieces.append([('od', l, hh, n_outs)])
            n_outs += 1
    per_layer = len(pieces) // layers
    issue_after = [[p + 2] for p in range(len(pieces))]
    tail = len(pieces) - HALVES
    issue_after[tail - 2] = []
    issue_after[tail - 1] = [tail + hh for hh in range(HALVES)]
    issue_after[tail:] = [[] for _ in range(HALVES)]

    def sources(block, core):
        kind, l, j, _ = block
        if kind == 'q':
            return [wq.at[l, :, pl.ds(pl.multiple_of(core * q_cols, q_cols), q_cols)]]
        if kind == 'kv':
            return [kv_stage.at[l, core]]
        if kind == 'gu':
            return [gu_stage.at[l, j, core]]
        cols = pl.ds(j * width, width)
        return [wo.at[l, pl.ds(pl.multiple_of(core * o_rows, o_rows), o_rows), cols],
                wd.at[l, pl.ds(pl.multiple_of(core * hid, hid), hid), cols]]

    def landing(block, chip, core):
        kind, l, j, _ = block
        if kind == 'kv':
            return bkv.at[l, chip * CORES + core, y]
        if kind == 'od':
            return bod.at[l, j, chip, :, pl.ds(pl.multiple_of(core * width, width), width)]
        row = pl.ds(pl.multiple_of((chip * CORES + core) * rows, rows), rows)
        return bq.at[l, row] if kind == 'q' else bgu.at[l, j, row]

    def landings(block):
        here = landing(block, x, c)
        return [here.at[pl.ds(0, o_rows)], here.at[pl.ds(o_rows, hid)]] if block[0] == 'od' else [here]

    def received(block, how):
        return c_recv.at[block[3], how] if block[0] == 'od' else w_recv.at[block[3], how]

    def prepare_kv(l):
        kv_load(l).wait()
        for core in range(CORES):
            kv_stage[l, core] = kv_raw[l, :, core, :]

    def prepare(p):
        if p >= len(pieces) or pieces[p][0][0] != 'gu':
            return
        _, l, j, _ = pieces[p][0]
        g = l * GU_CHUNKS + j
        step_rows = rows // 4
        pltpu.make_async_copy(gu_raw.at[g % 2], gu_raw.at[g % 2], raw_sem.at[g % 2]).wait()
        for core in range(CORES):
            def step(i, carry):
                at = pl.ds(pl.multiple_of(i * step_rows, step_rows), step_rows)
                for which in range(2):
                    gu_stage[l, j, core, at, which * g_cols:(which + 1) * g_cols] = gu_raw[g % 2, core, at, which, :]
                return carry
            lax.fori_loop(0, 4, step, 0)
            if g + 2 < n_gu:
                gu_load(g + 2, core).start()

    def issue_own(p, only=None):
        if p >= len(pieces):
            return
        for block in pieces[p] if only is None else [pieces[p][only]]:
            sent = w_send.at[order.index(block[0])]
            side = [SIDES * c, SIDES - c]
            near = OWN_CHIP if block[0] == 'od' else SIDES
            for core in range(CORES):
                for src, dst in zip(sources(block, core), landings(block)):
                    remote(src, dst, sent, received(block, side[0]), at_x(xr, core)).start()
                    remote(src, dst, sent, received(block, side[1]), at_x(xl, core)).start()
            for src, dst in zip(sources(block, 1 - c), landings(block)):
                remote(src, dst, sent, received(block, near), sibling).start()
            for src, dst in zip(sources(block, c), landings(block)):
                pltpu.make_async_copy(src, dst, received(block, near)).start()

    def wait_block(block, how):
        kind, l, j, _ = block
        if how in (L0, R1):
            ref = landing(block, xl, 0) if how == L0 else landing(block, xr, 1)
        elif kind == 'od':
            ref = bod.at[l, j, {SIDES: xl, OWN_CHIP: x, FAR_CHIP: xo}[how]]
        else:
            others = n_x * CORES - 2
            ref = bkv.at[l, pl.ds(0, others), y] if kind == 'kv' else (
                bq.at[l, pl.ds(0, others * rows)] if kind == 'q' else bgu.at[l, j, pl.ds(0, others * rows)])
        wait_in(ref, received(block, how), w_send.at[0])

    done = [0]

    def comm(p):
        if p >= len(pieces):
            return
        assert p == done[0]
        done[0] = p + 1
        for block in pieces[p]:
            far = FAR_CHIP if block[0] == 'od' else SIDES
            wait_block(block, L0)
            from_left = landing(block, xl, 0)
            remote(from_left, from_left, w_send.at[order.index(block[0])], received(block, far), at_x(xr, c)).start()
            wait_block(block, R1)
            from_right = landing(block, xr, 1)
            remote(from_right, from_right, w_send.at[order.index(block[0])], received(block, far), at_x(xl, c)).start()
        for later in issue_after[p]:
            issue_own(later)
        prepare(p + 3)

    def wait_piece(p, hows):
        for block in pieces[p]:
            for how in hows:
                wait_block(block, how)

    def drain_weights():
        n_src = n_x * CORES
        for n, ref in enumerate((bq.at[:, pl.ds(0, (n_src - 1) * rows)], bkv.at[:, pl.ds(0, n_src - 1), 0],
                                 bgu.at[:, :, pl.ds(0, (n_src - 1) * rows)],
                                 bod.at[:, :, :, pl.ds(0, (o_rows + hid) // n_src * (n_src - 1))])):
            wait_out(ref, w_recv.at[0, 0], w_send.at[n])

    def kv_quarter(l, yy, half=None):
        n_src = n_x * CORES
        return bkv.at[l, pl.ds(0 if half is None else half * (n_src // 2), n_src if half is None else n_src // 2), yy]

    def kvw_copy(l, ref, kind, peer):
        remote(ref, ref, kvw_send.at[l], kvw_recv.at[l, kind], peer).start()

    def kvw_send_own(l):
        kvw_copy(l, kv_quarter(l, y), A_L, right_y)
        kvw_copy(l, kv_quarter(l, y), A_R, left_y)

    def kvw_forward(l):
        wait_in(kv_quarter(l, yl), kvw_recv.at[l, A_L], kvw_send.at[l])
        kvw_copy(l, kv_quarter(l, yl, 0), A_TOP, right_y)
        wait_in(kv_quarter(l, yr), kvw_recv.at[l, A_R], kvw_send.at[l])
        kvw_copy(l, kv_quarter(l, yr, 1), A_BOT, left_y)

    def kvw_finish(l):
        wait_in(kv_quarter(l, yo, 0), kvw_recv.at[l, A_TOP], kvw_send.at[l])
        wait_in(kv_quarter(l, yo, 1), kvw_recv.at[l, A_BOT], kvw_send.at[l])
        wait_out(bkv.at[l, :, pl.ds(0, n_y - 1)], kvw_recv.at[l, A_L], kvw_send.at[l])

    def prompt(slot, part_of=None):
        if part_of is None:
            return hbuf.at[pl.ds(pl.multiple_of(slot * seq, seq), seq)]
        half = seq // 2
        return hbuf.at[pl.ds(pl.multiple_of(slot * seq + part_of * half, half), half)]

    def a_copy(l, src, dst, kind, peer):
        remote(src, dst, a_send.at[l], a_recv.at[l, kind], peer).start()

    def a_wait(l, ref, kind):
        wait_in(ref, a_recv.at[l, kind], a_send.at[l])

    def gather_send(l):
        a_copy(l, prompt(y), prompt(y), A_L, right_y)
        a_copy(l, prompt(y), prompt(y), A_R, left_y)
        a_copy(l, prompt(y), prompt(n_y + y), A_SIB, sibling)

    def gather_forward(l):
        a_wait(l, prompt(yl), A_L)
        a_copy(l, prompt(yl, 0), prompt(yl, 0), A_TOP, right_y)
        a_copy(l, prompt(yl), prompt(n_y + yl), A_SIB, sibling)
        a_wait(l, prompt(yr), A_R)
        a_copy(l, prompt(yr, 1), prompt(yr, 1), A_BOT, left_y)
        a_copy(l, prompt(yr), prompt(n_y + yr), A_SIB, sibling)

    def gather_share(l):
        a_wait(l, prompt(yo, 0), A_TOP)
        a_copy(l, prompt(yo, 0), prompt(n_y + yo, 0), A_SIB, sibling)
        a_wait(l, prompt(yo, 1), A_BOT)
        a_copy(l, prompt(yo, 1), prompt(n_y + yo, 1), A_SIB, sibling)

    def gather_finish(l):
        a_wait(l, hbuf.at[pl.ds(keep, keep)], A_SIB)

    def gather_drain(l):
        wait_out(hbuf.at[pl.ds(0, 7 * seq)], a_recv.at[l, A_L], a_send.at[l])

    n_res = resid.shape[0]
    d_model = n_res * width

    def norm_own(l):
        total = jnp.zeros((seq, 1), F32)
        for i in range(n_res):
            total += jnp.sum(resid[i].astype(F32), axis=-1, keepdims=True)
        mean = total / d_model
        square = jnp.zeros((seq, 1), F32)
        for i in range(n_res):
            centered = resid[i].astype(F32) - mean
            square += jnp.sum(centered * centered, axis=-1, keepdims=True)
        scale = lax.rsqrt(square / d_model + LN_EPS)
        own = pl.ds(pl.multiple_of(y * seq, seq), seq)
        for i in range(n_res):
            value = (resid[i].astype(F32) - mean) * scale * gamma_ref[l:l + 1, i * width:(i + 1) * width]
            hbuf[own, i * width:(i + 1) * width] = value.astype(BF)

    def rotate(value):
        value = value.astype(F32)
        cos_all = jnp.concatenate([cos_ref[...]] * (tile // seq), axis=0)
        sin_all = jnp.concatenate([sin_ref[...]] * (tile // seq), axis=0)
        return (value * cos_all + pltpu.roll(value, head_dim // 2, 1) * sin_all).astype(BF)

    def tiles(body, n=4, size=tile):
        def step(i, carry):
            body(pl.multiple_of(i * size, size))
            return carry
        lax.fori_loop(0, n, step, 0)

    def project_q(l):
        def body(start):
            at = pl.ds(start, tile)
            acc = jnp.dot(hbuf[at, :], bq[l], preferred_element_type=F32).astype(BF)
            for n in range(heads):
                qbuf[at, n * head_dim:(n + 1) * head_dim] = rotate(acc[:, n * head_dim:(n + 1) * head_dim])
        tiles(body)

    def project_kv(l):
        def body(start):
            at = pl.ds(start, tile)
            weights = bkv[l].reshape(d_model, head_dim)
            kv = jnp.dot(hbuf[at, :], weights, preferred_element_type=F32).astype(BF)
            kvbuf[c, at, :] = jnp.where(c == 0, rotate(kv), kv)
        tiles(body)

    def kv_refs(lo):
        return kvbuf.at[c, pl.ds(lo * keep, keep)]

    def kv_exchange(l):
        for lo in range(2):
            remote(kv_refs(lo), kv_refs(1 - lo), kv_send.at[l], kv_recv.at[l], sibling).start()

    def kv_outs(l):
        own = pl.ds(pl.multiple_of(y * seq, seq), seq)
        return [pltpu.make_async_copy(kvbuf.at[0, own], k_out.at[l, 0], out_sem.at[l]),
                pltpu.make_async_copy(kvbuf.at[1, own], v_out.at[l, 0], out_sem.at[l])]

    def kv_finish(l):
        wait_in(kvbuf.at[1 - c], kv_recv.at[l], kv_send.at[l])
        for copy in kv_outs(l):
            copy.start()

    def kv_drain(l):
        wait_out(kvbuf.at[c], kv_recv.at[l], kv_send.at[l])
        both = kvbuf.at[0, pl.ds(0, 2 * seq)]
        pltpu.make_async_copy(both, both, out_sem.at[l]).wait()

    def attend():
        score_scale = head_dim ** -0.5
        allowed = lax.broadcasted_iota(jnp.int32, (seq, seq), 0) >= lax.broadcasted_iota(jnp.int32, (seq, seq), 1)

        def body(start):
            at = pl.ds(start, seq)
            key, val = kvbuf[0, at, :], kvbuf[1, at, :]
            for n in range(heads):
                query = qbuf[at, n * head_dim:(n + 1) * head_dim]
                scores = lax.dot_general(query, key, (((1,), (1,)), ((), ())), preferred_element_type=F32) * score_scale
                scores = jnp.where(allowed, scores, -jnp.inf)
                weights = jnp.exp(scores - jnp.max(scores, axis=-1, keepdims=True))
                probs = (weights / jnp.sum(weights, axis=-1, keepdims=True)).astype(BF)
                ombuf[at, n * head_dim:(n + 1) * head_dim] = jnp.dot(probs, val, preferred_element_type=F32).astype(BF)
        tiles(body, n_prompts, seq)

    def gate_up(l, j):
        def body(start):
            at = pl.ds(start, tile)
            acc = jnp.dot(hbuf[at, :], bgu[l, j], preferred_element_type=F32).astype(BF).astype(F32)
            ombuf[at, q_cols + j * g_cols:q_cols + (j + 1) * g_cols] = (jax.nn.silu(acc[:, :g_cols]) * acc[:, g_cols:]).astype(BF)
        tiles(body)

    chips = [x, xl, xr, xo]
    half_w = width

    def chunk(b, hh):
        return b * HALVES + hh

    def project_out(l, b, hh):
        k = chunk(b, hh)

        def step(i, carry):
            at = pl.ds(pl.multiple_of((1 - i) * keep, keep), keep)
            part[k, at, :] = jnp.dot(ombuf[at, :], bod[l, hh, chips[b]], preferred_element_type=F32)

            @pl.when(i == 0)
            def _():
                remote(part.at[k, pl.ds(keep, keep)], rs0.at[k], r_send.at[0], r_recv.at[k, 0], sibling).start()
            return carry
        lax.fori_loop(0, 2, step, 0)

    def of_chip_half(k, yy, side):
        return part.at[k, pl.ds(pl.multiple_of(yy * seq, seq), seq), pl.ds(side * half_w, half_w)]

    def send_near(k, target, side, half, peer):
        remote(of_chip_half(k, target, half), rs2.at[k, side, :, pl.ds(half * half_w, half_w)],
               r_send.at[2], r_recv.at[k, 3], peer).start()

    def reduce_cores(b, hh):
        k = chunk(b, hh)
        wait_in(rs0.at[k], r_recv.at[k, 0], r_send.at[0])
        part[k, 0:keep, :] += rs0[k]
        remote(of_chip_half(k, yo, 0), rs1.at[k, 0], r_send.at[1], r_recv.at[k, 1], right_y).start()
        remote(of_chip_half(k, yo, 1), rs1.at[k, 1], r_send.at[1], r_recv.at[k, 2], left_y).start()
        send_near(k, yr, 0, 1, right_y)
        send_near(k, yl, 1, 0, left_y)

    def reduce_far(b, hh):
        k = chunk(b, hh)
        for side, target, peer in ((0, yr, right_y), (1, yl, left_y)):
            wait_in(rs1.at[k, side], r_recv.at[k, 1 + side], r_send.at[1])
            at = pl.ds(pl.multiple_of(target * seq, seq), seq)
            part[k, at, side * half_w:(side + 1) * half_w] += rs1[k, side]
            send_near(k, target, side, side, peer)

    def out_copy(i):
        return pltpu.make_async_copy(resid.at[i], y_out.at[0, :, pl.ds(pl.multiple_of(i * width, width), width)],
                                     out_sem.at[layers])

    def reduce_last(l, b, hh):
        k = chunk(b, hh)
        wait_in(rs2.at[k], r_recv.at[k, 3], r_send.at[2])
        own = pl.ds(pl.multiple_of(y * seq, seq), seq)
        total = part[k, own, :] + rs2[k, 0] + rs2[k, 1]
        for core in range(CORES):
            i = (chips[b] * CORES + core) * HALVES + hh
            resid[i] = (resid[i].astype(F32) + total[:, core * width:(core + 1) * width]).astype(BF)
            if l == layers - 1:
                out_copy(i).start()

    def reduce_drain():
        for n, ref in enumerate((rs0, rs1, rs2)):
            wait_out(ref, r_recv.at[0, 0], r_send.at[n])

    issue_own(0, 0)
    for l in range(layers):
        prepare_kv(l)
    prepare(1)
    issue_own(0, 1)
    issue_own(1)
    prepare(2)
    pltpu.make_async_copy(resid, resid, raw_sem.at[2]).wait()
    for n, (table, held) in enumerate(tables):
        pltpu.make_async_copy(table, held, raw_sem.at[3 + layers + n]).wait()
    norm_own(0)
    gather_send(0)
    comm(0)
    gather_forward(0)
    gather_share(0)
    gather_finish(0)
    OWN, LEFT, RIGHT, FAR = range(4)
    rest = (SIDES,)
    for l in range(layers):
        base = l * per_layer
        last = l == layers - 1

        def ahead(p):
            while done[0] <= p:
                comm(done[0])

        ahead(base + 1)
        if l == 0:
            wait_piece(base, rest)
            kvw_send_own(l)
        project_q(l)
        ahead(base + 2)
        if l == 0:
            kvw_forward(l)
        wait_piece(base + 1, rest)
        gate_up(l, 0)
        kvw_finish(l)
        project_kv(l)
        kv_exchange(l)
        for j in range(1, GU_CHUNKS):
            ahead(base + 1 + j if last and j == GU_CHUNKS - 1 else base + 2 + j)
            wait_piece(base + 1 + j, rest)
            gate_up(l, j)
            if j == 1:
                kv_finish(l)
                attend()
        gather_drain(l)
        kv_drain(l)
        c0, c1 = base + 1 + GU_CHUNKS, base + 2 + GU_CHUNKS
        wait_piece(c0, (OWN_CHIP,))
        project_out(l, OWN, 0)
        wait_piece(c1, (OWN_CHIP,))
        project_out(l, OWN, 1)
        reduce_cores(OWN, 0)
        reduce_cores(OWN, 1)
        reduce_far(OWN, 0)
        ahead(c0)
        wait_piece(c0, (SIDES,))
        project_out(l, LEFT, 0)
        reduce_far(OWN, 1)
        project_out(l, RIGHT, 0)
        reduce_cores(LEFT, 0)
        reduce_cores(RIGHT, 0)
        reduce_last(l, OWN, 0)
        reduce_far(LEFT, 0)
        comm(c1)
        wait_piece(c1, (SIDES,))
        project_out(l, LEFT, 1)
        reduce_far(RIGHT, 0)
        reduce_last(l, OWN, 1)
        project_out(l, RIGHT, 1)
        reduce_cores(LEFT, 1)
        reduce_cores(RIGHT, 1)
        wait_piece(c0, (FAR_CHIP,))
        project_out(l, FAR, 0)
        reduce_last(l, LEFT, 0)
        reduce_far(LEFT, 1)
        reduce_far(RIGHT, 1)
        reduce_cores(FAR, 0)
        if not last:
            comm(c1 + 1)
        wait_piece(c1, (FAR_CHIP,))
        project_out(l, FAR, 1)
        reduce_far(FAR, 0)
        reduce_cores(FAR, 1)
        reduce_last(l, RIGHT, 0)
        reduce_last(l, LEFT, 1)
        reduce_last(l, RIGHT, 1)
        reduce_far(FAR, 1)
        reduce_last(l, FAR, 0)
        reduce_last(l, FAR, 1)
        reduce_drain()
        if not last:
            norm_own(l + 1)
            comm(c1 + 2)
            gather_send(l + 1)
            wait_piece(base + per_layer, rest)
            kvw_send_own(l + 1)
            gather_forward(l + 1)
            comm(c1 + 3)
            gather_share(l + 1)
            kvw_forward(l + 1)
            gather_finish(l + 1)
    drain_weights()
    pltpu.make_async_copy(resid, resid, out_sem.at[layers]).wait()


def take_over(y_in, k_in, v_in, y_out, k_out, v_out, y_held, k_held, v_held, sems):
    half = y_in.shape[1] // 2
    top, bottom = pl.ds(0, half), pl.ds(half, half)
    moves = [(y_in.at[0, top], y_held.at[top], y_out.at[0, top]), (y_in.at[0, bottom], y_held.at[bottom], y_out.at[0, bottom]),
             (k_in, k_held, k_out), (v_in, v_held, v_out)]
    loads = [pltpu.make_async_copy(src, held, sems.at[0, n]) for n, (src, held, _) in enumerate(moves)]
    stores = [pltpu.make_async_copy(held, dst, sems.at[1, n]) for n, (_, held, dst) in enumerate(moves)]
    for load in loads:
        load.start()
    for load, store in zip(loads, stores):
        load.wait()
        store.start()
    for store in stores:
        store.wait()


def run_layers(mesh_sizes, x_tokens, gamma_ln, w_q, w_kv, w_gu, w_o, w_d):
    n_x, n_y = mesh_sizes['wx'] // CORES, mesh_sizes['wy']
    assert n_x == 4 and n_y == 4 and x_tokens.shape[0] == 1
    layers, rows, q_loc = w_q.shape
    seq, d_model = x_tokens.shape[1:]
    head_dim = w_kv.shape[-1]
    hid_loc = w_gu.shape[-1]
    hid = hid_loc // CORES
    g_cols = hid // GU_CHUNKS
    q_cols = q_loc // CORES
    width = rows // HALVES
    toks = CORES * n_y * seq
    n_chunks = n_x * HALVES
    n_res = d_model // width
    cos_all, sin_all = rope_tables(seq, head_dim)
    dma = pltpu.SemaphoreType.DMA
    anywhere = pl.BlockSpec(memory_space=pl.ANY)
    cache = jax.ShapeDtypeStruct((layers, 1, seq, head_dim), BF)
    results = pl.pallas_call(
        functools.partial(layers_kernel, (layers, n_x, n_y, seq, head_dim, rows, width)),
        out_shape=(jax.ShapeDtypeStruct(x_tokens.shape, BF), cache, cache),
        in_specs=[anywhere] * 9,
        out_specs=(anywhere,) * 3,
        scratch_shapes=[
            pltpu.VMEM((layers, d_model, q_cols), BF),
            pltpu.VMEM((layers, n_x * CORES, n_y, rows // n_y, head_dim), BF),
            pltpu.VMEM((layers, GU_CHUNKS, d_model, 2 * g_cols), BF),
            pltpu.VMEM((layers, HALVES, n_x, q_cols + hid, CORES * width), BF),
            pltpu.VMEM((toks, d_model), BF),
            pltpu.VMEM((toks, q_cols), BF),
            pltpu.VMEM((2, toks, head_dim), BF),
            pltpu.VMEM((toks, q_cols + hid), BF),
            pltpu.VMEM((n_chunks, toks, CORES * width), F32),
            pltpu.VMEM((n_chunks, toks // CORES, CORES * width), F32),
            pltpu.VMEM((n_chunks, 2, seq, width), F32),
            pltpu.VMEM((n_chunks, 2, seq, CORES * width), F32),
            pltpu.VMEM((n_res, seq, width), BF),
            pltpu.VMEM((2, CORES, rows, 2, g_cols), BF),
            pltpu.VMEM((layers, rows // n_y, 2, head_dim), BF),
            pltpu.VMEM((layers, GU_CHUNKS, CORES, rows, 2 * g_cols), BF),
            pltpu.VMEM((layers, 2, rows // n_y, head_dim), BF),
            pltpu.VMEM(gamma_ln.shape, F32), pltpu.VMEM(cos_all.shape, F32), pltpu.VMEM(sin_all.shape, F32),
            dma((6 + layers,)),
            dma((4,)), dma((layers * (2 + GU_CHUNKS), 3)), dma((layers * HALVES, 5)),
            dma((layers,)), dma((layers, 4)),
            dma((layers,)), dma((layers, 5)),
            dma((layers,)), dma((layers,)),
            dma((3,)), dma((n_chunks, 4)),
            dma((layers + 1,)),
        ],
        compiler_params=pltpu.CompilerParams(collective_id=0, has_side_effects=True, vmem_limit_bytes=67043328),
    )(gamma_ln, cos_all, sin_all, x_tokens, w_q, w_kv, w_gu, w_o, w_d)
    shapes = [jax.ShapeDtypeStruct(r.shape, r.dtype) for r in results]
    return pl.pallas_call(
        take_over, out_shape=shapes, in_specs=[anywhere] * 3, out_specs=[anywhere] * 3,
        scratch_shapes=[pltpu.VMEM((seq, d_model), BF), pltpu.VMEM(cache.shape, BF), pltpu.VMEM(cache.shape, BF), dma((2, 4))],
    )(*results)


def solution(mesh):
    batch_axes = ('dp', 'wy', 'wx')
    in_specs = (P(batch_axes), P(), P(None, 'wx', 'wy'), P(None, 'wx'), P(None, 'wx', None, 'wy'), P(None, 'wy', 'wx'), P(None, 'wy', 'wx'))
    out_specs = (P(batch_axes), P(None, batch_axes), P(None, batch_axes))
    sizes = dict(mesh.shape)
    return jax.shard_map(functools.partial(run_layers, sizes), mesh=mesh, in_specs=in_specs, out_specs=out_specs, check_vma=False)
```

```python
import functools

import jax
import jax.numpy as jnp
import numpy as np
from jax import lax
from jax.experimental import pallas as pl
from jax.experimental.pallas import tpu as pltpu
from jax.sharding import PartitionSpec as P

LN_EPS = 1e-6
ROPE_BASE = 10000.0
CORES = 2
GU_CHUNKS = 4
HALVES = 2
BF, F32 = jnp.bfloat16, jnp.float32

L0, R1, SIDES, OWN_CHIP, FAR_CHIP = range(5)
A_L, A_R, A_TOP, A_BOT, A_SIB = range(5)


def rope_tables(seq_len, head_dim):
    inv_freq = np.float32(ROPE_BASE) ** (-2.0 * np.arange(head_dim // 2, dtype=np.float32) / head_dim).astype(np.float32)
    angles = np.arange(seq_len, dtype=np.float32)[:, None] * inv_freq[None, :]
    cos_tab, sin_tab = np.cos(angles.astype(np.float64)), np.sin(angles.astype(np.float64))
    return (np.concatenate([cos_tab, cos_tab], axis=-1).astype(np.float32),
            np.concatenate([-sin_tab, sin_tab], axis=-1).astype(np.float32))


def layers_kernel(dims, gamma_in, cos_in, sin_in, x_ref, wq, wkv, wgu, wo, wd,
                  y_out, k_out, v_out,
                  bq, bkv, bgu, bod, hbuf, qbuf, kvbuf, ombuf, part, rs0, rs1, rs2, resid,
                  gu_raw, kv_raw, gu_stage, kv_stage, gamma_ref, cos_ref, sin_ref, raw_sem,
                  w_send, w_recv, c_recv, kvw_send, kvw_recv, a_send, a_recv, kv_send, kv_recv, r_send, r_recv, out_sem):
    layers, n_x, n_y, seq, head_dim, rows, width = dims
    heads = wo.shape[1] // CORES // head_dim
    hid = wd.shape[1] // CORES
    o_rows = wo.shape[1] // CORES
    q_cols = heads * head_dim
    g_cols = hid // GU_CHUNKS
    n_prompts = CORES * n_y
    toks = n_prompts * seq
    keep = n_y * seq
    tile = toks // 2
    pair = keep // 2

    wx = lax.axis_index('wx')
    y = lax.axis_index('wy')
    x, c = wx // CORES, wx % CORES
    xr, xl, xo = (x + 1) % n_x, (x + n_x - 1) % n_x, (x + 2) % n_x
    yr, yl, yo = (y + 1) % n_y, (y + n_y - 1) % n_y, (y + 2) % n_y
    sibling = {'wx': x * CORES + 1 - c}
    right_y, left_y = {'wy': yr}, {'wy': yl}

    def at_x(chip, core):
        return {'wx': chip * CORES + core}

    n_gu = layers * GU_CHUNKS
    tables = ((gamma_in, gamma_ref), (cos_in, cos_ref), (sin_in, sin_ref))
    kv_rows = rows // n_y

    def gu_load(g, core):
        cols = pl.ds(core * hid + (g % GU_CHUNKS) * g_cols, g_cols)
        return pltpu.make_async_copy(wgu.at[g // GU_CHUNKS, :, :, cols], gu_raw.at[g % 2, core], raw_sem.at[g % 2])

    def kv_load(l):
        mine = pl.ds(pl.multiple_of(y * kv_rows, kv_rows), kv_rows)
        return pltpu.make_async_copy(wkv.at[l, mine], kv_raw.at[l], raw_sem.at[3 + l])

    def x_load(i):
        return pltpu.make_async_copy(x_ref.at[0, :, pl.ds(i * width, width)], resid.at[i], raw_sem.at[2])

    barrier = pltpu.get_barrier_semaphore()
    peers = [sibling, right_y, left_y] + [at_x(chip, core) for chip in (xr, xl) for core in range(CORES)]
    for peer in peers:
        pl.semaphore_signal(barrier, inc=1, device_id=peer, device_id_type=pl.DeviceIdType.MESH)
    kv_load(0).start()
    for core in range(CORES):
        gu_load(0, core).start()
    for core in range(CORES):
        gu_load(1, core).start()
    for i in range(resid.shape[0]):
        x_load(i).start()
    for n, (table, held) in enumerate(tables):
        pltpu.make_async_copy(table, held, raw_sem.at[3 + layers + n]).start()
    for l in range(1, layers):
        kv_load(l).start()
    pl.semaphore_wait(barrier, len(peers))

    def remote(src, dst, send_sem, recv_sem, peer):
        return pltpu.make_async_remote_copy(src_ref=src, dst_ref=dst, send_sem=send_sem, recv_sem=recv_sem,
                                            device_id=peer, device_id_type=pl.DeviceIdType.MESH)

    def wait_in(ref, recv_sem, send_sem):
        remote(ref, ref, send_sem, recv_sem, sibling).wait_recv()

    def wait_out(ref, recv_sem, send_sem):
        remote(ref, ref, send_sem, recv_sem, sibling).wait_send()

    order = ('q', 'kv', 'gu', 'od')
    pieces = []
    n_blocks = n_outs = 0
    for l in range(layers):
        pieces.append([('q', l, 0, n_blocks), ('kv', l, 0, n_blocks + 1)])
        n_blocks += 2
        for j in range(GU_CHUNKS):
            pieces.append([('gu', l, j, n_blocks)])
            n_blocks += 1
        for hh in range(HALVES):
            pieces.append([('od', l, hh, n_outs)])
            n_outs += 1
    per_layer = len(pieces) // layers
    issue_after = [[p + 2] for p in range(len(pieces))]
    tail = len(pieces) - HALVES
    issue_after[tail - 2] = []
    issue_after[tail - 1] = [tail + hh for hh in range(HALVES)]
    issue_after[tail:] = [[] for _ in range(HALVES)]

    def sources(block, core):
        kind, l, j, _ = block
        if kind == 'q':
            return [wq.at[l, :, pl.ds(pl.multiple_of(core * q_cols, q_cols), q_cols)]]
        if kind == 'kv':
            return [kv_stage.at[l, core]]
        if kind == 'gu':
            return [gu_stage.at[l, j, core]]
        cols = pl.ds(j * width, width)
        return [wo.at[l, pl.ds(pl.multiple_of(core * o_rows, o_rows), o_rows), cols],
                wd.at[l, pl.ds(pl.multiple_of(core * hid, hid), hid), cols]]

    def landing(block, chip, core):
        kind, l, j, _ = block
        if kind == 'kv':
            return bkv.at[l, chip * CORES + core, y]
        if kind == 'od':
            return bod.at[l, j, chip, :, pl.ds(pl.multiple_of(core * width, width), width)]
        row = pl.ds(pl.multiple_of((chip * CORES + core) * rows, rows), rows)
        return bq.at[l, row] if kind == 'q' else bgu.at[l, j, row]

    def landings(block):
        here = landing(block, x, c)
        return [here.at[pl.ds(0, o_rows)], here.at[pl.ds(o_rows, hid)]] if block[0] == 'od' else [here]

    def received(block, how):
        return c_recv.at[block[3], how] if block[0] == 'od' else w_recv.at[block[3], how]

    def prepare_kv(l):
        kv_load(l).wait()
        for core in range(CORES):
            kv_stage[l, core] = kv_raw[l, :, core, :]

    def prepare(p):
        if p >= len(pieces) or pieces[p][0][0] != 'gu':
            return
        _, l, j, _ = pieces[p][0]
        g = l * GU_CHUNKS + j
        step_rows = rows // 4
        pltpu.make_async_copy(gu_raw.at[g % 2], gu_raw.at[g % 2], raw_sem.at[g % 2]).wait()
        for core in range(CORES):
            def step(i, carry):
                at = pl.ds(pl.multiple_of(i * step_rows, step_rows), step_rows)
                for which in range(2):
                    gu_stage[l, j, core, at, which * g_cols:(which + 1) * g_cols] = gu_raw[g % 2, core, at, which, :]
                return carry
            lax.fori_loop(0, 4, step, 0)
            if g + 2 < n_gu:
                gu_load(g + 2, core).start()

    def issue_own(p, only=None):
        if p >= len(pieces):
            return
        for block in pieces[p] if only is None else [pieces[p][only]]:
            sent = w_send.at[order.index(block[0])]
            side = [SIDES * c, SIDES - c]
            near = OWN_CHIP if block[0] == 'od' else SIDES
            for core in range(CORES):
                for src, dst in zip(sources(block, core), landings(block)):
                    remote(src, dst, sent, received(block, side[0]), at_x(xr, core)).start()
                    remote(src, dst, sent, received(block, side[1]), at_x(xl, core)).start()
            for src, dst in zip(sources(block, 1 - c), landings(block)):
                remote(src, dst, sent, received(block, near), sibling).start()
            for src, dst in zip(sources(block, c), landings(block)):
                pltpu.make_async_copy(src, dst, received(block, near)).start()

    def wait_block(block, how):
        kind, l, j, _ = block
        if how in (L0, R1):
            ref = landing(block, xl, 0) if how == L0 else landing(block, xr, 1)
        elif kind == 'od':
            ref = bod.at[l, j, {SIDES: xl, OWN_CHIP: x, FAR_CHIP: xo}[how]]
        else:
            others = n_x * CORES - 2
            ref = bkv.at[l, pl.ds(0, others), y] if kind == 'kv' else (
                bq.at[l, pl.ds(0, others * rows)] if kind == 'q' else bgu.at[l, j, pl.ds(0, others * rows)])
        wait_in(ref, received(block, how), w_send.at[0])

    done = [0]

    def comm(p):
        if p >= len(pieces):
            return
        assert p == done[0]
        done[0] = p + 1
        for block in pieces[p]:
            far = FAR_CHIP if block[0] == 'od' else SIDES
            wait_block(block, L0)
            from_left = landing(block, xl, 0)
            remote(from_left, from_left, w_send.at[order.index(block[0])], received(block, far), at_x(xr, c)).start()
            wait_block(block, R1)
            from_right = landing(block, xr, 1)
            remote(from_right, from_right, w_send.at[order.index(block[0])], received(block, far), at_x(xl, c)).start()
        for later in issue_after[p]:
            issue_own(later)
        prepare(p + 3)

    def wait_piece(p, hows):
        for block in pieces[p]:
            for how in hows:
                wait_block(block, how)

    def drain_weights():
        n_src = n_x * CORES
        for n, ref in enumerate((bq.at[:, pl.ds(0, (n_src - 1) * rows)], bkv.at[:, pl.ds(0, n_src - 1), 0],
                                 bgu.at[:, :, pl.ds(0, (n_src - 1) * rows)],
                                 bod.at[:, :, :, pl.ds(0, (o_rows + hid) // n_src * (n_src - 1))])):
            wait_out(ref, w_recv.at[0, 0], w_send.at[n])

    def kv_quarter(l, yy, half=None):
        n_src = n_x * CORES
        return bkv.at[l, pl.ds(0 if half is None else half * (n_src // 2), n_src if half is None else n_src // 2), yy]

    def kvw_copy(l, ref, kind, peer):
        remote(ref, ref, kvw_send.at[l], kvw_recv.at[l, kind], peer).start()

    def kvw_send_own(l):
        kvw_copy(l, kv_quarter(l, y), A_L, right_y)
        kvw_copy(l, kv_quarter(l, y), A_R, left_y)

    def kvw_forward(l):
        wait_in(kv_quarter(l, yl), kvw_recv.at[l, A_L], kvw_send.at[l])
        kvw_copy(l, kv_quarter(l, yl, 0), A_TOP, right_y)
        wait_in(kv_quarter(l, yr), kvw_recv.at[l, A_R], kvw_send.at[l])
        kvw_copy(l, kv_quarter(l, yr, 1), A_BOT, left_y)

    def kvw_finish(l):
        wait_in(kv_quarter(l, yo, 0), kvw_recv.at[l, A_TOP], kvw_send.at[l])
        wait_in(kv_quarter(l, yo, 1), kvw_recv.at[l, A_BOT], kvw_send.at[l])
        wait_out(bkv.at[l, :, pl.ds(0, n_y - 1)], kvw_recv.at[l, A_L], kvw_send.at[l])

    def prompt(slot, part_of=None):
        if part_of is None:
            return hbuf.at[pl.ds(pl.multiple_of(slot * seq, seq), seq)]
        half = seq // 2
        return hbuf.at[pl.ds(pl.multiple_of(slot * seq + part_of * half, half), half)]

    def a_copy(l, src, dst, kind, peer):
        remote(src, dst, a_send.at[l], a_recv.at[l, kind], peer).start()

    def a_wait(l, ref, kind):
        wait_in(ref, a_recv.at[l, kind], a_send.at[l])

    def gather_send(l):
        a_copy(l, prompt(y), prompt(y), A_L, right_y)
        a_copy(l, prompt(y), prompt(y), A_R, left_y)
        a_copy(l, prompt(y), prompt(n_y + y), A_SIB, sibling)

    def gather_forward(l):
        a_wait(l, prompt(yl), A_L)
        a_copy(l, prompt(yl, 0), prompt(yl, 0), A_TOP, right_y)
        a_copy(l, prompt(yl), prompt(n_y + yl), A_SIB, sibling)
        a_wait(l, prompt(yr), A_R)
        a_copy(l, prompt(yr, 1), prompt(yr, 1), A_BOT, left_y)
        a_copy(l, prompt(yr), prompt(n_y + yr), A_SIB, sibling)

    def gather_share(l):
        a_wait(l, prompt(yo, 0), A_TOP)
        a_copy(l, prompt(yo, 0), prompt(n_y + yo, 0), A_SIB, sibling)
        a_wait(l, prompt(yo, 1), A_BOT)
        a_copy(l, prompt(yo, 1), prompt(n_y + yo, 1), A_SIB, sibling)

    def gather_finish(l):
        a_wait(l, hbuf.at[pl.ds(keep, keep)], A_SIB)

    def gather_drain(l):
        wait_out(hbuf.at[pl.ds(0, 7 * seq)], a_recv.at[l, A_L], a_send.at[l])

    n_res = resid.shape[0]
    d_model = n_res * width

    def norm_own(l):
        total = jnp.zeros((seq, 1), F32)
        for i in range(n_res):
            total += jnp.sum(resid[i].astype(F32), axis=-1, keepdims=True)
        mean = total / d_model
        square = jnp.zeros((seq, 1), F32)
        for i in range(n_res):
            centered = resid[i].astype(F32) - mean
            square += jnp.sum(centered * centered, axis=-1, keepdims=True)
        scale = lax.rsqrt(square / d_model + LN_EPS)
        own = pl.ds(pl.multiple_of(y * seq, seq), seq)
        for i in range(n_res):
            value = (resid[i].astype(F32) - mean) * scale * gamma_ref[l:l + 1, i * width:(i + 1) * width]
            hbuf[own, i * width:(i + 1) * width] = value.astype(BF)

    def rotate(value):
        value = value.astype(F32)
        cos_all = jnp.concatenate([cos_ref[...]] * (tile // seq), axis=0)
        sin_all = jnp.concatenate([sin_ref[...]] * (tile // seq), axis=0)
        return (value * cos_all + pltpu.roll(value, head_dim // 2, 1) * sin_all).astype(BF)

    def tiles(body, n=2, size=tile):
        def step(i, carry):
            body(pl.multiple_of(i * size, size))
            return carry
        lax.fori_loop(0, n, step, 0)

    def project_q(l):
        def body(start):
            at = pl.ds(start, tile)
            acc = jnp.dot(hbuf[at, :], bq[l], preferred_element_type=F32).astype(BF)
            for n in range(heads):
                qbuf[at, n * head_dim:(n + 1) * head_dim] = rotate(acc[:, n * head_dim:(n + 1) * head_dim])
        tiles(body)

    def project_kv(l):
        def body(start):
            at = pl.ds(start, tile)
            weights = bkv[l].reshape(d_model, head_dim)
            kv = jnp.dot(hbuf[at, :], weights, preferred_element_type=F32).astype(BF)
            kvbuf[c, at, :] = jnp.where(c == 0, rotate(kv), kv)
        tiles(body)

    def kv_refs(lo):
        return kvbuf.at[c, pl.ds(lo * keep, keep)]

    def kv_exchange(l):
        for lo in range(2):
            remote(kv_refs(lo), kv_refs(1 - lo), kv_send.at[l], kv_recv.at[l], sibling).start()

    def kv_outs(l):
        own = pl.ds(pl.multiple_of(y * seq, seq), seq)
        return [pltpu.make_async_copy(kvbuf.at[0, own], k_out.at[l, 0], out_sem.at[l]),
                pltpu.make_async_copy(kvbuf.at[1, own], v_out.at[l, 0], out_sem.at[l])]

    def kv_finish(l):
        wait_in(kvbuf.at[1 - c], kv_recv.at[l], kv_send.at[l])
        for copy in kv_outs(l):
            copy.start()

    def kv_drain(l):
        wait_out(kvbuf.at[c], kv_recv.at[l], kv_send.at[l])
        both = kvbuf.at[0, pl.ds(0, 2 * seq)]
        pltpu.make_async_copy(both, both, out_sem.at[l]).wait()

    def attend():
        score_scale = head_dim ** -0.5
        allowed = lax.broadcasted_iota(jnp.int32, (seq, seq), 0) >= lax.broadcasted_iota(jnp.int32, (seq, seq), 1)

        def body(start):
            at = pl.ds(start, seq)
            key, val = kvbuf[0, at, :], kvbuf[1, at, :]
            for n in range(heads):
                query = qbuf[at, n * head_dim:(n + 1) * head_dim]
                scores = lax.dot_general(query, key, (((1,), (1,)), ((), ())), preferred_element_type=F32) * score_scale
                scores = jnp.where(allowed, scores, -jnp.inf)
                weights = jnp.exp(scores - jnp.max(scores, axis=-1, keepdims=True))
                probs = (weights / jnp.sum(weights, axis=-1, keepdims=True)).astype(BF)
                ombuf[at, n * head_dim:(n + 1) * head_dim] = jnp.dot(probs, val, preferred_element_type=F32).astype(BF)
        tiles(body, n_prompts, seq)

    def gate_up(l, j):
        def body(start):
            at = pl.ds(start, tile)
            acc = jnp.dot(hbuf[at, :], bgu[l, j], preferred_element_type=F32).astype(BF).astype(F32)
            ombuf[at, q_cols + j * g_cols:q_cols + (j + 1) * g_cols] = (jax.nn.silu(acc[:, :g_cols]) * acc[:, g_cols:]).astype(BF)
        tiles(body)

    chips = [x, xl, xr, xo]
    half_w = width

    def chunk(b, hh):
        return b * HALVES + hh

    def pair_rows(n):
        return pl.multiple_of((yo // 2 + n) % 2 * pair, pair)

    def project_out(l, b, hh):
        k = chunk(b, hh)

        def step(i, carry):
            at = pl.ds(pl.multiple_of((1 - i) * keep, keep), keep)
            part[k, at, :] = jnp.dot(ombuf[at, :], bod[l, hh, chips[b]], preferred_element_type=F32)

            @pl.when(i == 0)
            def _():
                for n in range(2):
                    rows_at = pair_rows(n)
                    remote(part.at[k, pl.ds(pl.multiple_of(keep + rows_at, pair), pair)],
                           rs0.at[k, pl.ds(rows_at, pair)], r_send.at[0], r_recv.at[k, 4 * n], sibling).start()
            return carry
        lax.fori_loop(0, 2, step, 0)

    def of_chip_half(k, yy, side):
        return part.at[k, pl.ds(pl.multiple_of(yy * seq, seq), seq), pl.ds(side * half_w, half_w)]

    def send_near(k, target, side, half, peer):
        remote(of_chip_half(k, target, half), rs2.at[k, side, :, pl.ds(half * half_w, half_w)],
               r_send.at[2], r_recv.at[k, 3], peer).start()

    def reduce_cores(b, hh):
        k = chunk(b, hh)
        at = pl.ds(pair_rows(0), pair)
        wait_in(rs0.at[k, at], r_recv.at[k, 0], r_send.at[0])
        part[k, at, :] += rs0[k, at, :]
        remote(of_chip_half(k, yo, 0), rs1.at[k, 0], r_send.at[1], r_recv.at[k, 1], right_y).start()
        remote(of_chip_half(k, yo, 1), rs1.at[k, 1], r_send.at[1], r_recv.at[k, 2], left_y).start()
        at = pl.ds(pair_rows(1), pair)
        wait_in(rs0.at[k, at], r_recv.at[k, 4], r_send.at[0])
        part[k, at, :] += rs0[k, at, :]
        send_near(k, yr, 0, 1, right_y)
        send_near(k, yl, 1, 0, left_y)

    def reduce_far(b, hh):
        k = chunk(b, hh)
        for side, target, peer in ((0, yr, right_y), (1, yl, left_y)):
            wait_in(rs1.at[k, side], r_recv.at[k, 1 + side], r_send.at[1])
            at = pl.ds(pl.multiple_of(target * seq, seq), seq)
            part[k, at, side * half_w:(side + 1) * half_w] += rs1[k, side]
            send_near(k, target, side, side, peer)

    def out_copy(i):
        return pltpu.make_async_copy(resid.at[i], y_out.at[0, :, pl.ds(pl.multiple_of(i * width, width), width)],
                                     out_sem.at[layers])

    def reduce_last(l, b, hh):
        k = chunk(b, hh)
        wait_in(rs2.at[k], r_recv.at[k, 3], r_send.at[2])
        own = pl.ds(pl.multiple_of(y * seq, seq), seq)
        total = part[k, own, :] + rs2[k, 0] + rs2[k, 1]
        for core in range(CORES):
            i = (chips[b] * CORES + core) * HALVES + hh
            resid[i] = (resid[i].astype(F32) + total[:, core * width:(core + 1) * width]).astype(BF)
            if l == layers - 1:
                out_copy(i).start()

    def reduce_drain():
        for n, ref in enumerate((rs0, rs1, rs2)):
            wait_out(ref, r_recv.at[0, 0], r_send.at[n])

    issue_own(0, 0)
    for l in range(layers):
        prepare_kv(l)
    prepare(1)
    issue_own(0, 1)
    issue_own(1)
    prepare(2)
    pltpu.make_async_copy(resid, resid, raw_sem.at[2]).wait()
    for n, (table, held) in enumerate(tables):
        pltpu.make_async_copy(table, held, raw_sem.at[3 + layers + n]).wait()
    norm_own(0)
    gather_send(0)
    comm(0)
    gather_forward(0)
    gather_share(0)
    gather_finish(0)
    OWN, LEFT, RIGHT, FAR = range(4)
    rest = (SIDES,)
    for l in range(layers):
        base = l * per_layer
        last = l == layers - 1

        def ahead(p):
            while done[0] <= p:
                comm(done[0])

        ahead(base + 1)
        if l == 0:
            wait_piece(base, rest)
            kvw_send_own(l)
        project_q(l)
        ahead(base + 2)
        if l == 0:
            kvw_forward(l)
        wait_piece(base + 1, rest)
        gate_up(l, 0)
        kvw_finish(l)
        project_kv(l)
        kv_exchange(l)
        for j in range(1, GU_CHUNKS):
            ahead(base + 1 + j if last and j == GU_CHUNKS - 1 else base + 2 + j)
            wait_piece(base + 1 + j, rest)
            gate_up(l, j)
            if j == 1:
                kv_finish(l)
                attend()
        gather_drain(l)
        kv_drain(l)
        c0, c1 = base + 1 + GU_CHUNKS, base + 2 + GU_CHUNKS
        wait_piece(c0, (OWN_CHIP,))
        project_out(l, OWN, 0)
        wait_piece(c1, (OWN_CHIP,))
        project_out(l, OWN, 1)
        reduce_cores(OWN, 0)
        reduce_cores(OWN, 1)
        reduce_far(OWN, 0)
        ahead(c0)
        wait_piece(c0, (SIDES,))
        project_out(l, LEFT, 0)
        reduce_far(OWN, 1)
        project_out(l, RIGHT, 0)
        reduce_cores(LEFT, 0)
        reduce_cores(RIGHT, 0)
        reduce_last(l, OWN, 0)
        reduce_far(LEFT, 0)
        comm(c1)
        wait_piece(c1, (SIDES,))
        project_out(l, LEFT, 1)
        reduce_far(RIGHT, 0)
        reduce_last(l, OWN, 1)
        project_out(l, RIGHT, 1)
        reduce_cores(LEFT, 1)
        reduce_cores(RIGHT, 1)
        wait_piece(c0, (FAR_CHIP,))
        project_out(l, FAR, 0)
        reduce_last(l, LEFT, 0)
        reduce_far(LEFT, 1)
        reduce_far(RIGHT, 1)
        reduce_cores(FAR, 0)
        if not last:
            comm(c1 + 1)
        wait_piece(c1, (FAR_CHIP,))
        project_out(l, FAR, 1)
        reduce_far(FAR, 0)
        reduce_cores(FAR, 1)
        reduce_last(l, RIGHT, 0)
        reduce_last(l, LEFT, 1)
        reduce_last(l, RIGHT, 1)
        reduce_far(FAR, 1)
        reduce_last(l, FAR, 0)
        reduce_last(l, FAR, 1)
        reduce_drain()
        if not last:
            norm_own(l + 1)
            comm(c1 + 2)
            gather_send(l + 1)
            wait_piece(base + per_layer, rest)
            kvw_send_own(l + 1)
            gather_forward(l + 1)
            comm(c1 + 3)
            gather_share(l + 1)
            kvw_forward(l + 1)
            gather_finish(l + 1)
    drain_weights()
    pltpu.make_async_copy(resid, resid, out_sem.at[layers]).wait()


def take_over(y_in, k_in, v_in, y_out, k_out, v_out, y_held, k_held, v_held, sems):
    half = y_in.shape[1] // 2
    top, bottom = pl.ds(0, half), pl.ds(half, half)
    moves = [(y_in.at[0, top], y_held.at[top], y_out.at[0, top]), (y_in.at[0, bottom], y_held.at[bottom], y_out.at[0, bottom]),
             (k_in, k_held, k_out), (v_in, v_held, v_out)]
    loads = [pltpu.make_async_copy(src, held, sems.at[0, n]) for n, (src, held, _) in enumerate(moves)]
    stores = [pltpu.make_async_copy(held, dst, sems.at[1, n]) for n, (_, held, dst) in enumerate(moves)]
    for load in loads:
        load.start()
    for load, store in zip(loads, stores):
        load.wait()
        store.start()
    for store in stores:
        store.wait()


def run_layers(mesh_sizes, x_tokens, gamma_ln, w_q, w_kv, w_gu, w_o, w_d):
    n_x, n_y = mesh_sizes['wx'] // CORES, mesh_sizes['wy']
    assert n_x == 4 and n_y == 4 and x_tokens.shape[0] == 1
    layers, rows, q_loc = w_q.shape
    seq, d_model = x_tokens.shape[1:]
    head_dim = w_kv.shape[-1]
    hid_loc = w_gu.shape[-1]
    hid = hid_loc // CORES
    g_cols = hid // GU_CHUNKS
    q_cols = q_loc // CORES
    width = rows // HALVES
    toks = CORES * n_y * seq
    n_chunks = n_x * HALVES
    n_res = d_model // width
    cos_all, sin_all = rope_tables(seq, head_dim)
    dma = pltpu.SemaphoreType.DMA
    anywhere = pl.BlockSpec(memory_space=pl.ANY)
    cache = jax.ShapeDtypeStruct((layers, 1, seq, head_dim), BF)
    results = pl.pallas_call(
        functools.partial(layers_kernel, (layers, n_x, n_y, seq, head_dim, rows, width)),
        out_shape=(jax.ShapeDtypeStruct(x_tokens.shape, BF), cache, cache),
        in_specs=[anywhere] * 9,
        out_specs=(anywhere,) * 3,
        scratch_shapes=[
            pltpu.VMEM((layers, d_model, q_cols), BF),
            pltpu.VMEM((layers, n_x * CORES, n_y, rows // n_y, head_dim), BF),
            pltpu.VMEM((layers, GU_CHUNKS, d_model, 2 * g_cols), BF),
            pltpu.VMEM((layers, HALVES, n_x, q_cols + hid, CORES * width), BF),
            pltpu.VMEM((toks, d_model), BF),
            pltpu.VMEM((toks, q_cols), BF),
            pltpu.VMEM((2, toks, head_dim), BF),
            pltpu.VMEM((toks, q_cols + hid), BF),
            pltpu.VMEM((n_chunks, toks, CORES * width), F32),
            pltpu.VMEM((n_chunks, toks // CORES, CORES * width), F32),
            pltpu.VMEM((n_chunks, 2, seq, width), F32),
            pltpu.VMEM((n_chunks, 2, seq, CORES * width), F32),
            pltpu.VMEM((n_res, seq, width), BF),
            pltpu.VMEM((2, CORES, rows, 2, g_cols), BF),
            pltpu.VMEM((layers, rows // n_y, 2, head_dim), BF),
            pltpu.VMEM((layers, GU_CHUNKS, CORES, rows, 2 * g_cols), BF),
            pltpu.VMEM((layers, 2, rows // n_y, head_dim), BF),
            pltpu.VMEM(gamma_ln.shape, F32), pltpu.VMEM(cos_all.shape, F32), pltpu.VMEM(sin_all.shape, F32),
            dma((6 + layers,)),
            dma((4,)), dma((layers * (2 + GU_CHUNKS), 3)), dma((layers * HALVES, 5)),
            dma((layers,)), dma((layers, 4)),
            dma((layers,)), dma((layers, 5)),
            dma((layers,)), dma((layers,)),
            dma((3,)), dma((n_chunks, 5)),
            dma((layers + 1,)),
        ],
        compiler_params=pltpu.CompilerParams(collective_id=0, has_side_effects=True, vmem_limit_bytes=67043328),
    )(gamma_ln, cos_all, sin_all, x_tokens, w_q, w_kv, w_gu, w_o, w_d)
    shapes = [jax.ShapeDtypeStruct(r.shape, r.dtype) for r in results]
    return pl.pallas_call(
        take_over, out_shape=shapes, in_specs=[anywhere] * 3, out_specs=[anywhere] * 3,
        scratch_shapes=[pltpu.VMEM((seq, d_model), BF), pltpu.VMEM(cache.shape, BF), pltpu.VMEM(cache.shape, BF), dma((2, 4))],
    )(*results)


def solution(mesh):
    batch_axes = ('dp', 'wy', 'wx')
    in_specs = (P(batch_axes), P(), P(None, 'wx', 'wy'), P(None, 'wx'), P(None, 'wx', None, 'wy'), P(None, 'wy', 'wx'), P(None, 'wy', 'wx'))
    out_specs = (P(batch_axes), P(None, batch_axes), P(None, batch_axes))
    sizes = dict(mesh.shape)
    return jax.shard_map(functools.partial(run_layers, sizes), mesh=mesh, in_specs=in_specs, out_specs=out_specs, check_vma=False)
```

```python
import functools

import jax
import jax.numpy as jnp
import numpy as np
from jax import lax
from jax.experimental import pallas as pl
from jax.experimental.pallas import tpu as pltpu
from jax.sharding import PartitionSpec as P

LN_EPS = 1e-6
ROPE_BASE = 10000.0
CORES = 2
GU_CHUNKS = 4
HALVES = 2
BF, F32 = jnp.bfloat16, jnp.float32

L0, R1, SIDES, OWN_CHIP, FAR_CHIP = range(5)
A_L, A_R, A_TOP, A_BOT, A_SIB = range(5)


def rope_tables(seq_len, head_dim):
    inv_freq = np.float32(ROPE_BASE) ** (-2.0 * np.arange(head_dim // 2, dtype=np.float32) / head_dim).astype(np.float32)
    angles = np.arange(seq_len, dtype=np.float32)[:, None] * inv_freq[None, :]
    cos_tab, sin_tab = np.cos(angles.astype(np.float64)), np.sin(angles.astype(np.float64))
    return (np.concatenate([cos_tab, cos_tab], axis=-1).astype(np.float32),
            np.concatenate([-sin_tab, sin_tab], axis=-1).astype(np.float32))


def layers_kernel(dims, gamma_in, cos_in, sin_in, x_ref, wq, wkv, wgu, wo, wd,
                  y_out, k_out, v_out,
                  bq, bkv, bgu, bod, hbuf, qbuf, kvbuf, ombuf, part, rs0, rs1, rs2, resid,
                  gu_raw, kv_raw, gu_stage, kv_stage, gamma_ref, cos_ref, sin_ref, raw_sem,
                  w_send, w_recv, c_recv, kvw_send, kvw_recv, a_send, a_recv, kv_send, kv_recv, r_send, r_recv, out_sem):
    layers, n_x, n_y, seq, head_dim, rows, width = dims
    heads = wo.shape[1] // CORES // head_dim
    hid = wd.shape[1] // CORES
    o_rows = wo.shape[1] // CORES
    q_cols = heads * head_dim
    g_cols = hid // GU_CHUNKS
    n_prompts = CORES * n_y
    toks = n_prompts * seq
    keep = n_y * seq
    tile = toks // 2
    pair = keep // 2

    wx = lax.axis_index('wx')
    y = lax.axis_index('wy')
    x, c = wx // CORES, wx % CORES
    xr, xl, xo = (x + 1) % n_x, (x + n_x - 1) % n_x, (x + 2) % n_x
    yr, yl, yo = (y + 1) % n_y, (y + n_y - 1) % n_y, (y + 2) % n_y
    sibling = {'wx': x * CORES + 1 - c}
    right_y, left_y = {'wy': yr}, {'wy': yl}

    def at_x(chip, core):
        return {'wx': chip * CORES + core}

    n_gu = layers * GU_CHUNKS
    tables = ((gamma_in, gamma_ref), (cos_in, cos_ref), (sin_in, sin_ref))
    kv_rows = rows // n_y

    def gu_load(g, core):
        cols = pl.ds(core * hid + (g % GU_CHUNKS) * g_cols, g_cols)
        return pltpu.make_async_copy(wgu.at[g // GU_CHUNKS, :, :, cols], gu_raw.at[g % 2, core], raw_sem.at[g % 2])

    def kv_load(l):
        mine = pl.ds(pl.multiple_of(y * kv_rows, kv_rows), kv_rows)
        return pltpu.make_async_copy(wkv.at[l, mine], kv_raw.at[l], raw_sem.at[3 + l])

    def x_load(i):
        return pltpu.make_async_copy(x_ref.at[0, :, pl.ds(i * width, width)], resid.at[i], raw_sem.at[2])

    barrier = pltpu.get_barrier_semaphore()
    peers = [sibling, right_y, left_y] + [at_x(chip, core) for chip in (xr, xl) for core in range(CORES)]
    for peer in peers:
        pl.semaphore_signal(barrier, inc=1, device_id=peer, device_id_type=pl.DeviceIdType.MESH)
    kv_load(0).start()
    for core in range(CORES):
        gu_load(0, core).start()
    for core in range(CORES):
        gu_load(1, core).start()
    for i in range(resid.shape[0]):
        x_load(i).start()
    for n, (table, held) in enumerate(tables):
        pltpu.make_async_copy(table, held, raw_sem.at[3 + layers + n]).start()
    for l in range(1, layers):
        kv_load(l).start()
    pl.semaphore_wait(barrier, len(peers))

    def remote(src, dst, send_sem, recv_sem, peer):
        return pltpu.make_async_remote_copy(src_ref=src, dst_ref=dst, send_sem=send_sem, recv_sem=recv_sem,
                                            device_id=peer, device_id_type=pl.DeviceIdType.MESH)

    def wait_in(ref, recv_sem, send_sem):
        remote(ref, ref, send_sem, recv_sem, sibling).wait_recv()

    def wait_out(ref, recv_sem, send_sem):
        remote(ref, ref, send_sem, recv_sem, sibling).wait_send()

    order = ('q', 'kv', 'gu', 'od')
    pieces = []
    n_blocks = n_outs = 0
    for l in range(layers):
        pieces.append([('q', l, 0, n_blocks), ('kv', l, 0, n_blocks + 1)])
        n_blocks += 2
        for j in range(GU_CHUNKS):
            pieces.append([('gu', l, j, n_blocks)])
            n_blocks += 1
        for hh in range(HALVES):
            pieces.append([('od', l, hh, n_outs)])
            n_outs += 1
    per_layer = len(pieces) // layers
    issue_after = [[p + 2] for p in range(len(pieces))]
    tail = len(pieces) - HALVES
    issue_after[tail - 2] = []
    issue_after[tail - 1] = [tail + hh for hh in range(HALVES)]
    issue_after[tail:] = [[] for _ in range(HALVES)]

    def sources(block, core):
        kind, l, j, _ = block
        if kind == 'q':
            return [wq.at[l, :, pl.ds(pl.multiple_of(core * q_cols, q_cols), q_cols)]]
        if kind == 'kv':
            return [kv_stage.at[l, core]]
        if kind == 'gu':
            return [gu_stage.at[l, j, core]]
        cols = pl.ds(j * width, width)
        return [wo.at[l, pl.ds(pl.multiple_of(core * o_rows, o_rows), o_rows), cols],
                wd.at[l, pl.ds(pl.multiple_of(core * hid, hid), hid), cols]]

    def landing(block, chip, core):
        kind, l, j, _ = block
        if kind == 'kv':
            return bkv.at[l, chip * CORES + core, y]
        if kind == 'od':
            return bod.at[l, j, chip, :, pl.ds(pl.multiple_of(core * width, width), width)]
        row = pl.ds(pl.multiple_of((chip * CORES + core) * rows, rows), rows)
        return bq.at[l, row] if kind == 'q' else bgu.at[l, j, row]

    def landings(block):
        here = landing(block, x, c)
        return [here.at[pl.ds(0, o_rows)], here.at[pl.ds(o_rows, hid)]] if block[0] == 'od' else [here]

    def received(block, how):
        return c_recv.at[block[3], how] if block[0] == 'od' else w_recv.at[block[3], how]

    def prepare_kv(l):
        kv_load(l).wait()
        for core in range(CORES):
            kv_stage[l, core] = kv_raw[l, :, core, :]

    def prepare(p):
        if p >= len(pieces) or pieces[p][0][0] != 'gu':
            return
        _, l, j, _ = pieces[p][0]
        g = l * GU_CHUNKS + j
        step_rows = rows // 4
        pltpu.make_async_copy(gu_raw.at[g % 2], gu_raw.at[g % 2], raw_sem.at[g % 2]).wait()
        for core in range(CORES):
            def step(i, carry):
                at = pl.ds(pl.multiple_of(i * step_rows, step_rows), step_rows)
                for which in range(2):
                    gu_stage[l, j, core, at, which * g_cols:(which + 1) * g_cols] = gu_raw[g % 2, core, at, which, :]
                return carry
            lax.fori_loop(0, 4, step, 0)
            if g + 2 < n_gu:
                gu_load(g + 2, core).start()

    def issue_own(p, only=None):
        if p >= len(pieces):
            return
        for block in pieces[p] if only is None else [pieces[p][only]]:
            sent = w_send.at[order.index(block[0])]
            side = [SIDES * c, SIDES - c]
            near = OWN_CHIP if block[0] == 'od' else SIDES
            for core in range(CORES):
                for src, dst in zip(sources(block, core), landings(block)):
                    remote(src, dst, sent, received(block, side[0]), at_x(xr, core)).start()
                    remote(src, dst, sent, received(block, side[1]), at_x(xl, core)).start()
            for src, dst in zip(sources(block, 1 - c), landings(block)):
                remote(src, dst, sent, received(block, near), sibling).start()
            for src, dst in zip(sources(block, c), landings(block)):
                pltpu.make_async_copy(src, dst, received(block, near)).start()

    def wait_block(block, how):
        kind, l, j, _ = block
        if how in (L0, R1):
            ref = landing(block, xl, 0) if how == L0 else landing(block, xr, 1)
        elif kind == 'od':
            ref = bod.at[l, j, {SIDES: xl, OWN_CHIP: x, FAR_CHIP: xo}[how]]
        else:
            others = n_x * CORES - 2
            ref = bkv.at[l, pl.ds(0, others), y] if kind == 'kv' else (
                bq.at[l, pl.ds(0, others * rows)] if kind == 'q' else bgu.at[l, j, pl.ds(0, others * rows)])
        wait_in(ref, received(block, how), w_send.at[0])

    done = [0]

    def comm(p):
        if p >= len(pieces):
            return
        assert p == done[0]
        done[0] = p + 1
        for block in pieces[p]:
            far = FAR_CHIP if block[0] == 'od' else SIDES
            wait_block(block, L0)
            from_left = landing(block, xl, 0)
            remote(from_left, from_left, w_send.at[order.index(block[0])], received(block, far), at_x(xr, c)).start()
            wait_block(block, R1)
            from_right = landing(block, xr, 1)
            remote(from_right, from_right, w_send.at[order.index(block[0])], received(block, far), at_x(xl, c)).start()
        for later in issue_after[p]:
            issue_own(later)
        prepare(p + 3)

    def wait_piece(p, hows):
        for block in pieces[p]:
            for how in hows:
                wait_block(block, how)

    def drain_weights():
        n_src = n_x * CORES
        for n, ref in enumerate((bq.at[:, pl.ds(0, (n_src - 1) * rows)], bkv.at[:, pl.ds(0, n_src - 1), 0],
                                 bgu.at[:, :, pl.ds(0, (n_src - 1) * rows)],
                                 bod.at[:, :, :, pl.ds(0, (o_rows + hid) // n_src * (n_src - 1))])):
            wait_out(ref, w_recv.at[0, 0], w_send.at[n])

    def kv_quarter(l, yy, half=None):
        n_src = n_x * CORES
        return bkv.at[l, pl.ds(0 if half is None else half * (n_src // 2), n_src if half is None else n_src // 2), yy]

    def kvw_copy(l, ref, kind, peer):
        remote(ref, ref, kvw_send.at[l], kvw_recv.at[l, kind], peer).start()

    def kvw_send_own(l):
        kvw_copy(l, kv_quarter(l, y), A_L, right_y)
        kvw_copy(l, kv_quarter(l, y), A_R, left_y)

    def kvw_forward(l):
        wait_in(kv_quarter(l, yl), kvw_recv.at[l, A_L], kvw_send.at[l])
        kvw_copy(l, kv_quarter(l, yl, 0), A_TOP, right_y)
        wait_in(kv_quarter(l, yr), kvw_recv.at[l, A_R], kvw_send.at[l])
        kvw_copy(l, kv_quarter(l, yr, 1), A_BOT, left_y)

    def kvw_finish(l):
        wait_in(kv_quarter(l, yo, 0), kvw_recv.at[l, A_TOP], kvw_send.at[l])
        wait_in(kv_quarter(l, yo, 1), kvw_recv.at[l, A_BOT], kvw_send.at[l])
        wait_out(bkv.at[l, :, pl.ds(0, n_y - 1)], kvw_recv.at[l, A_L], kvw_send.at[l])

    def prompt(slot, part_of=None):
        if part_of is None:
            return hbuf.at[pl.ds(pl.multiple_of(slot * seq, seq), seq)]
        half = seq // 2
        return hbuf.at[pl.ds(pl.multiple_of(slot * seq + part_of * half, half), half)]

    def a_copy(l, src, dst, kind, peer):
        remote(src, dst, a_send.at[l], a_recv.at[l, kind], peer).start()

    def a_wait(l, ref, kind):
        wait_in(ref, a_recv.at[l, kind], a_send.at[l])

    def gather_send(l):
        a_copy(l, prompt(y), prompt(y), A_L, right_y)
        a_copy(l, prompt(y), prompt(y), A_R, left_y)
        a_copy(l, prompt(y), prompt(n_y + y), A_SIB, sibling)

    def gather_forward(l):
        a_wait(l, prompt(yl), A_L)
        a_copy(l, prompt(yl, 0), prompt(yl, 0), A_TOP, right_y)
        a_copy(l, prompt(yl), prompt(n_y + yl), A_SIB, sibling)
        a_wait(l, prompt(yr), A_R)
        a_copy(l, prompt(yr, 1), prompt(yr, 1), A_BOT, left_y)
        a_copy(l, prompt(yr), prompt(n_y + yr), A_SIB, sibling)

    def gather_share(l):
        a_wait(l, prompt(yo, 0), A_TOP)
        a_copy(l, prompt(yo, 0), prompt(n_y + yo, 0), A_SIB, sibling)
        a_wait(l, prompt(yo, 1), A_BOT)
        a_copy(l, prompt(yo, 1), prompt(n_y + yo, 1), A_SIB, sibling)

    def gather_finish(l):
        a_wait(l, hbuf.at[pl.ds(keep, keep)], A_SIB)

    def gather_drain(l):
        wait_out(hbuf.at[pl.ds(0, 7 * seq)], a_recv.at[l, A_L], a_send.at[l])

    n_res = resid.shape[0]
    d_model = n_res * width

    def norm_own(l):
        total = jnp.zeros((seq, 1), F32)
        for i in range(n_res):
            total += jnp.sum(resid[i].astype(F32), axis=-1, keepdims=True)
        mean = total / d_model
        square = jnp.zeros((seq, 1), F32)
        for i in range(n_res):
            centered = resid[i].astype(F32) - mean
            square += jnp.sum(centered * centered, axis=-1, keepdims=True)
        scale = lax.rsqrt(square / d_model + LN_EPS)
        own = pl.ds(pl.multiple_of(y * seq, seq), seq)
        for i in range(n_res):
            value = (resid[i].astype(F32) - mean) * scale * gamma_ref[l:l + 1, i * width:(i + 1) * width]
            hbuf[own, i * width:(i + 1) * width] = value.astype(BF)

    def rotate(value):
        value = value.astype(F32)
        cos_all = jnp.concatenate([cos_ref[...]] * (tile // seq), axis=0)
        sin_all = jnp.concatenate([sin_ref[...]] * (tile // seq), axis=0)
        return (value * cos_all + pltpu.roll(value, head_dim // 2, 1) * sin_all).astype(BF)

    def tiles(body, n=2, size=tile):
        def step(i, carry):
            body(pl.multiple_of(i * size, size))
            return carry
        lax.fori_loop(0, n, step, 0)

    def project_q(l):
        def body(start):
            at = pl.ds(start, tile)
            acc = jnp.dot(hbuf[at, :], bq[l], preferred_element_type=F32).astype(BF)
            for n in range(heads):
                qbuf[at, n * head_dim:(n + 1) * head_dim] = rotate(acc[:, n * head_dim:(n + 1) * head_dim])
        tiles(body)

    def project_kv(l):
        def body(start):
            at = pl.ds(start, tile)
            weights = bkv[l].reshape(d_model, head_dim)
            kv = jnp.dot(hbuf[at, :], weights, preferred_element_type=F32).astype(BF)
            kvbuf[c, at, :] = jnp.where(c == 0, rotate(kv), kv)
        tiles(body)

    def kv_refs(lo):
        return kvbuf.at[c, pl.ds(lo * keep, keep)]

    def kv_exchange(l):
        for lo in range(2):
            remote(kv_refs(lo), kv_refs(1 - lo), kv_send.at[l], kv_recv.at[l], sibling).start()

    def kv_outs(l):
        own = pl.ds(pl.multiple_of(y * seq, seq), seq)
        return [pltpu.make_async_copy(kvbuf.at[0, own], k_out.at[l, 0], out_sem.at[l]),
                pltpu.make_async_copy(kvbuf.at[1, own], v_out.at[l, 0], out_sem.at[l])]

    def kv_finish(l):
        wait_in(kvbuf.at[1 - c], kv_recv.at[l], kv_send.at[l])
        for copy in kv_outs(l):
            copy.start()

    def kv_drain(l):
        wait_out(kvbuf.at[c], kv_recv.at[l], kv_send.at[l])
        both = kvbuf.at[0, pl.ds(0, 2 * seq)]
        pltpu.make_async_copy(both, both, out_sem.at[l]).wait()

    def attend():
        score_scale = head_dim ** -0.5
        allowed = lax.broadcasted_iota(jnp.int32, (seq, seq), 0) >= lax.broadcasted_iota(jnp.int32, (seq, seq), 1)

        def body(start):
            at = pl.ds(start, seq)
            key, val = kvbuf[0, at, :], kvbuf[1, at, :]
            for n in range(heads):
                query = qbuf[at, n * head_dim:(n + 1) * head_dim]
                scores = lax.dot_general(query, key, (((1,), (1,)), ((), ())), preferred_element_type=F32) * score_scale
                scores = jnp.where(allowed, scores, -jnp.inf)
                weights = jnp.exp(scores - jnp.max(scores, axis=-1, keepdims=True))
                probs = (weights / jnp.sum(weights, axis=-1, keepdims=True)).astype(BF)
                ombuf[at, n * head_dim:(n + 1) * head_dim] = jnp.dot(probs, val, preferred_element_type=F32).astype(BF)
        tiles(body, n_prompts, seq)

    def gate_up(l, j):
        def body(start):
            at = pl.ds(start, tile)
            acc = jnp.dot(hbuf[at, :], bgu[l, j], preferred_element_type=F32).astype(BF).astype(F32)
            ombuf[at, q_cols + j * g_cols:q_cols + (j + 1) * g_cols] = (jax.nn.silu(acc[:, :g_cols]) * acc[:, g_cols:]).astype(BF)
        tiles(body)

    chips = [x, xl, xr, xo]
    half_w = width

    def chunk(b, hh):
        return b * HALVES + hh

    def pair_rows(n):
        return pl.multiple_of((yo // 2 + n) % 2 * pair, pair)

    def project_out(l, b, hh):
        k = chunk(b, hh)

        def step(i, carry):
            at = pl.ds(pl.multiple_of((1 - i) * keep, keep), keep)
            part[k, at, :] = jnp.dot(ombuf[at, :], bod[l, hh, chips[b]], preferred_element_type=F32)

            @pl.when(i == 0)
            def _():
                for n in range(2):
                    rows_at = pair_rows(n)
                    remote(part.at[k, pl.ds(pl.multiple_of(keep + rows_at, pair), pair)],
                           rs0.at[k, pl.ds(rows_at, pair)], r_send.at[0], r_recv.at[k, 4 * n], sibling).start()
            return carry
        lax.fori_loop(0, 2, step, 0)

    def of_chip_half(k, yy, side):
        return part.at[k, pl.ds(pl.multiple_of(yy * seq, seq), seq), pl.ds(side * half_w, half_w)]

    def send_near(k, target, side, half, peer):
        remote(of_chip_half(k, target, half), rs2.at[k, side, :, pl.ds(half * half_w, half_w)],
               r_send.at[2], r_recv.at[k, 3], peer).start()

    def reduce_cores(b, hh):
        k = chunk(b, hh)
        at = pl.ds(pair_rows(0), pair)
        wait_in(rs0.at[k, at], r_recv.at[k, 0], r_send.at[0])
        part[k, at, :] += rs0[k, at, :]
        remote(of_chip_half(k, yo, 0), rs1.at[k, 0], r_send.at[1], r_recv.at[k, 1], right_y).start()
        remote(of_chip_half(k, yo, 1), rs1.at[k, 1], r_send.at[1], r_recv.at[k, 2], left_y).start()
        at = pl.ds(pair_rows(1), pair)
        wait_in(rs0.at[k, at], r_recv.at[k, 4], r_send.at[0])
        part[k, at, :] += rs0[k, at, :]
        send_near(k, yr, 0, 1, right_y)
        send_near(k, yl, 1, 0, left_y)

    def reduce_far(b, hh):
        k = chunk(b, hh)
        for side, target, peer in ((0, yr, right_y), (1, yl, left_y)):
            wait_in(rs1.at[k, side], r_recv.at[k, 1 + side], r_send.at[1])
            at = pl.ds(pl.multiple_of(target * seq, seq), seq)
            part[k, at, side * half_w:(side + 1) * half_w] += rs1[k, side]
            send_near(k, target, side, side, peer)

    def out_copy(i):
        return pltpu.make_async_copy(resid.at[i], y_out.at[0, :, pl.ds(pl.multiple_of(i * width, width), width)],
                                     out_sem.at[layers])

    def reduce_last(l, b, hh):
        k = chunk(b, hh)
        wait_in(rs2.at[k], r_recv.at[k, 3], r_send.at[2])
        own = pl.ds(pl.multiple_of(y * seq, seq), seq)
        total = part[k, own, :] + rs2[k, 0] + rs2[k, 1]
        for core in range(CORES):
            i = (chips[b] * CORES + core) * HALVES + hh
            resid[i] = (resid[i].astype(F32) + total[:, core * width:(core + 1) * width]).astype(BF)
            if l == layers - 1:
                out_copy(i).start()

    def reduce_drain():
        for n, ref in enumerate((rs0, rs1, rs2)):
            wait_out(ref, r_recv.at[0, 0], r_send.at[n])

    issue_own(0, 0)
    for l in range(layers):
        prepare_kv(l)
    prepare(1)
    issue_own(0, 1)
    issue_own(1)
    prepare(2)
    pltpu.make_async_copy(resid, resid, raw_sem.at[2]).wait()
    for n, (table, held) in enumerate(tables):
        pltpu.make_async_copy(table, held, raw_sem.at[3 + layers + n]).wait()
    norm_own(0)
    gather_send(0)
    comm(0)
    gather_forward(0)
    gather_share(0)
    gather_finish(0)
    OWN, LEFT, RIGHT, FAR = range(4)
    rest = (SIDES,)
    for l in range(layers):
        base = l * per_layer
        last = l == layers - 1

        def ahead(p):
            while done[0] <= p:
                comm(done[0])

        ahead(base + 1)
        if l == 0:
            wait_piece(base, rest)
            kvw_send_own(l)
        project_q(l)
        ahead(base + 2)
        if l == 0:
            kvw_forward(l)
        wait_piece(base + 1, rest)
        gate_up(l, 0)
        kvw_finish(l)
        project_kv(l)
        kv_exchange(l)
        for j in range(1, GU_CHUNKS):
            ahead(base + 1 + j if last and j == GU_CHUNKS - 1 else base + 2 + j)
            wait_piece(base + 1 + j, rest)
            gate_up(l, j)
            if j == 1:
                kv_finish(l)
                attend()
        gather_drain(l)
        kv_drain(l)
        c0, c1 = base + 1 + GU_CHUNKS, base + 2 + GU_CHUNKS
        wait_piece(c0, (OWN_CHIP,))
        project_out(l, OWN, 0)
        wait_piece(c1, (OWN_CHIP,))
        project_out(l, OWN, 1)
        reduce_cores(OWN, 0)
        reduce_cores(OWN, 1)
        reduce_far(OWN, 0)
        reduce_far(OWN, 1)
        ahead(c0)
        wait_piece(c0, (SIDES,))
        project_out(l, LEFT, 0)
        project_out(l, RIGHT, 0)
        reduce_cores(LEFT, 0)
        reduce_cores(RIGHT, 0)
        reduce_last(l, OWN, 0)
        reduce_far(LEFT, 0)
        reduce_far(RIGHT, 0)
        comm(c1)
        wait_piece(c1, (SIDES,))
        project_out(l, LEFT, 1)
        reduce_last(l, OWN, 1)
        project_out(l, RIGHT, 1)
        reduce_cores(LEFT, 1)
        reduce_cores(RIGHT, 1)
        wait_piece(c0, (FAR_CHIP,))
        project_out(l, FAR, 0)
        reduce_last(l, LEFT, 0)
        reduce_far(LEFT, 1)
        reduce_far(RIGHT, 1)
        reduce_cores(FAR, 0)
        if not last:
            comm(c1 + 1)
        wait_piece(c1, (FAR_CHIP,))
        project_out(l, FAR, 1)
        reduce_far(FAR, 0)
        reduce_cores(FAR, 1)
        reduce_last(l, RIGHT, 0)
        reduce_last(l, LEFT, 1)
        reduce_last(l, RIGHT, 1)
        reduce_far(FAR, 1)
        reduce_last(l, FAR, 0)
        reduce_last(l, FAR, 1)
        reduce_drain()
        if not last:
            norm_own(l + 1)
            comm(c1 + 2)
            gather_send(l + 1)
            wait_piece(base + per_layer, rest)
            kvw_send_own(l + 1)
            gather_forward(l + 1)
            comm(c1 + 3)
            gather_share(l + 1)
            kvw_forward(l + 1)
            gather_finish(l + 1)
    drain_weights()
    pltpu.make_async_copy(resid, resid, out_sem.at[layers]).wait()


def take_over(y_in, k_in, v_in, y_out, k_out, v_out, y_held, k_held, v_held, sems):
    half = y_in.shape[1] // 2
    top, bottom = pl.ds(0, half), pl.ds(half, half)
    moves = [(y_in.at[0, top], y_held.at[top], y_out.at[0, top]), (y_in.at[0, bottom], y_held.at[bottom], y_out.at[0, bottom]),
             (k_in, k_held, k_out), (v_in, v_held, v_out)]
    loads = [pltpu.make_async_copy(src, held, sems.at[0, n]) for n, (src, held, _) in enumerate(moves)]
    stores = [pltpu.make_async_copy(held, dst, sems.at[1, n]) for n, (_, held, dst) in enumerate(moves)]
    for load in loads:
        load.start()
    for load, store in zip(loads, stores):
        load.wait()
        store.start()
    for store in stores:
        store.wait()


def run_layers(mesh_sizes, x_tokens, gamma_ln, w_q, w_kv, w_gu, w_o, w_d):
    n_x, n_y = mesh_sizes['wx'] // CORES, mesh_sizes['wy']
    assert n_x == 4 and n_y == 4 and x_tokens.shape[0] == 1
    layers, rows, q_loc = w_q.shape
    seq, d_model = x_tokens.shape[1:]
    head_dim = w_kv.shape[-1]
    hid_loc = w_gu.shape[-1]
    hid = hid_loc // CORES
    g_cols = hid // GU_CHUNKS
    q_cols = q_loc // CORES
    width = rows // HALVES
    toks = CORES * n_y * seq
    n_chunks = n_x * HALVES
    n_res = d_model // width
    cos_all, sin_all = rope_tables(seq, head_dim)
    dma = pltpu.SemaphoreType.DMA
    anywhere = pl.BlockSpec(memory_space=pl.ANY)
    cache = jax.ShapeDtypeStruct((layers, 1, seq, head_dim), BF)
    results = pl.pallas_call(
        functools.partial(layers_kernel, (layers, n_x, n_y, seq, head_dim, rows, width)),
        out_shape=(jax.ShapeDtypeStruct(x_tokens.shape, BF), cache, cache),
        in_specs=[anywhere] * 9,
        out_specs=(anywhere,) * 3,
        scratch_shapes=[
            pltpu.VMEM((layers, d_model, q_cols), BF),
            pltpu.VMEM((layers, n_x * CORES, n_y, rows // n_y, head_dim), BF),
            pltpu.VMEM((layers, GU_CHUNKS, d_model, 2 * g_cols), BF),
            pltpu.VMEM((layers, HALVES, n_x, q_cols + hid, CORES * width), BF),
            pltpu.VMEM((toks, d_model), BF),
            pltpu.VMEM((toks, q_cols), BF),
            pltpu.VMEM((2, toks, head_dim), BF),
            pltpu.VMEM((toks, q_cols + hid), BF),
            pltpu.VMEM((n_chunks, toks, CORES * width), F32),
            pltpu.VMEM((n_chunks, toks // CORES, CORES * width), F32),
            pltpu.VMEM((n_chunks, 2, seq, width), F32),
            pltpu.VMEM((n_chunks, 2, seq, CORES * width), F32),
            pltpu.VMEM((n_res, seq, width), BF),
            pltpu.VMEM((2, CORES, rows, 2, g_cols), BF),
            pltpu.VMEM((layers, rows // n_y, 2, head_dim), BF),
            pltpu.VMEM((layers, GU_CHUNKS, CORES, rows, 2 * g_cols), BF),
            pltpu.VMEM((layers, 2, rows // n_y, head_dim), BF),
            pltpu.VMEM(gamma_ln.shape, F32), pltpu.VMEM(cos_all.shape, F32), pltpu.VMEM(sin_all.shape, F32),
            dma((6 + layers,)),
            dma((4,)), dma((layers * (2 + GU_CHUNKS), 3)), dma((layers * HALVES, 5)),
            dma((layers,)), dma((layers, 4)),
            dma((layers,)), dma((layers, 5)),
            dma((layers,)), dma((layers,)),
            dma((3,)), dma((n_chunks, 5)),
            dma((layers + 1,)),
        ],
        compiler_params=pltpu.CompilerParams(collective_id=0, has_side_effects=True, vmem_limit_bytes=67043328),
    )(gamma_ln, cos_all, sin_all, x_tokens, w_q, w_kv, w_gu, w_o, w_d)
    shapes = [jax.ShapeDtypeStruct(r.shape, r.dtype) for r in results]
    return pl.pallas_call(
        take_over, out_shape=shapes, in_specs=[anywhere] * 3, out_specs=[anywhere] * 3,
        scratch_shapes=[pltpu.VMEM((seq, d_model), BF), pltpu.VMEM(cache.shape, BF), pltpu.VMEM(cache.shape, BF), dma((2, 4))],
    )(*results)


def solution(mesh):
    batch_axes = ('dp', 'wy', 'wx')
    in_specs = (P(batch_axes), P(), P(None, 'wx', 'wy'), P(None, 'wx'), P(None, 'wx', None, 'wy'), P(None, 'wy', 'wx'), P(None, 'wy', 'wx'))
    out_specs = (P(batch_axes), P(None, batch_axes), P(None, batch_axes))
    sizes = dict(mesh.shape)
    return jax.shard_map(functools.partial(run_layers, sizes), mesh=mesh, in_specs=in_specs, out_specs=out_specs, check_vma=False)
```
